256 devices in a mesh: gz: 8 (over z), xy: 32 (over x, y, core).
Axes of the slice: x: 4, y: 4, z: 8, core: 2. Of those that a mesh axis runs over, the one named last changes fastest.
Arguments:
- volume: float32 [128, 1536, 128], P('gz', 'xy'), may hold values from 0 to 1
- measured: float32 [2, 5, 160, 1536], P(None, None, 'gz', 'xy'), may hold values from 0 to 1
- view_order: int32 [48], replicated, may hold values from 0 to 47, each once
Outputs:
- volume_out: float32 [128, 1536, 128], P('gz', 'xy')
- residual: float32 [5, 160, 1536], P(None, 'gz', 'xy')
The draws below stay inside these ranges and needn't reach their ends.
Inputs may be any that keep to these rules, and one draw needn't show every extreme that they name: `view_order`: A permutation of the numbers 0 to 47.
All inputs are finite; a program needn't handle non-finite values.
Results may differ from the reference program's by a relative error of at most 0.00078.
Values may be sent and summed in bfloat16 or wider, within the bound.
No kernel may reach another device: no remote copies, remote signals or barrier semaphores. Data moves between devices by JAX's collectives and lax.ppermute only.
A program may use at most 64 MiB of HBM per device.

```python
import math
import jax
import jax.numpy as jnp
from jax import lax

X_DEV = 48
NY = 128
VIEWS = 5
SUBSETS = 2
ANGLES = 48
NX = 1536
NZ = 128
DR = 160
DC = 1536
N_XY = 32


def levels(own_key, extent, shards, smallest, top_value):
    def one(dim, parts):
        heights = jax.random.uniform(jax.random.fold_in(jax.random.fold_in(own_key, 6), dim), (parts,), jnp.float32, smallest / len(shards), top_value / len(shards))
        return jnp.repeat(jnp.exp(heights), extent[dim] // parts).reshape((-1,) + (1,) * (len(extent) - dim - 1))

    level = one(*shards[0])
    for cut in shards[1:]:
        level = level * one(*cut)
    return level


def setup_inputs(seed: int = 0) -> dict:
    seeds = jax.random.split(jax.random.key(seed), 4)
    return {
        "volume": jnp.clip(1.0 * jax.random.uniform(seeds[0], (NZ, NX, NY), jnp.float32) ** levels(seeds[0], (NZ, NX, NY), ((0, 8), (1, 32)), -0.2, 0.2), 0.0, 1.0),
        "measured": jnp.clip(1.0 * jax.random.uniform(seeds[1], (SUBSETS, VIEWS, DR, DC), jnp.float32) ** levels(seeds[1], (SUBSETS, VIEWS, DR, DC), ((2, 8), (3, 32)), -0.2, 0.2), 0.0, 1.0),
        "view_order": jax.random.permutation(seeds[2], ANGLES).astype(jnp.int32),
    }


def column_weights(view_angle, x_first, x_count, nx_all, ny_all, dc_all):
    x_coords = jnp.asarray(x_first).astype(jnp.float32) + jnp.arange(x_count, dtype=jnp.float32) - (nx_all - 1) / 2.0
    y_coords = jnp.arange(ny_all, dtype=jnp.float32) - (ny_all - 1) / 2.0
    cosine = jnp.cos(view_angle)
    sine_value = jnp.sin(view_angle)
    along_axis = x_coords[:, None] * cosine + y_coords[None, :] * sine_value
    depth_axis = y_coords[None, :] * cosine - x_coords[:, None] * sine_value
    source = 2.0 * nx_all
    position = (dc_all - 1) / 2.0 + 0.9 * (dc_all / nx_all) * along_axis * source / (source + depth_axis)
    position = position.reshape(x_count // 8, 8, ny_all // 16, 16).transpose(0, 2, 1, 3).reshape(-1, 128)
    lowest = jnp.min(position, axis=1)
    first_block = jnp.clip(jnp.floor(lowest / 64.0), 0, dc_all // 64 - 2).astype(jnp.int32)
    columns = (first_block * 64)[:, None] + jnp.arange(128, dtype=jnp.int32)[None, :]
    weights = jnp.maximum(0.0, 1.0 - jnp.abs(position[:, :, None] - columns[:, None, :].astype(position.dtype)))
    return weights.astype(jnp.bfloat16), first_block


def place_blocks(values, first_block, block_count):
    block_ids = jnp.arange(block_count, dtype=jnp.int32)
    low_onehot = (first_block[:, None] == block_ids[None, :]).astype(values.dtype)
    high_onehot = (first_block[:, None] + 1 == block_ids[None, :]).astype(values.dtype)
    result = jnp.einsum('sb,skc->kbc', low_onehot, values[:, :, :64], precision=lax.Precision.HIGHEST)
    result = result + jnp.einsum('sb,skc->kbc', high_onehot, values[:, :, 64:], precision=lax.Precision.HIGHEST)
    return result.reshape(values.shape[1], block_count * 64)


def row_weights(row_ids, slice_ids, dr_all, nz_all):
    position = (dr_all - 1) / 2.0 + 0.96 * (dr_all / nz_all) * (slice_ids.astype(jnp.float32) - (nz_all - 1) / 2.0)
    inside = ((row_ids >= 0) & (row_ids < dr_all)).astype(jnp.float32)
    hat = jnp.maximum(0.0, 1.0 - jnp.abs(position[None, :] - row_ids[:, None].astype(jnp.float32)) / 2.0)
    return hat * inside[:, None]


def reference(volume, measured, view_order):
    block_count = DC // 64
    tiled = volume.reshape(NZ, N_XY, X_DEV // 8, 8, NY // 16, 16).transpose(1, 2, 4, 0, 3, 5).reshape(N_XY, -1, NZ, 128)
    axial_weights = row_weights(jnp.arange(DR, dtype=jnp.int32), jnp.arange(NZ, dtype=jnp.int32), DR, NZ)
    slice_total = jnp.sum(axial_weights, axis=0)
    ray_rows = jnp.sum(axial_weights, axis=1)
    strip_ids = jnp.arange(N_XY, dtype=jnp.int32)
    residual = jnp.zeros((VIEWS, DR, DC), jnp.float32)
    for subset in range(SUBSETS):
        chosen = view_order[subset * VIEWS:(subset + 1) * VIEWS]
        angles = 2.0 * math.pi * chosen.astype(jnp.float32) / ANGLES

        def forward(totals, item):
            tiles, strip_index = item
            placed_sum, column_sum = totals
            tiles_rounded = lax.optimization_barrier(tiles.astype(jnp.bfloat16)).astype(jnp.float32)
            new_placed = []
            new_columns = []
            for view_index in range(VIEWS):
                weights, first_block = column_weights(angles[view_index], strip_index * X_DEV, X_DEV, NX, NY, DC)
                weights = lax.optimization_barrier(weights).astype(jnp.float32)
                column_sums = jnp.einsum('szv,svc->szc', tiles_rounded, weights, precision=lax.Precision.HIGHEST)
                new_placed.append(place_blocks(column_sums, first_block, block_count))
                new_columns.append(place_blocks(jnp.sum(weights, axis=1)[:, None, :], first_block, block_count)[0])
            return (placed_sum + jnp.stack(new_placed), column_sum + jnp.stack(new_columns)), None

        start = (jnp.zeros((VIEWS, NZ, DC), jnp.float32), jnp.zeros((VIEWS, DC), jnp.float32))
        (placed, column_total), leftover = lax.scan(forward, start, (tiled, strip_ids))
        projection = jnp.einsum('rz,vzc->vrc', axial_weights, placed, precision=lax.Precision.HIGHEST)
        ray_sums = ray_rows[None, :, None] * column_total[:, None, :]
        residual = measured[subset] - projection / jnp.maximum(ray_sums, 1.0)
        rounded = lax.optimization_barrier(residual.astype(jnp.bfloat16)).astype(jnp.float32)
        smeared = jnp.einsum('rz,vrc->vzc', axial_weights, rounded, precision=lax.Precision.HIGHEST).astype(jnp.bfloat16)
        smeared = lax.optimization_barrier(smeared).astype(jnp.float32)

        def backward(item):
            tiles, strip_index = item
            back_total = jnp.zeros(tiles.shape, jnp.float32)
            norm_total = jnp.zeros(tiles.shape, jnp.float32)
            for view_index in range(VIEWS):
                weights, first_block = column_weights(angles[view_index], strip_index * X_DEV, X_DEV, NX, NY, DC)
                weights = lax.optimization_barrier(weights).astype(jnp.float32)
                pieces = smeared[view_index].reshape(NZ, block_count, 64)
                window = jnp.concatenate((jnp.take(pieces, first_block, axis=1), jnp.take(pieces, first_block + 1, axis=1)), axis=2)
                back_total = back_total + jnp.einsum('zsc,svc->szv', window, weights, precision=lax.Precision.HIGHEST)
                norm_total = norm_total + slice_total[None, :, None] * jnp.sum(weights, axis=2)[:, None, :]
            return tiles + back_total / jnp.maximum(norm_total, 1.0)

        tiled = lax.map(backward, (tiled, strip_ids))
    volume_out = tiled.reshape(N_XY, X_DEV // 8, NY // 16, NZ, 8, 16).transpose(3, 0, 1, 4, 2, 5).reshape(NZ, NX, NY)
    return volume_out, residual
```

```python
import functools
import math

import jax
import jax.numpy as jnp
from jax import lax
from jax.experimental import pallas as pl
from jax.experimental.pallas import tpu as pltpu
from jax.sharding import PartitionSpec as P

Z_DEV = 16
X_DEV = 48
NY = 128
COLS_DEV = 48
ROWS_DEV = 20
VIEWS = 5
SUBSETS = 2
ANGLES = 48
N_XY = 32
N_GZ = 8
NX = X_DEV * N_XY
NZ = Z_DEV * N_GZ
DR = ROWS_DEV * N_GZ
DC = COLS_DEV * N_XY

WIN = 176
LANES = 256
MEAS_AT = LANES - COLS_DEV
Z_HALO = 6
Z_ALL = Z_DEV + 2 * Z_HALO
ONES = Z_ALL
Z_PAD = 32
GROUPS = 6
ROWS_PER = (5, 4)
ROWS_BELOW = (3, 0)
M_HALO = 8
M_ROWS = 40
FULL = 15 * 128
SUMS = 4
TILE = 16
TILES_Y = NY // TILE
TILES = X_DEV // TILE * TILES_Y
VOXELS = TILE * TILE
COLS_TILE = 40
VOLUME = (Z_DEV, X_DEV, NY)
PLACE = (0, 40, 80, 128, 168)
DEPTH = 208
HALO_ROWS = Z_HALO * X_DEV
INNER_ROWS = HALO_ROWS // 2
EDGE_AT = HALO_ROWS + INNER_ROWS
EDGE_ROWS = SUBSETS * VIEWS * M_HALO
SENT_ROWS = EDGE_AT + EDGE_ROWS
PITCH = 56
OUT_PITCH = 24
TABLE = (16, 128)
SHIFT_AT = 32
TILE_AT = 64


def iota(shape, dim):
    return lax.broadcasted_iota(jnp.int32, shape, dim)


def slice_of(i, gz):
    low = Z_DEV * gz - Z_HALO + (i - Z_DEV)
    high = Z_DEV * gz + Z_DEV + (i - Z_DEV - Z_HALO)
    return jnp.where(i < Z_DEV, Z_DEV * gz + i, jnp.where(i < Z_DEV + Z_HALO, low, high))


def hat(row, z):
    position = (DR - 1) / 2.0 + 0.96 * (DR / NZ) * (z.astype(jnp.float32) - (NZ - 1) / 2.0)
    value = jnp.maximum(0.0, 1.0 - jnp.abs(position - row.astype(jnp.float32)) / 2.0)
    ok = (row >= 0) & (row < DR) & (z >= 0) & (z < NZ)
    return jnp.where(ok, value, 0.0)


def first_row(gz, subset):
    return ROWS_DEV * gz - ROWS_BELOW[subset] - ((gz + 1) >> 1)


def slot_weights(group, slot, i, gz, subset):
    per = ROWS_PER[subset]
    row = first_row(gz, subset) + group * per + slot
    return jnp.where((slot < per) & (i < Z_ALL), hat(row, slice_of(i, gz)), 0.0)


def tile_offsets(table_ref, subset, tile):
    return [
        pl.multiple_of(table_ref[subset * VIEWS + v, TILE_AT + tile], 8) for v in range(VIEWS)
    ]


def coordinate(x, y, cosine, sine):
    xc = x - (NX - 1) / 2.0
    yc = y - (NY - 1) / 2.0
    source = 2.0 * NX
    along = xc * cosine + yc * sine
    depth = yc * cosine - xc * sine
    return (DC - 1) / 2.0 + 0.9 * (DC / NX) * along * source / (source + depth)


def fill_table(cosine, sine, xy):
    lane = iota(TABLE, 1)
    tile = lane - TILE_AT
    is_tile = lane >= TILE_AT
    strip = lane & (N_XY - 1)
    x = jnp.where(is_tile, xy * X_DEV + (tile >> 3) * TILE, strip * X_DEV).astype(jnp.float32)
    y = jnp.where(is_tile, (tile & 7) * TILE, 0).astype(jnp.float32)
    dx = jnp.where(is_tile, TILE - 1.0, X_DEV - 1.0)
    dy = jnp.where(is_tile, TILE - 1.0, NY - 1.0)
    least = jnp.minimum(
        jnp.minimum(coordinate(x, y, cosine, sine), coordinate(x + dx, y, cosine, sine)),
        jnp.minimum(coordinate(x, y + dy, cosine, sine), coordinate(x + dx, y + dy, cosine, sine)),
    )
    least = jnp.floor(least).astype(jnp.int32)
    start = least - 2
    own = jnp.sum(jnp.where(lane == xy, start, 0).astype(jnp.float32), axis=1, keepdims=True)
    tiles = jnp.maximum(least - 1 - own.astype(jnp.int32), 0) & ~7
    table = jnp.where(lane < SHIFT_AT, start & ~127, start & 127)
    return jnp.where(is_tile, tiles, table), own


def positions(u_ref, cosine, sine, own, subset, xy):
    t = iota((TILES, VOXELS), 0)
    l = iota((TILES, VOXELS), 1)
    x = ((t >> 3) * TILE + (l >> 4) + xy * X_DEV).astype(jnp.float32)
    y = ((t & 7) * TILE + (l & 15)).astype(jnp.float32)
    for v in range(VIEWS):
        at = subset * VIEWS + v
        u = coordinate(x, y, cosine[at : at + 1, 0:1], sine[at : at + 1, 0:1])
        u_ref[v] = u - own[at : at + 1, :]


def weights(u_ref, offsets, tile):
    c = iota((COLS_TILE, VOXELS), 0).astype(jnp.float32)
    pieces = []
    for v in range(VIEWS):
        u = u_ref[v, pl.ds(tile, 1), :] - offsets[v].astype(jnp.float32)
        pieces.append(jnp.maximum(0.0, 1.0 - jnp.abs(u - c)))
    pieces.insert(3, jnp.zeros((8, VOXELS), jnp.float32))
    return jnp.concatenate(pieces, axis=0).astype(jnp.bfloat16)


def forward(w_ref, slices, acc_ref, m_ref, table_ref, out_ref, subset, gz):
    acc_ref[...] = jnp.zeros_like(acc_ref)
    for tile in range(TILES):
        offsets = tile_offsets(table_ref, subset, tile)
        part = lax.dot_general(
            w_ref[tile],
            jnp.concatenate([slices(tile)] * 4, axis=0),
            (((1,), (1,)), ((), ())),
            preferred_element_type=jnp.float32,
        )
        for v in range(VIEWS):
            acc_ref[v, pl.ds(offsets[v], COLS_TILE), :] += part[PLACE[v] : PLACE[v] + COLS_TILE]
    per = ROWS_PER[subset]
    half = per + 1
    size = GROUPS * 2 * half
    k = iota((size, 128), 0)
    lane = iota((size, 128), 1)
    i = lane & (Z_PAD - 1)
    group = (k * 43) >> 9 if half == 6 else (k * 205) >> 11
    slot = k - group * 2 * half
    is_low = slot < half
    slot = jnp.where(is_low, slot, slot - half)
    rows = slot_weights(group, slot, i, gz, subset)
    rows = jnp.where((slot == per) & (i == ONES), 1.0, rows)
    rounded = rows.astype(jnp.bfloat16).astype(jnp.float32)
    rows = jnp.where(lane < 2 * Z_PAD, rounded, rows - rounded).astype(jnp.bfloat16)
    left_over = (iota((WIN, 128), 1) & Z_PAD) != 0
    used = GROUPS * VIEWS * 2 * half
    out_ref[used:, :] = jnp.zeros((out_ref.shape[0] - used, 128), jnp.float32)
    for v in range(VIEWS):
        sums = acc_ref[v]
        rounded = sums.astype(jnp.bfloat16).astype(jnp.float32)
        sums = jnp.where(left_over, sums - rounded, rounded).astype(jnp.bfloat16)
        sums = lax.dot_general(
            rows, sums, (((1,), (1,)), ((), ())), preferred_element_type=jnp.float32
        )
        high = jnp.concatenate(
            (sums[:, 128:WIN], jnp.zeros((size, LANES - WIN), jnp.float32)), axis=1
        )
        part = jnp.where(is_low, sums[:, 0:128], high) + m_ref[v, 0:size, :]
        out_ref[v * size : (v + 1) * size, :] = part


def smear(recv_ref, sm_ref, gz):
    i = iota((Z_PAD, GROUPS * 8), 0)
    k = iota((Z_PAD, GROUPS * 8), 1)
    rows = slot_weights(k >> 3, k & 7, i, gz, 0)
    ones = iota((Z_PAD, LANES), 0) == ONES
    for v in range(VIEWS):
        got = recv_ref[v * GROUPS : (v + 1) * GROUPS]
        got = got.astype(jnp.float32).reshape(GROUPS * 8, LANES)
        smeared = jnp.dot(
            rows, got, precision=lax.Precision.HIGHEST, preferred_element_type=jnp.float32
        )
        sm_ref[v] = jnp.where(ones, 1.0, smeared).astype(jnp.bfloat16).astype(jnp.float32)


def smear_last(recv_ref, sm_ref, res_ref, gz):
    size = 2 * Z_PAD + 24
    i = iota((size, GROUPS * 8), 0)
    k = iota((size, GROUPS * 8), 1)
    part = k & 7
    rows = slot_weights(k >> 3, part & 3, i & (Z_PAD - 1), gz, 1)
    rows = jnp.where((part >= 4) == (i >= Z_PAD), rows, 0.0)
    j = i - 2 * Z_PAD + ((gz + 1) >> 1)
    picked = (k == ((j >> 2) << 3) + 4 + (j & 3)).astype(jnp.float32)
    rows = jnp.where(i >= 2 * Z_PAD, picked, rows)
    ones = iota((Z_PAD, LANES), 0) == ONES
    part = iota((GROUPS * 8, 128), 0) & 7
    exact = (part >= 4) & (iota((GROUPS * 8, 128), 1) >= MEAS_AT - 128)
    for v in range(VIEWS):
        got = recv_ref[v * GROUPS * 8 : (v + 1) * GROUPS * 8, :]
        got = jnp.where(exact, got, got.astype(jnp.bfloat16).astype(jnp.float32))
        sums = jnp.dot(
            rows, got, precision=lax.Precision.HIGHEST, preferred_element_type=jnp.float32
        )
        smeared = jnp.concatenate((sums[0:Z_PAD], sums[Z_PAD : 2 * Z_PAD]), axis=1)
        sm_ref[v] = jnp.where(ones, 1.0, smeared).astype(jnp.bfloat16).astype(jnp.float32)
        own = pltpu.roll(sums[2 * Z_PAD :], 256 - MEAS_AT, 1)
        res_ref[v] = own[0:ROWS_DEV, 0:COLS_DEV]


def windows(sm_ref, offsets):
    lane = iota((Z_PAD, 128), 1)
    placed = []
    for v in range(VIEWS):
        at = PLACE[v] & 127
        shift = (at - offsets[v]) & 127
        low = pltpu.roll(sm_ref[v, :, 0:128], shift, 1)
        high = pltpu.roll(sm_ref[v, :, 128:256], shift, 1)
        placed.append(jnp.where(lane < at + 128 - offsets[v], low, high))
    first = jnp.where(lane < 40, placed[0], jnp.where(lane < 80, placed[1], placed[2]))
    first = jnp.where(lane < 120, first, 0.0)
    second = jnp.where(lane < 40, placed[3], jnp.where(lane < 80, placed[4], 0.0))
    both = jnp.concatenate((first, second), axis=1)
    return both.astype(jnp.bfloat16)[:, 0:DEPTH]


def backward(w_ref, sm_ref, table_ref, old, store, subset, gz):
    zi = slice_of(iota((Z_PAD, LANES), 0), gz)
    inside = iota((Z_PAD, LANES), 0) < Z_ALL
    total = jnp.sum(jnp.where(inside, hat(iota((Z_PAD, LANES), 1), zi), 0.0), axis=1, keepdims=True)

    for tile in range(TILES):
        offsets = tile_offsets(table_ref, subset, tile)
        back = jnp.dot(
            windows(sm_ref, offsets), w_ref[tile], preferred_element_type=jnp.float32
        )
        norm = total * back[ONES : ONES + 1, :]
        store(tile, old(tile), back / jnp.maximum(norm, 1.0))


def swap_blocks(rows):
    block = iota((8, 128), 1) >> 4
    for d in (4, 2, 1):
        high = (block & d) != 0
        new = list(rows)
        for i in range(8):
            if i & d == 0:
                a, b = (rows[i], rows[i + d])
                new[i] = jnp.where(high, pltpu.roll(b, 16 * d, 1), a)
                new[i + d] = jnp.where(high, b, pltpu.roll(a, 128 - 16 * d, 1))
        rows = new
    return rows


def relay(source_ref, out_ref, pitch):
    def step(xb, nothing):
        for half in range(2):
            for b in range(2):
                at = xb * TILE + half * 8 + b * 8 * pitch
                rows = [source_ref[pl.ds(at + i, 8, stride=pitch), :] for i in range(8)]
                for q, block in enumerate(swap_blocks(rows)):
                    out_ref[
                        xb * TILES_Y + q, b * 8 : b * 8 + 8, half * 128 : half * 128 + 128
                    ] = block
        return nothing

    lax.fori_loop(0, X_DEV // TILE, step, 0)


def pack_kernel(vol_ref, meas_ref, up_ref, down_ref, row_ref):
    row_ref[...] = jnp.zeros_like(row_ref)
    for out_ref, z, inner, r in (
        (up_ref, Z_DEV - Z_HALO, Z_HALO // 2, ROWS_DEV - M_HALO),
        (down_ref, 0, 0, 0),
    ):
        slices = vol_ref[z * X_DEV : (z + Z_HALO) * X_DEV, :]
        rounded = slices.astype(jnp.bfloat16)
        out_ref[0:HALO_ROWS, :] = rounded
        left = slices - rounded.astype(jnp.float32)
        at = inner * X_DEV
        out_ref[HALO_ROWS:EDGE_AT, :] = left[at : at + INNER_ROWS].astype(jnp.bfloat16)
        for v in range(VIEWS):
            at = (v * ROWS_DEV + r) * SUBSETS
            row_ref[:, 0:COLS_DEV] = meas_ref[at : at + SUBSETS * M_HALO, :]
            row = row_ref[...]
            rounded = row.astype(jnp.bfloat16).astype(jnp.float32)
            both = pltpu.roll(rounded, MEAS_AT - 128, 1)
            both = both + pltpu.roll(row - rounded, MEAS_AT - 128 - COLS_DEV, 1)
            at = EDGE_AT + v * SUBSETS * M_HALO
            out_ref[at : at + SUBSETS * M_HALO, :] = both.astype(jnp.bfloat16)


def prepare_kernel(
    cosine_ref, sine_ref, vol_ref, meas_ref,
    w0_ref, w1_ref, own_ref, mown_ref, flat_ref, table_ref, sem, u_ref,
):
    xy = lax.axis_index("xy")
    cosine = cosine_ref[...]
    sine = sine_ref[...]
    flat_ref[...], own = fill_table(cosine, sine, xy)
    copy = pltpu.make_async_copy(flat_ref, table_ref, sem)
    copy.start()
    relay(vol_ref, own_ref, X_DEV)
    mown_ref[...] = jnp.zeros_like(mown_ref)
    for s in range(SUBSETS):
        for v in range(VIEWS):
            for at, count in ((0, 8), (8, 8), (16, 4)):
                rows = meas_ref[pl.ds((v * ROWS_DEV + at) * 2 + s, count, stride=2), :]
                mown_ref[s, v, at : at + count, MEAS_AT - 128 : 128] = rows
    copy.wait()
    for subset, w_ref in ((0, w0_ref), (1, w1_ref)):
        positions(u_ref, cosine, sine, own, subset, xy)

        def step(tt, nothing):
            for t in range(8):
                tile = tt * 8 + t
                w_ref[tile] = weights(u_ref, tile_offsets(table_ref, subset, tile), tile)
            return nothing

        lax.fori_loop(0, TILES // 8, step, 0)


def first_kernel(
    flat_ref, w_ref, own_ref, mown_ref, low_ref, high_ref,
    out_ref, side_ref, m1_ref, table_ref, sem, halo_ref, acc_ref, raw_ref, m0_ref, edge_ref,
):
    gz = lax.axis_index("gz")
    copy = pltpu.make_async_copy(flat_ref, table_ref, sem)
    copy.start()
    for side, (sent_ref, inner) in enumerate(((low_ref, Z_HALO // 2), (high_ref, 0))):
        left_at = HALO_ROWS - inner * X_DEV
        for z in range(Z_HALO):
            at = z * X_DEV
            rows = sent_ref[at : at + X_DEV, :].astype(jnp.float32)
            if inner <= z < inner + Z_HALO // 2:
                rows = rows + sent_ref[left_at + at : left_at + at + X_DEV, :].astype(jnp.float32)
            at = (side * Z_HALO + z) * PITCH
            halo_ref[at : at + X_DEV, :] = rows
        edge = sent_ref[EDGE_AT:SENT_ROWS, :].astype(jnp.float32)
        edge = edge + pltpu.roll(edge, COLS_DEV, 1)
        edge_ref[side] = jnp.where(iota(edge.shape, 1) >= MEAS_AT - 128, edge, 0.0)
    for z in range(2 * Z_HALO, Z_DEV):
        value = 1.0 if z == ONES - Z_DEV else 0.0
        halo_ref[z * PITCH : z * PITCH + X_DEV, :] = jnp.full((X_DEV, NY), value, jnp.float32)
    relay(halo_ref, side_ref, PITCH)
    for s, m_ref in ((0, m0_ref), (1, m1_ref)):
        per = ROWS_PER[s]
        m_ref[...] = jnp.zeros_like(m_ref)
        for v in range(VIEWS):
            edge = pl.ds(v * 2 * M_HALO + s, M_HALO, stride=2)
            high = edge_ref[1, edge, :]
            joined = jnp.concatenate(
                (
                    edge_ref[0, edge, :],
                    mown_ref[s, v, 0:16, :],
                    jnp.concatenate((mown_ref[s, v, 16:20, :], high[0:4]), axis=0),
                    jnp.concatenate((high[4:8], jnp.zeros((4, 128), jnp.float32)), axis=0),
                ),
                axis=0,
            )
            raw_ref[s, v] = pltpu.roll(
                joined, M_ROWS + ((gz + 1) >> 1) - (M_HALO - ROWS_BELOW[s]), 0
            )
            for group in range(GROUPS):
                at = group * 2 * (per + 1) + per + 1
                m_ref[v, at : at + per, :] = raw_ref[s, v, group * per : (group + 1) * per, :]

    def slices(tile):
        return jnp.concatenate((own_ref[tile], side_ref[tile]), axis=0).astype(jnp.bfloat16)

    copy.wait()
    forward(w_ref, slices, acc_ref, m0_ref, table_ref, out_ref, 0, gz)


def middle_kernel(
    flat_ref, recv_ref, own_ref, side_ref, m_ref, w0_ref, w1_ref,
    out_ref, new_ref, table_ref, sem, sm_ref, vb_ref, acc_ref,
):
    gz = lax.axis_index("gz")
    copy = pltpu.make_async_copy(flat_ref, table_ref, sem)
    copy.start()
    smear(recv_ref, sm_ref, gz)
    copy.wait()
    ones = iota((Z_PAD, VOXELS), 0) == ONES

    def old(tile):
        return jnp.concatenate((own_ref[tile], side_ref[tile]), axis=0)

    def store(tile, old, change):
        new = jnp.where(ones, 1.0, old + change)
        new_ref[tile] = new[0:Z_DEV]
        vb_ref[tile] = new.astype(jnp.bfloat16)

    backward(w0_ref, sm_ref, table_ref, old, store, 0, gz)
    forward(w1_ref, lambda tile: vb_ref[tile], acc_ref, m_ref, table_ref, out_ref, 1, gz)


def last_kernel(
    flat_ref, recv_ref, old_ref, w_ref,
    out_ref, res_ref, table_ref, sem, sm_ref, new_ref, block_ref, sems,
):
    gz = lax.axis_index("gz")
    copy = pltpu.make_async_copy(flat_ref, table_ref, sem)
    copy.start()
    smear_last(recv_ref, sm_ref, res_ref, gz)
    copy.wait()
    copies = []

    def store(tile, old, change):
        new_ref[tile] = old + change[0:Z_DEV]
        xb = tile // TILES_Y
        if tile % TILES_Y < TILES_Y - 1:
            return
        for half in range(2):
            for b in range(Z_DEV // 8):
                blocks = [
                    new_ref[xb * TILES_Y + q, b * 8 : b * 8 + 8, half * 128 : half * 128 + 128]
                    for q in range(TILES_Y)
                ]
                at = half * 8 + b * 8 * OUT_PITCH
                for i, row in enumerate(swap_blocks(blocks)):
                    block_ref[xb, pl.ds(at + i, 8, stride=OUT_PITCH), :] = row
        for z in range(Z_DEV):
            copies.append(
                pltpu.make_async_copy(
                    block_ref.at[xb, pl.ds(z * OUT_PITCH, TILE), :],
                    out_ref.at[z, pl.ds(xb * TILE, TILE), :],
                    sems.at[xb, z],
                )
            )
            copies[-1].start()

    backward(w_ref, sm_ref, table_ref, lambda tile: old_ref[tile], store, 1, gz)
    for copy in copies:
        copy.wait()


def owner_kernel(flat_ref, recv_ref, out_ref, table_ref, sem, acc_ref, sum_ref, mea_ref, *, subset):
    gz = lax.axis_index("gz")
    xy = lax.axis_index("xy")
    copy = pltpu.make_async_copy(flat_ref, table_ref, sem)
    copy.start()
    view = jnp.minimum(xy // GROUPS, VIEWS - 1)
    group = xy % GROUPS
    at = subset * VIEWS + view
    per = ROWS_PER[subset]
    half = per + 1
    lane = iota((8, 128), 1)
    sum_ref[...] = jnp.zeros_like(sum_ref)
    mea_ref[...] = jnp.zeros_like(mea_ref)
    end = N_XY * 2 * half - 8

    def upper(s):
        row = s * 2 * half + half
        last = recv_ref[min(row, end) : min(row, end) + 8, :]
        return pltpu.roll(last, 8 - (row - end), 0) if row > end else last

    for s in range(N_XY):
        column = s * COLS_DEV
        own = jnp.where(lane >= MEAS_AT - 128, upper(s), 0.0)
        own = pltpu.roll(own, (column + 256 - MEAS_AT) % 128, 1)
        block = column // 128 * 128
        offset = column - block
        mea_ref[:, block : block + 128] += jnp.where(lane >= offset, own, 0.0)
        if offset + COLS_DEV > 128:
            mea_ref[:, block + 128 : block + 256] += jnp.where(lane < offset, own, 0.0)
    copy.wait()
    for s in range(N_XY):
        base = pl.multiple_of(table_ref[at, s], 128)
        shift = table_ref[at, SHIFT_AT + s]
        row = s * 2 * half
        low = pltpu.roll(recv_ref[row : row + 8, :], shift, 1)
        high = pltpu.roll(jnp.where(lane < WIN - 128, upper(s), 0.0), shift, 1)
        wrapped = lane < shift
        part_ref = sum_ref.at[s % SUMS]
        part_ref[:, pl.ds(base, 128)] += jnp.where(wrapped, 0.0, low)
        part_ref[:, pl.ds(base + 128, 128)] += jnp.where(wrapped, low, high)
        part_ref[:, pl.ds(base + 256, 128)] += jnp.where(wrapped, high, 0.0)
    slot = iota((8, NZ), 0)
    row = first_row(gz, subset) + group * per + slot
    ray_rows = jnp.where(slot < per, hat(row, iota((8, NZ), 1)), 0.0)
    ray_rows = jnp.sum(ray_rows, axis=1, keepdims=True)
    sums = sum_ref[0]
    for part in range(1, SUMS):
        sums = sums + sum_ref[part]
    totals = sums[per : per + 1, :]
    acc_ref[...] = mea_ref[...] - sums / jnp.maximum(ray_rows * totals, 1.0)
    for t in range(N_XY):
        base = pl.multiple_of(table_ref[at, t], 128)
        shift = table_ref[at, SHIFT_AT + t]
        back = (128 - shift) & 127
        a = pltpu.roll(acc_ref[:, pl.ds(base, 128)], back, 1)
        b = pltpu.roll(acc_ref[:, pl.ds(base + 128, 128)], back, 1)
        c = pltpu.roll(acc_ref[:, pl.ds(base + 256, 128)], back, 1)
        kept = lane < 128 - shift
        low = jnp.where(kept, a, b)
        high = jnp.where(kept, b, c)
        if subset == 0:
            out_ref[t, :, 0:128] = low.astype(jnp.bfloat16)
            out_ref[t, :, 128:256] = high.astype(jnp.bfloat16)
            continue
        column = t * COLS_DEV
        block = column // 128 * 128
        offset = column - block
        turn = (MEAS_AT - 128 - offset) % 128
        own = pltpu.roll(acc_ref[:, block : block + 128], turn, 1)
        if offset + COLS_DEV > 128:
            more = pltpu.roll(acc_ref[:, block + 128 : block + 256], turn, 1)
            own = jnp.where(lane < MEAS_AT - offset, own, more)
        high = jnp.where(lane >= MEAS_AT - 128, own, high)
        out_ref[t * 8 : (t + 1) * 8, :] = jnp.where(slot < 4, low, pltpu.roll(high, 4, 0))


def call(kernel, inputs, outs, scratch, name, table=True):
    vmem = pl.BlockSpec(memory_space=pltpu.VMEM)
    anywhere = pl.BlockSpec(memory_space=pl.ANY)
    inputs = [pltpu.with_memory_space_constraint(x, pltpu.VMEM) for x in inputs]
    if table:
        scratch = [pltpu.SMEM(TABLE, jnp.int32), pltpu.SemaphoreType.DMA, *scratch]
    return pl.pallas_call(
        kernel,
        in_specs=[vmem] * len(inputs),
        out_specs=[anywhere if out.shape == VOLUME else vmem for out in outs],
        out_shape=outs,
        scratch_shapes=scratch,
        compiler_params=pltpu.CompilerParams(vmem_limit_bytes=12 * 1024 * 1024),
        name=name,
    )(*inputs)


def exchanged(parts, shape):
    sent = lax.all_to_all(
        parts.reshape(shape), "xy", split_axis=0, concat_axis=0, tiled=True
    )
    return sent.reshape(parts.shape)


def local(volume, measured, view_order):
    f32 = jnp.float32
    bf16 = jnp.bfloat16
    vmem = pltpu.VMEM
    angles = 2.0 * math.pi * view_order[: SUBSETS * VIEWS].astype(f32) / ANGLES
    angles = jnp.broadcast_to(jnp.pad(angles, (0, TABLE[0] - SUBSETS * VIEWS))[:, None], TABLE)
    flat = pltpu.with_memory_space_constraint(volume.reshape(Z_DEV * X_DEV, NY), vmem)
    rows = measured.transpose(1, 2, 0, 3).reshape(VIEWS * ROWS_DEV * SUBSETS, COLS_DEV)
    made = vmem((TILES, DEPTH, VOXELS), bf16)
    slices = vmem((TILES, Z_DEV, VOXELS), f32)
    sm_scratch = vmem((VIEWS, Z_PAD, LANES), f32)
    acc_scratch = vmem((VIEWS, WIN, 128), f32)
    row_scratch = vmem((8, FULL), f32)
    owner_scratch = [row_scratch, vmem((SUMS, 8, FULL), f32), row_scratch]

    sent = vmem((SENT_ROWS, 128), bf16)
    up, down = call(
        pack_kernel,
        (flat, rows),
        [sent, sent],
        [vmem((SUBSETS * M_HALO, 128), f32)],
        "pack",
        table=False,
    )
    next_up = [(i, (i + 1) % N_GZ) for i in range(N_GZ)]
    low = lax.ppermute(up, "gz", next_up)
    high = lax.ppermute(down, "gz", [(j, i) for i, j in next_up])
    w0, w1, own, mown, table = call(
        prepare_kernel,
        (jnp.cos(angles), jnp.sin(angles), flat, rows),
        [made, made, slices, vmem((SUBSETS, VIEWS, 24, 128), f32), vmem(TABLE, jnp.int32)],
        [vmem((VIEWS, TILES, VOXELS), f32)],
        "prepare",
    )
    partial, side, m1 = call(
        first_kernel,
        (table, w0, own, mown, low, high),
        [vmem((N_XY * 12, 128), f32), slices, vmem((VIEWS, 64, 128), f32)],
        [
            vmem((Z_DEV * PITCH, NY), f32),
            acc_scratch,
            vmem((SUBSETS, VIEWS, M_ROWS, 128), f32),
            vmem((VIEWS, 72, 128), f32),
            vmem((2, EDGE_ROWS, 128), f32),
        ],
        "first",
    )
    (rounded,) = call(
        functools.partial(owner_kernel, subset=0),
        (table, exchanged(partial, (N_XY, 3, 4, 128))),
        [vmem((N_XY, 8, LANES), bf16)],
        owner_scratch,
        "owner_a",
    )
    partial, new = call(
        middle_kernel,
        (table, exchanged(rounded, rounded.shape), own, side, m1, w0, w1),
        [vmem((N_XY * 10, 128), f32), slices],
        [sm_scratch, vmem((TILES, Z_PAD, VOXELS), bf16), acc_scratch],
        "middle",
    )
    (final,) = call(
        functools.partial(owner_kernel, subset=1),
        (table, exchanged(partial, (N_XY, 5, 2, 128))),
        [vmem((N_XY * 8, 128), f32)],
        owner_scratch,
        "owner_b",
    )
    volume_out, residual = call(
        last_kernel,
        (table, exchanged(final, (N_XY, 8, 128)), new, w1),
        [
            jax.ShapeDtypeStruct(VOLUME, f32),
            jax.ShapeDtypeStruct((VIEWS, ROWS_DEV, COLS_DEV), f32),
        ],
        [
            sm_scratch,
            slices,
            vmem((X_DEV // TILE, Z_DEV * OUT_PITCH, NY), f32),
            pltpu.SemaphoreType.DMA((X_DEV // TILE, Z_DEV)),
        ],
        "last",
    )
    return volume_out, residual


def solution(mesh):
    in_specs = (P("gz", "xy", None), P(None, None, "gz", "xy"), P())
    out_specs = (P("gz", "xy", None), P(None, "gz", "xy"))
    return jax.shard_map(local, mesh=mesh, in_specs=in_specs, out_specs=out_specs, check_vma=False)
```

```python
import functools
import math

import jax
import jax.numpy as jnp
from jax import lax
from jax.experimental import pallas as pl
from jax.experimental.pallas import tpu as pltpu
from jax.sharding import PartitionSpec as P

Z_DEV = 16
X_DEV = 48
NY = 128
COLS_DEV = 48
ROWS_DEV = 20
VIEWS = 5
SUBSETS = 2
ANGLES = 48
N_XY = 32
N_GZ = 8
NX = X_DEV * N_XY
NZ = Z_DEV * N_GZ
DR = ROWS_DEV * N_GZ
DC = COLS_DEV * N_XY

WIN = 176
LANES = 256
MEAS_AT = LANES - COLS_DEV
Z_HALO = 6
Z_ALL = Z_DEV + 2 * Z_HALO
ONES = Z_ALL
Z_PAD = 32
GROUPS = 6
ROWS_PER = (5, 4)
ROWS_BELOW = (3, 0)
M_HALO = 8
M_ROWS = 40
FULL = 15 * 128
SUMS = 4
TILE = 16
TILES_Y = NY // TILE
TILES = X_DEV // TILE * TILES_Y
VOXELS = TILE * TILE
COLS_TILE = 40
VOLUME = (Z_DEV, X_DEV, NY)
PLACE = (0, 40, 80, 128, 168)
DEPTH = 208
HALO_ROWS = Z_HALO * X_DEV
INNER_ROWS = HALO_ROWS // 2
EDGE_AT = HALO_ROWS + INNER_ROWS
EDGE_ROWS = SUBSETS * VIEWS * M_HALO
SENT_ROWS = EDGE_AT + EDGE_ROWS
PITCH = 56
OUT_PITCH = 24
TABLE = (16, 128)
SHIFT_AT = 32
TILE_AT = 64


def iota(shape, dim):
    return lax.broadcasted_iota(jnp.int32, shape, dim)


def slice_of(i, gz):
    low = Z_DEV * gz - Z_HALO + (i - Z_DEV)
    high = Z_DEV * gz + Z_DEV + (i - Z_DEV - Z_HALO)
    return jnp.where(i < Z_DEV, Z_DEV * gz + i, jnp.where(i < Z_DEV + Z_HALO, low, high))


def hat(row, z):
    position = (DR - 1) / 2.0 + 0.96 * (DR / NZ) * (z.astype(jnp.float32) - (NZ - 1) / 2.0)
    value = jnp.maximum(0.0, 1.0 - jnp.abs(position - row.astype(jnp.float32)) / 2.0)
    ok = (row >= 0) & (row < DR) & (z >= 0) & (z < NZ)
    return jnp.where(ok, value, 0.0)


def first_row(gz, subset):
    return ROWS_DEV * gz - ROWS_BELOW[subset] - ((gz + 1) >> 1)


def slot_weights(group, slot, i, gz, subset):
    per = ROWS_PER[subset]
    row = first_row(gz, subset) + group * per + slot
    return jnp.where((slot < per) & (i < Z_ALL), hat(row, slice_of(i, gz)), 0.0)


def tile_offsets(table_ref, subset, tile):
    return [
        pl.multiple_of(table_ref[subset * VIEWS + v, TILE_AT + tile], 8) for v in range(VIEWS)
    ]


def coordinate(x, y, cosine, sine):
    xc = x - (NX - 1) / 2.0
    yc = y - (NY - 1) / 2.0
    source = 2.0 * NX
    along = xc * cosine + yc * sine
    depth = yc * cosine - xc * sine
    return (DC - 1) / 2.0 + 0.9 * (DC / NX) * along * source / (source + depth)


def fill_table(cosine, sine, xy):
    lane = iota(TABLE, 1)
    tile = lane - TILE_AT
    is_tile = lane >= TILE_AT
    strip = lane & (N_XY - 1)
    x = jnp.where(is_tile, xy * X_DEV + (tile >> 3) * TILE, strip * X_DEV).astype(jnp.float32)
    y = jnp.where(is_tile, (tile & 7) * TILE, 0).astype(jnp.float32)
    dx = jnp.where(is_tile, TILE - 1.0, X_DEV - 1.0)
    dy = jnp.where(is_tile, TILE - 1.0, NY - 1.0)
    least = jnp.minimum(
        jnp.minimum(coordinate(x, y, cosine, sine), coordinate(x + dx, y, cosine, sine)),
        jnp.minimum(coordinate(x, y + dy, cosine, sine), coordinate(x + dx, y + dy, cosine, sine)),
    )
    least = jnp.floor(least).astype(jnp.int32)
    start = least - 2
    own = jnp.sum(jnp.where(lane == xy, start, 0).astype(jnp.float32), axis=1, keepdims=True)
    tiles = jnp.maximum(least - 1 - own.astype(jnp.int32), 0) & ~7
    table = jnp.where(lane < SHIFT_AT, start & ~127, start & 127)
    return jnp.where(is_tile, tiles, table), own


def positions(u_ref, cosine, sine, own, subset, xy):
    t = iota((TILES, VOXELS), 0)
    l = iota((TILES, VOXELS), 1)
    x = ((t >> 3) * TILE + (l >> 4) + xy * X_DEV).astype(jnp.float32)
    y = ((t & 7) * TILE + (l & 15)).astype(jnp.float32)
    for v in range(VIEWS):
        at = subset * VIEWS + v
        u = coordinate(x, y, cosine[at : at + 1, 0:1], sine[at : at + 1, 0:1])
        u_ref[v] = u - own[at : at + 1, :]


def weights(u_ref, offsets, tile):
    c = iota((COLS_TILE, VOXELS), 0).astype(jnp.float32)
    pieces = []
    for v in range(VIEWS):
        u = u_ref[v, pl.ds(tile, 1), :] - offsets[v].astype(jnp.float32)
        pieces.append(jnp.maximum(0.0, 1.0 - jnp.abs(u - c)))
    pieces.insert(3, jnp.zeros((8, VOXELS), jnp.float32))
    return jnp.concatenate(pieces, axis=0).astype(jnp.bfloat16)


def forward(w_ref, slices, acc_ref, m_ref, table_ref, out_ref, subset, gz):
    acc_ref[...] = jnp.zeros_like(acc_ref)
    for tile in range(TILES):
        offsets = tile_offsets(table_ref, subset, tile)
        part = lax.dot_general(
            w_ref[tile],
            jnp.concatenate([slices(tile)] * 4, axis=0),
            (((1,), (1,)), ((), ())),
            preferred_element_type=jnp.float32,
        )
        for v in range(VIEWS):
            acc_ref[v, pl.ds(offsets[v], COLS_TILE), :] += part[PLACE[v] : PLACE[v] + COLS_TILE]
    per = ROWS_PER[subset]
    half = per + 1
    size = GROUPS * 2 * half
    k = iota((size, 128), 0)
    lane = iota((size, 128), 1)
    i = lane & (Z_PAD - 1)
    group = (k * 43) >> 9 if half == 6 else (k * 205) >> 11
    slot = k - group * 2 * half
    is_low = slot < half
    slot = jnp.where(is_low, slot, slot - half)
    rows = slot_weights(group, slot, i, gz, subset)
    rows = jnp.where((slot == per) & (i == ONES), 1.0, rows)
    rounded = rows.astype(jnp.bfloat16).astype(jnp.float32)
    rows = jnp.where(lane < 2 * Z_PAD, rounded, rows - rounded).astype(jnp.bfloat16)
    left_over = (iota((WIN, 128), 1) & Z_PAD) != 0
    used = GROUPS * VIEWS * 2 * half
    out_ref[used:, :] = jnp.zeros((out_ref.shape[0] - used, 128), jnp.float32)
    for v in range(VIEWS):
        sums = acc_ref[v]
        rounded = sums.astype(jnp.bfloat16).astype(jnp.float32)
        sums = jnp.where(left_over, sums - rounded, rounded).astype(jnp.bfloat16)
        sums = lax.dot_general(
            rows, sums, (((1,), (1,)), ((), ())), preferred_element_type=jnp.float32
        )
        high = jnp.concatenate(
            (sums[:, 128:WIN], jnp.zeros((size, LANES - WIN), jnp.float32)), axis=1
        )
        part = jnp.where(is_low, sums[:, 0:128], high) + m_ref[v, 0:size, :]
        out_ref[v * size : (v + 1) * size, :] = part


def smear(recv_ref, sm_ref, gz):
    i = iota((Z_PAD, GROUPS * 8), 0)
    k = iota((Z_PAD, GROUPS * 8), 1)
    rows = slot_weights(k >> 3, k & 7, i, gz, 0)
    ones = iota((Z_PAD, LANES), 0) == ONES
    for v in range(VIEWS):
        got = recv_ref[v * GROUPS : (v + 1) * GROUPS]
        got = got.astype(jnp.float32).reshape(GROUPS * 8, LANES)
        smeared = jnp.dot(
            rows, got, precision=lax.Precision.HIGHEST, preferred_element_type=jnp.float32
        )
        sm_ref[v] = jnp.where(ones, 1.0, smeared).astype(jnp.bfloat16).astype(jnp.float32)


def smear_last(recv_ref, sm_ref, res_ref, gz):
    size = 2 * Z_PAD + 24
    i = iota((size, GROUPS * 8), 0)
    k = iota((size, GROUPS * 8), 1)
    part = k & 7
    rows = slot_weights(k >> 3, part & 3, i & (Z_PAD - 1), gz, 1)
    rows = jnp.where((part >= 4) == (i >= Z_PAD), rows, 0.0)
    j = i - 2 * Z_PAD + ((gz + 1) >> 1)
    picked = (k == ((j >> 2) << 3) + 4 + (j & 3)).astype(jnp.float32)
    rows = jnp.where(i >= 2 * Z_PAD, picked, rows)
    ones = iota((Z_PAD, LANES), 0) == ONES
    part = iota((GROUPS * 8, 128), 0) & 7
    exact = (part >= 4) & (iota((GROUPS * 8, 128), 1) >= MEAS_AT - 128)
    for v in range(VIEWS):
        got = recv_ref[v * GROUPS * 8 : (v + 1) * GROUPS * 8, :]
        got = jnp.where(exact, got, got.astype(jnp.bfloat16).astype(jnp.float32))
        sums = jnp.dot(
            rows, got, precision=lax.Precision.HIGHEST, preferred_element_type=jnp.float32
        )
        smeared = jnp.concatenate((sums[0:Z_PAD], sums[Z_PAD : 2 * Z_PAD]), axis=1)
        sm_ref[v] = jnp.where(ones, 1.0, smeared).astype(jnp.bfloat16).astype(jnp.float32)
        own = pltpu.roll(sums[2 * Z_PAD :], 256 - MEAS_AT, 1)
        res_ref[v] = own[0:ROWS_DEV, 0:COLS_DEV]


def windows(sm_ref, offsets):
    lane = iota((Z_PAD, 128), 1)
    placed = []
    for v in range(VIEWS):
        at = PLACE[v] & 127
        shift = (at - offsets[v]) & 127
        low = pltpu.roll(sm_ref[v, :, 0:128], shift, 1)
        high = pltpu.roll(sm_ref[v, :, 128:256], shift, 1)
        placed.append(jnp.where(lane < at + 128 - offsets[v], low, high))
    first = jnp.where(lane < 40, placed[0], jnp.where(lane < 80, placed[1], placed[2]))
    first = jnp.where(lane < 120, first, 0.0)
    second = jnp.where(lane < 40, placed[3], jnp.where(lane < 80, placed[4], 0.0))
    both = jnp.concatenate((first, second), axis=1)
    return both.astype(jnp.bfloat16)[:, 0:DEPTH]


def backward(w_ref, sm_ref, table_ref, old, store, subset, gz):
    zi = slice_of(iota((Z_PAD, LANES), 0), gz)
    inside = iota((Z_PAD, LANES), 0) < Z_ALL
    total = jnp.sum(jnp.where(inside, hat(iota((Z_PAD, LANES), 1), zi), 0.0), axis=1, keepdims=True)

    for tile in range(TILES):
        offsets = tile_offsets(table_ref, subset, tile)
        back = jnp.dot(
            windows(sm_ref, offsets), w_ref[tile], preferred_element_type=jnp.float32
        )
        norm = total * back[ONES : ONES + 1, :]
        store(tile, old(tile), back / jnp.maximum(norm, 1.0))


def swap_blocks(rows):
    block = iota((8, 128), 1) >> 4
    for d in (4, 2, 1):
        high = (block & d) != 0
        new = list(rows)
        for i in range(8):
            if i & d == 0:
                a, b = (rows[i], rows[i + d])
                new[i] = jnp.where(high, pltpu.roll(b, 16 * d, 1), a)
                new[i + d] = jnp.where(high, b, pltpu.roll(a, 128 - 16 * d, 1))
        rows = new
    return rows


def relay(source_ref, out_ref, pitch):
    def step(xb, nothing):
        for half in range(2):
            for b in range(2):
                at = xb * TILE + half * 8 + b * 8 * pitch
                rows = [source_ref[pl.ds(at + i, 8, stride=pitch), :] for i in range(8)]
                for q, block in enumerate(swap_blocks(rows)):
                    out_ref[
                        xb * TILES_Y + q, b * 8 : b * 8 + 8, half * 128 : half * 128 + 128
                    ] = block
        return nothing

    lax.fori_loop(0, X_DEV // TILE, step, 0)


def pack_kernel(
    vol_hbm, meas_hbm, up_ref, down_ref, vol_ref, meas_ref, row_ref, sems
):
    copies = [
        pltpu.make_async_copy(vol_hbm, vol_ref, sems.at[0]),
        pltpu.make_async_copy(meas_hbm, meas_ref, sems.at[1]),
    ]
    for copy in copies:
        copy.start()
    row_ref[...] = jnp.zeros_like(row_ref)
    for copy in copies:
        copy.wait()
    for out_ref, z, inner, r in (
        (up_ref, Z_DEV - Z_HALO, Z_HALO // 2, ROWS_DEV - M_HALO),
        (down_ref, 0, 0, 0),
    ):
        slices = vol_ref[z * X_DEV : (z + Z_HALO) * X_DEV, :]
        rounded = slices.astype(jnp.bfloat16)
        out_ref[0:HALO_ROWS, :] = rounded
        left = slices - rounded.astype(jnp.float32)
        at = inner * X_DEV
        out_ref[HALO_ROWS:EDGE_AT, :] = left[at : at + INNER_ROWS].astype(jnp.bfloat16)
        for v in range(VIEWS):
            at = (v * ROWS_DEV + r) * SUBSETS
            row_ref[:, 0:COLS_DEV] = meas_ref[at : at + SUBSETS * M_HALO, :]
            row = row_ref[...]
            rounded = row.astype(jnp.bfloat16).astype(jnp.float32)
            both = pltpu.roll(rounded, MEAS_AT - 128, 1)
            both = both + pltpu.roll(row - rounded, MEAS_AT - 128 - COLS_DEV, 1)
            at = EDGE_AT + v * SUBSETS * M_HALO
            out_ref[at : at + SUBSETS * M_HALO, :] = both.astype(jnp.bfloat16)


def prepare_kernel(
    cosine_ref, sine_ref, vol_ref, meas_ref,
    w0_ref, w1_ref, own_ref, mown_ref, flat_ref, table_ref, sem, u_ref,
):
    xy = lax.axis_index("xy")
    cosine = cosine_ref[...]
    sine = sine_ref[...]
    flat_ref[...], own = fill_table(cosine, sine, xy)
    copy = pltpu.make_async_copy(flat_ref, table_ref, sem)
    copy.start()
    relay(vol_ref, own_ref, X_DEV)
    mown_ref[...] = jnp.zeros_like(mown_ref)
    for s in range(SUBSETS):
        for v in range(VIEWS):
            for at, count in ((0, 8), (8, 8), (16, 4)):
                rows = meas_ref[pl.ds((v * ROWS_DEV + at) * 2 + s, count, stride=2), :]
                mown_ref[s, v, at : at + count, MEAS_AT - 128 : 128] = rows
    copy.wait()
    for subset, w_ref in ((0, w0_ref), (1, w1_ref)):
        positions(u_ref, cosine, sine, own, subset, xy)

        def step(tt, nothing):
            for t in range(8):
                tile = tt * 8 + t
                w_ref[tile] = weights(u_ref, tile_offsets(table_ref, subset, tile), tile)
            return nothing

        lax.fori_loop(0, TILES // 8, step, 0)


def first_kernel(
    flat_ref, w_ref, own_ref, mown_ref, low_ref, high_ref,
    out_ref, side_ref, m1_ref, table_ref, sem, halo_ref, acc_ref, raw_ref, m0_ref, edge_ref,
):
    gz = lax.axis_index("gz")
    copy = pltpu.make_async_copy(flat_ref, table_ref, sem)
    copy.start()
    for side, (sent_ref, inner) in enumerate(((low_ref, Z_HALO // 2), (high_ref, 0))):
        left_at = HALO_ROWS - inner * X_DEV
        for z in range(Z_HALO):
            at = z * X_DEV
            rows = sent_ref[at : at + X_DEV, :].astype(jnp.float32)
            if inner <= z < inner + Z_HALO // 2:
                rows = rows + sent_ref[left_at + at : left_at + at + X_DEV, :].astype(jnp.float32)
            at = (side * Z_HALO + z) * PITCH
            halo_ref[at : at + X_DEV, :] = rows
        edge = sent_ref[EDGE_AT:SENT_ROWS, :].astype(jnp.float32)
        edge = edge + pltpu.roll(edge, COLS_DEV, 1)
        edge_ref[side] = jnp.where(iota(edge.shape, 1) >= MEAS_AT - 128, edge, 0.0)
    for z in range(2 * Z_HALO, Z_DEV):
        value = 1.0 if z == ONES - Z_DEV else 0.0
        halo_ref[z * PITCH : z * PITCH + X_DEV, :] = jnp.full((X_DEV, NY), value, jnp.float32)
    relay(halo_ref, side_ref, PITCH)
    for s, m_ref in ((0, m0_ref), (1, m1_ref)):
        per = ROWS_PER[s]
        m_ref[...] = jnp.zeros_like(m_ref)
        for v in range(VIEWS):
            edge = pl.ds(v * 2 * M_HALO + s, M_HALO, stride=2)
            high = edge_ref[1, edge, :]
            joined = jnp.concatenate(
                (
                    edge_ref[0, edge, :],
                    mown_ref[s, v, 0:16, :],
                    jnp.concatenate((mown_ref[s, v, 16:20, :], high[0:4]), axis=0),
                    jnp.concatenate((high[4:8], jnp.zeros((4, 128), jnp.float32)), axis=0),
                ),
                axis=0,
            )
            raw_ref[s, v] = pltpu.roll(
                joined, M_ROWS + ((gz + 1) >> 1) - (M_HALO - ROWS_BELOW[s]), 0
            )
            for group in range(GROUPS):
                at = group * 2 * (per + 1) + per + 1
                m_ref[v, at : at + per, :] = raw_ref[s, v, group * per : (group + 1) * per, :]

    def slices(tile):
        return jnp.concatenate((own_ref[tile], side_ref[tile]), axis=0).astype(jnp.bfloat16)

    copy.wait()
    forward(w_ref, slices, acc_ref, m0_ref, table_ref, out_ref, 0, gz)


def middle_kernel(
    flat_ref, recv_ref, own_ref, side_ref, m_ref, w0_ref, w1_ref,
    out_ref, new_ref, table_ref, sem, sm_ref, vb_ref, acc_ref,
):
    gz = lax.axis_index("gz")
    copy = pltpu.make_async_copy(flat_ref, table_ref, sem)
    copy.start()
    smear(recv_ref, sm_ref, gz)
    copy.wait()
    ones = iota((Z_PAD, VOXELS), 0) == ONES

    def old(tile):
        return jnp.concatenate((own_ref[tile], side_ref[tile]), axis=0)

    def store(tile, old, change):
        new = jnp.where(ones, 1.0, old + change)
        new_ref[tile] = new[0:Z_DEV]
        vb_ref[tile] = new.astype(jnp.bfloat16)

    backward(w0_ref, sm_ref, table_ref, old, store, 0, gz)
    forward(w1_ref, lambda tile: vb_ref[tile], acc_ref, m_ref, table_ref, out_ref, 1, gz)


def last_kernel(
    flat_ref, recv_ref, old_ref, w_ref,
    out_ref, res_ref, table_ref, sem, sm_ref, new_ref, block_ref, sems,
):
    gz = lax.axis_index("gz")
    copy = pltpu.make_async_copy(flat_ref, table_ref, sem)
    copy.start()
    smear_last(recv_ref, sm_ref, res_ref, gz)
    copy.wait()

    def store(tile, old, change):
        new_ref[tile] = old + change[0:Z_DEV]

    backward(w_ref, sm_ref, table_ref, lambda tile: old_ref[tile], store, 1, gz)
    copies = []
    for xb in range(X_DEV // TILE):
        for half in range(2):
            for b in range(Z_DEV // 8):
                blocks = [
                    new_ref[xb * TILES_Y + q, b * 8 : b * 8 + 8, half * 128 : half * 128 + 128]
                    for q in range(TILES_Y)
                ]
                at = half * 8 + b * 8 * OUT_PITCH
                for i, row in enumerate(swap_blocks(blocks)):
                    block_ref[xb, pl.ds(at + i, 8, stride=OUT_PITCH), :] = row
        copies.append(
            pltpu.make_async_copy(
                block_ref.at[xb].reshape(Z_DEV, OUT_PITCH, NY).at[:, 0:TILE, :],
                out_ref.at[:, pl.ds(xb * TILE, TILE), :],
                sems.at[xb],
            )
        )
        copies[-1].start()
    for copy in copies:
        copy.wait()


def owner_kernel(flat_ref, recv_ref, out_ref, table_ref, sem, acc_ref, sum_ref, mea_ref, *, subset):
    gz = lax.axis_index("gz")
    xy = lax.axis_index("xy")
    copy = pltpu.make_async_copy(flat_ref, table_ref, sem)
    copy.start()
    view = jnp.minimum(xy // GROUPS, VIEWS - 1)
    group = xy % GROUPS
    at = subset * VIEWS + view
    per = ROWS_PER[subset]
    half = per + 1
    lane = iota((8, 128), 1)
    sum_ref[...] = jnp.zeros_like(sum_ref)
    mea_ref[...] = jnp.zeros_like(mea_ref)
    end = N_XY * 2 * half - 8

    def upper(s):
        row = s * 2 * half + half
        last = recv_ref[min(row, end) : min(row, end) + 8, :]
        return pltpu.roll(last, 8 - (row - end), 0) if row > end else last

    for s in range(N_XY):
        column = s * COLS_DEV
        own = jnp.where(lane >= MEAS_AT - 128, upper(s), 0.0)
        own = pltpu.roll(own, (column + 256 - MEAS_AT) % 128, 1)
        block = column // 128 * 128
        offset = column - block
        mea_ref[:, block : block + 128] += jnp.where(lane >= offset, own, 0.0)
        if offset + COLS_DEV > 128:
            mea_ref[:, block + 128 : block + 256] += jnp.where(lane < offset, own, 0.0)
    copy.wait()
    for s in range(N_XY):
        base = pl.multiple_of(table_ref[at, s], 128)
        shift = table_ref[at, SHIFT_AT + s]
        row = s * 2 * half
        low = pltpu.roll(recv_ref[row : row + 8, :], shift, 1)
        high = pltpu.roll(jnp.where(lane < WIN - 128, upper(s), 0.0), shift, 1)
        wrapped = lane < shift
        part_ref = sum_ref.at[s % SUMS]
        part_ref[:, pl.ds(base, 128)] += jnp.where(wrapped, 0.0, low)
        part_ref[:, pl.ds(base + 128, 128)] += jnp.where(wrapped, low, high)
        part_ref[:, pl.ds(base + 256, 128)] += jnp.where(wrapped, high, 0.0)
    slot = iota((8, NZ), 0)
    row = first_row(gz, subset) + group * per + slot
    ray_rows = jnp.where(slot < per, hat(row, iota((8, NZ), 1)), 0.0)
    ray_rows = jnp.sum(ray_rows, axis=1, keepdims=True)
    sums = sum_ref[0]
    for part in range(1, SUMS):
        sums = sums + sum_ref[part]
    totals = sums[per : per + 1, :]
    acc_ref[...] = mea_ref[...] - sums / jnp.maximum(ray_rows * totals, 1.0)
    for t in range(N_XY):
        base = pl.multiple_of(table_ref[at, t], 128)
        shift = table_ref[at, SHIFT_AT + t]
        back = (128 - shift) & 127
        a = pltpu.roll(acc_ref[:, pl.ds(base, 128)], back, 1)
        b = pltpu.roll(acc_ref[:, pl.ds(base + 128, 128)], back, 1)
        c = pltpu.roll(acc_ref[:, pl.ds(base + 256, 128)], back, 1)
        kept = lane < 128 - shift
        low = jnp.where(kept, a, b)
        high = jnp.where(kept, b, c)
        if subset == 0:
            out_ref[t, :, 0:128] = low.astype(jnp.bfloat16)
            out_ref[t, :, 128:256] = high.astype(jnp.bfloat16)
            continue
        column = t * COLS_DEV
        block = column // 128 * 128
        offset = column - block
        turn = (MEAS_AT - 128 - offset) % 128
        own = pltpu.roll(acc_ref[:, block : block + 128], turn, 1)
        if offset + COLS_DEV > 128:
            more = pltpu.roll(acc_ref[:, block + 128 : block + 256], turn, 1)
            own = jnp.where(lane < MEAS_AT - offset, own, more)
        high = jnp.where(lane >= MEAS_AT - 128, own, high)
        out_ref[t * 8 : (t + 1) * 8, :] = jnp.where(slot < 4, low, pltpu.roll(high, 4, 0))


def call(kernel, inputs, outs, scratch, name):
    vmem = pl.BlockSpec(memory_space=pltpu.VMEM)
    anywhere = pl.BlockSpec(memory_space=pl.ANY)
    inputs = [pltpu.with_memory_space_constraint(x, pltpu.VMEM) for x in inputs]
    scratch = [pltpu.SMEM(TABLE, jnp.int32), pltpu.SemaphoreType.DMA, *scratch]
    return pl.pallas_call(
        kernel,
        in_specs=[vmem] * len(inputs),
        out_specs=[anywhere if out.shape == VOLUME else vmem for out in outs],
        out_shape=outs,
        scratch_shapes=scratch,
        compiler_params=pltpu.CompilerParams(vmem_limit_bytes=12 * 1024 * 1024),
        name=name,
    )(*inputs)


def exchanged(parts, shape):
    sent = lax.all_to_all(
        parts.reshape(shape), "xy", split_axis=0, concat_axis=0, tiled=True
    )
    return sent.reshape(parts.shape)


def local(volume, measured, view_order):
    f32 = jnp.float32
    bf16 = jnp.bfloat16
    vmem = pltpu.VMEM
    angles = 2.0 * math.pi * view_order[: SUBSETS * VIEWS].astype(f32) / ANGLES
    angles = jnp.broadcast_to(jnp.pad(angles, (0, TABLE[0] - SUBSETS * VIEWS))[:, None], TABLE)
    flat = volume.reshape(Z_DEV * X_DEV, NY)
    rows = measured.transpose(1, 2, 0, 3).reshape(VIEWS * ROWS_DEV * SUBSETS, COLS_DEV)
    made = vmem((TILES, DEPTH, VOXELS), bf16)
    slices = vmem((TILES, Z_DEV, VOXELS), f32)
    sm_scratch = vmem((VIEWS, Z_PAD, LANES), f32)
    acc_scratch = vmem((VIEWS, WIN, 128), f32)
    row_scratch = vmem((8, FULL), f32)
    owner_scratch = [row_scratch, vmem((SUMS, 8, FULL), f32), row_scratch]

    sent = vmem((SENT_ROWS, 128), bf16)
    up, down, flat, rows = pl.pallas_call(
        pack_kernel,
        in_specs=[pl.BlockSpec(memory_space=pl.ANY)] * 2,
        out_specs=[pl.BlockSpec(memory_space=vmem)] * 4,
        out_shape=[sent, sent, vmem(flat.shape, f32), vmem(rows.shape, f32)],
        scratch_shapes=[vmem((SUBSETS * M_HALO, 128), f32), pltpu.SemaphoreType.DMA((2,))],
        compiler_params=pltpu.CompilerParams(vmem_limit_bytes=12 * 1024 * 1024),
        name="pack",
    )(flat, rows)
    next_up = [(i, (i + 1) % N_GZ) for i in range(N_GZ)]
    low = lax.ppermute(up, "gz", next_up)
    high = lax.ppermute(down, "gz", [(j, i) for i, j in next_up])
    w0, w1, own, mown, table = call(
        prepare_kernel,
        (jnp.cos(angles), jnp.sin(angles), flat, rows),
        [made, made, slices, vmem((SUBSETS, VIEWS, 24, 128), f32), vmem(TABLE, jnp.int32)],
        [vmem((VIEWS, TILES, VOXELS), f32)],
        "prepare",
    )
    partial, side, m1 = call(
        first_kernel,
        (table, w0, own, mown, low, high),
        [vmem((N_XY * 12, 128), f32), slices, vmem((VIEWS, 64, 128), f32)],
        [
            vmem((Z_DEV * PITCH, NY), f32),
            acc_scratch,
            vmem((SUBSETS, VIEWS, M_ROWS, 128), f32),
            vmem((VIEWS, 72, 128), f32),
            vmem((2, EDGE_ROWS, 128), f32),
        ],
        "first",
    )
    (rounded,) = call(
        functools.partial(owner_kernel, subset=0),
        (table, exchanged(partial, (N_XY, 3, 4, 128))),
        [vmem((N_XY, 8, LANES), bf16)],
        owner_scratch,
        "owner_a",
    )
    partial, new = call(
        middle_kernel,
        (table, exchanged(rounded, rounded.shape), own, side, m1, w0, w1),
        [vmem((N_XY * 10, 128), f32), slices],
        [sm_scratch, vmem((TILES, Z_PAD, VOXELS), bf16), acc_scratch],
        "middle",
    )
    (final,) = call(
        functools.partial(owner_kernel, subset=1),
        (table, exchanged(partial, (N_XY, 5, 2, 128))),
        [vmem((N_XY * 8, 128), f32)],
        owner_scratch,
        "owner_b",
    )
    volume_out, residual = call(
        last_kernel,
        (table, exchanged(final, (N_XY, 8, 128)), new, w1),
        [
            jax.ShapeDtypeStruct(VOLUME, f32),
            jax.ShapeDtypeStruct((VIEWS, ROWS_DEV, COLS_DEV), f32),
        ],
        [
            sm_scratch,
            slices,
            vmem((X_DEV // TILE, Z_DEV * OUT_PITCH, NY), f32),
            pltpu.SemaphoreType.DMA((X_DEV // TILE,)),
        ],
        "last",
    )
    return volume_out, residual


def solution(mesh):
    in_specs = (P("gz", "xy", None), P(None, None, "gz", "xy"), P())
    out_specs = (P("gz", "xy", None), P(None, "gz", "xy"))
    return jax.shard_map(local, mesh=mesh, in_specs=in_specs, out_specs=out_specs, check_vma=False)
```

```python
import functools
import math

import jax
import jax.numpy as jnp
from jax import lax
from jax.experimental import pallas as pl
from jax.experimental.pallas import tpu as pltpu
from jax.sharding import PartitionSpec as P

Z_DEV = 16
X_DEV = 48
NY = 128
COLS_DEV = 48
ROWS_DEV = 20
VIEWS = 5
SUBSETS = 2
ANGLES = 48
N_XY = 32
N_GZ = 8
NX = X_DEV * N_XY
NZ = Z_DEV * N_GZ
DR = ROWS_DEV * N_GZ
DC = COLS_DEV * N_XY

WIN = 176
LANES = 256
MEAS_AT = LANES - COLS_DEV
Z_HALO = 6
Z_ALL = Z_DEV + 2 * Z_HALO
ONES = Z_ALL
Z_PAD = 32
GROUPS = 6
ROWS_PER = (5, 4)
ROWS_BELOW = (3, 0)
M_HALO = 8
M_ROWS = 40
FULL = 15 * 128
SUMS = 4
TILE = 16
TILES_Y = NY // TILE
TILES = X_DEV // TILE * TILES_Y
VOXELS = TILE * TILE
COLS_TILE = 40
VOLUME = (Z_DEV, X_DEV, NY)
PLACE = (0, 40, 80, 128, 168)
DEPTH = 208
HALO_ROWS = Z_HALO * X_DEV
INNER_ROWS = HALO_ROWS // 2
EDGE_AT = HALO_ROWS + INNER_ROWS
EDGE_ROWS = SUBSETS * VIEWS * M_HALO
SENT_ROWS = EDGE_AT + EDGE_ROWS
PITCH = 56
OUT_PITCH = 24
TABLE = (16, 128)
SHIFT_AT = 32
TILE_AT = 64


def iota(shape, dim):
    return lax.broadcasted_iota(jnp.int32, shape, dim)


def slice_of(i, gz):
    low = Z_DEV * gz - Z_HALO + (i - Z_DEV)
    high = Z_DEV * gz + Z_DEV + (i - Z_DEV - Z_HALO)
    return jnp.where(i < Z_DEV, Z_DEV * gz + i, jnp.where(i < Z_DEV + Z_HALO, low, high))


def hat(row, z):
    position = (DR - 1) / 2.0 + 0.96 * (DR / NZ) * (z.astype(jnp.float32) - (NZ - 1) / 2.0)
    value = jnp.maximum(0.0, 1.0 - jnp.abs(position - row.astype(jnp.float32)) / 2.0)
    ok = (row >= 0) & (row < DR) & (z >= 0) & (z < NZ)
    return jnp.where(ok, value, 0.0)


def first_row(gz, subset):
    return ROWS_DEV * gz - ROWS_BELOW[subset] - ((gz + 1) >> 1)


def slot_weights(group, slot, i, gz, subset):
    per = ROWS_PER[subset]
    row = first_row(gz, subset) + group * per + slot
    return jnp.where((slot < per) & (i < Z_ALL), hat(row, slice_of(i, gz)), 0.0)


def tile_offsets(table_ref, subset, tile):
    return [
        pl.multiple_of(table_ref[subset * VIEWS + v, TILE_AT + tile], 8) for v in range(VIEWS)
    ]


def coordinate(x, y, cosine, sine):
    xc = x - (NX - 1) / 2.0
    yc = y - (NY - 1) / 2.0
    source = 2.0 * NX
    along = xc * cosine + yc * sine
    depth = yc * cosine - xc * sine
    return (DC - 1) / 2.0 + 0.9 * (DC / NX) * along * source / (source + depth)


def fill_table(cosine, sine, xy):
    lane = iota(TABLE, 1)
    tile = lane - TILE_AT
    is_tile = lane >= TILE_AT
    strip = lane & (N_XY - 1)
    x = jnp.where(is_tile, xy * X_DEV + (tile >> 3) * TILE, strip * X_DEV).astype(jnp.float32)
    y = jnp.where(is_tile, (tile & 7) * TILE, 0).astype(jnp.float32)
    dx = jnp.where(is_tile, TILE - 1.0, X_DEV - 1.0)
    dy = jnp.where(is_tile, TILE - 1.0, NY - 1.0)
    least = jnp.minimum(
        jnp.minimum(coordinate(x, y, cosine, sine), coordinate(x + dx, y, cosine, sine)),
        jnp.minimum(coordinate(x, y + dy, cosine, sine), coordinate(x + dx, y + dy, cosine, sine)),
    )
    least = jnp.floor(least).astype(jnp.int32)
    start = least - 2
    own = jnp.sum(jnp.where(lane == xy, start, 0).astype(jnp.float32), axis=1, keepdims=True)
    tiles = jnp.maximum(least - 1 - own.astype(jnp.int32), 0) & ~7
    table = jnp.where(lane < SHIFT_AT, start & ~127, start & 127)
    return jnp.where(is_tile, tiles, table), own


def positions(u_ref, cosine, sine, own, subset, xy):
    t = iota((TILES, VOXELS), 0)
    l = iota((TILES, VOXELS), 1)
    x = ((t >> 3) * TILE + (l >> 4) + xy * X_DEV).astype(jnp.float32)
    y = ((t & 7) * TILE + (l & 15)).astype(jnp.float32)
    for v in range(VIEWS):
        at = subset * VIEWS + v
        u = coordinate(x, y, cosine[at : at + 1, 0:1], sine[at : at + 1, 0:1])
        u_ref[v] = u - own[at : at + 1, :]


def weights(u_ref, offsets, tile):
    c = iota((COLS_TILE, VOXELS), 0).astype(jnp.float32)
    pieces = []
    for v in range(VIEWS):
        u = u_ref[v, pl.ds(tile, 1), :] - offsets[v].astype(jnp.float32)
        pieces.append(jnp.maximum(0.0, 1.0 - jnp.abs(u - c)))
    pieces.insert(3, jnp.zeros((8, VOXELS), jnp.float32))
    return jnp.concatenate(pieces, axis=0).astype(jnp.bfloat16)


def forward(w_ref, slices, acc_ref, m_ref, table_ref, out_ref, subset, gz):
    acc_ref[...] = jnp.zeros_like(acc_ref)
    for tile in range(TILES):
        offsets = tile_offsets(table_ref, subset, tile)
        part = lax.dot_general(
            w_ref[tile],
            jnp.concatenate([slices(tile)] * 4, axis=0),
            (((1,), (1,)), ((), ())),
            preferred_element_type=jnp.float32,
        )
        for v in range(VIEWS):
            acc_ref[v, pl.ds(offsets[v], COLS_TILE), :] += part[PLACE[v] : PLACE[v] + COLS_TILE]
    per = ROWS_PER[subset]
    half = per + 1
    size = GROUPS * 2 * half
    k = iota((size, 128), 0)
    lane = iota((size, 128), 1)
    i = lane & (Z_PAD - 1)
    group = (k * 43) >> 9 if half == 6 else (k * 205) >> 11
    slot = k - group * 2 * half
    is_low = slot < half
    slot = jnp.where(is_low, slot, slot - half)
    rows = slot_weights(group, slot, i, gz, subset)
    rows = jnp.where((slot == per) & (i == ONES), 1.0, rows)
    rounded = rows.astype(jnp.bfloat16).astype(jnp.float32)
    rows = jnp.where(lane < 2 * Z_PAD, rounded, rows - rounded).astype(jnp.bfloat16)
    left_over = (iota((WIN, 128), 1) & Z_PAD) != 0
    used = GROUPS * VIEWS * 2 * half
    out_ref[used:, :] = jnp.zeros((out_ref.shape[0] - used, 128), jnp.float32)
    for v in range(VIEWS):
        sums = acc_ref[v]
        rounded = sums.astype(jnp.bfloat16).astype(jnp.float32)
        sums = jnp.where(left_over, sums - rounded, rounded).astype(jnp.bfloat16)
        sums = lax.dot_general(
            rows, sums, (((1,), (1,)), ((), ())), preferred_element_type=jnp.float32
        )
        high = jnp.concatenate(
            (sums[:, 128:WIN], jnp.zeros((size, LANES - WIN), jnp.float32)), axis=1
        )
        part = jnp.where(is_low, sums[:, 0:128], high) + m_ref[v, 0:size, :]
        out_ref[v * size : (v + 1) * size, :] = part


def smear(recv_ref, sm_ref, gz):
    i = iota((3 * Z_PAD, GROUPS * 8), 0)
    k = iota((3 * Z_PAD, GROUPS * 8), 1)
    part = k & 7
    third = i >> 5
    slot = jnp.where(third == 0, part, 2 * (part - 5) + third - 1)
    rows = slot_weights(k >> 3, slot, i & (Z_PAD - 1), gz, 0)
    rows = jnp.where((third == 0) == (part < 5), rows, 0.0)
    ones = iota((Z_PAD, LANES), 0) == ONES
    for v in range(VIEWS):
        got = recv_ref[v * GROUPS : (v + 1) * GROUPS]
        got = got.astype(jnp.float32).reshape(GROUPS * 8, 128)
        sums = jnp.dot(
            rows, got, precision=lax.Precision.HIGHEST, preferred_element_type=jnp.float32
        )
        high = sums[Z_PAD : 2 * Z_PAD] + pltpu.roll(sums[2 * Z_PAD :], 128 - COLS_DEV, 1)
        smeared = jnp.concatenate((sums[0:Z_PAD], high), axis=1)
        sm_ref[v] = jnp.where(ones, 1.0, smeared).astype(jnp.bfloat16).astype(jnp.float32)


def smear_last(recv_ref, sm_ref, res_ref, gz):
    size = 2 * Z_PAD + 24
    i = iota((size, GROUPS * 8), 0)
    k = iota((size, GROUPS * 8), 1)
    part = k & 7
    rows = slot_weights(k >> 3, part & 3, i & (Z_PAD - 1), gz, 1)
    rows = jnp.where((part >= 4) == (i >= Z_PAD), rows, 0.0)
    j = i - 2 * Z_PAD + ((gz + 1) >> 1)
    picked = (k == ((j >> 2) << 3) + 4 + (j & 3)).astype(jnp.float32)
    rows = jnp.where(i >= 2 * Z_PAD, picked, rows)
    ones = iota((Z_PAD, LANES), 0) == ONES
    part = iota((GROUPS * 8, 128), 0) & 7
    exact = (part >= 4) & (iota((GROUPS * 8, 128), 1) >= MEAS_AT - 128)
    for v in range(VIEWS):
        got = recv_ref[v * GROUPS * 8 : (v + 1) * GROUPS * 8, :]
        got = jnp.where(exact, got, got.astype(jnp.bfloat16).astype(jnp.float32))
        sums = jnp.dot(
            rows, got, precision=lax.Precision.HIGHEST, preferred_element_type=jnp.float32
        )
        smeared = jnp.concatenate((sums[0:Z_PAD], sums[Z_PAD : 2 * Z_PAD]), axis=1)
        sm_ref[v] = jnp.where(ones, 1.0, smeared).astype(jnp.bfloat16).astype(jnp.float32)
        own = pltpu.roll(sums[2 * Z_PAD :], 256 - MEAS_AT, 1)
        res_ref[v] = own[0:ROWS_DEV, 0:COLS_DEV]


def windows(sm_ref, offsets):
    lane = iota((Z_PAD, 128), 1)
    placed = []
    for v in range(VIEWS):
        at = PLACE[v] & 127
        shift = (at - offsets[v]) & 127
        low = pltpu.roll(sm_ref[v, :, 0:128], shift, 1)
        high = pltpu.roll(sm_ref[v, :, 128:256], shift, 1)
        placed.append(jnp.where(lane < at + 128 - offsets[v], low, high))
    first = jnp.where(lane < 40, placed[0], jnp.where(lane < 80, placed[1], placed[2]))
    first = jnp.where(lane < 120, first, 0.0)
    second = jnp.where(lane < 40, placed[3], jnp.where(lane < 80, placed[4], 0.0))
    both = jnp.concatenate((first, second), axis=1)
    return both.astype(jnp.bfloat16)[:, 0:DEPTH]


def backward(w_ref, sm_ref, table_ref, old, store, subset, gz):
    zi = slice_of(iota((Z_PAD, LANES), 0), gz)
    inside = iota((Z_PAD, LANES), 0) < Z_ALL
    total = jnp.sum(jnp.where(inside, hat(iota((Z_PAD, LANES), 1), zi), 0.0), axis=1, keepdims=True)

    for tile in range(TILES):
        offsets = tile_offsets(table_ref, subset, tile)
        back = jnp.dot(
            windows(sm_ref, offsets), w_ref[tile], preferred_element_type=jnp.float32
        )
        norm = total * back[ONES : ONES + 1, :]
        store(tile, old(tile), back / jnp.maximum(norm, 1.0))


def swap_blocks(rows):
    block = iota((8, 128), 1) >> 4
    for d in (4, 2, 1):
        high = (block & d) != 0
        new = list(rows)
        for i in range(8):
            if i & d == 0:
                a, b = (rows[i], rows[i + d])
                new[i] = jnp.where(high, pltpu.roll(b, 16 * d, 1), a)
                new[i + d] = jnp.where(high, b, pltpu.roll(a, 128 - 16 * d, 1))
        rows = new
    return rows


def relay(source_ref, out_ref, pitch):
    def step(xb, nothing):
        for half in range(2):
            for b in range(2):
                at = xb * TILE + half * 8 + b * 8 * pitch
                rows = [source_ref[pl.ds(at + i, 8, stride=pitch), :] for i in range(8)]
                for q, block in enumerate(swap_blocks(rows)):
                    out_ref[
                        xb * TILES_Y + q, b * 8 : b * 8 + 8, half * 128 : half * 128 + 128
                    ] = block
        return nothing

    lax.fori_loop(0, X_DEV // TILE, step, 0)


def pack_kernel(
    vol_hbm, meas_hbm, order_hbm, up_ref, down_ref, vol_ref, meas_ref, order_ref, row_ref, sems
):
    copies = [
        pltpu.make_async_copy(vol_hbm, vol_ref, sems.at[0]),
        pltpu.make_async_copy(meas_hbm, meas_ref, sems.at[1]),
        pltpu.make_async_copy(order_hbm, order_ref, sems.at[2]),
    ]
    for copy in copies:
        copy.start()
    row_ref[...] = jnp.zeros_like(row_ref)
    for copy in copies:
        copy.wait()
    for out_ref, z, inner, r in (
        (up_ref, Z_DEV - Z_HALO, Z_HALO // 2, ROWS_DEV - M_HALO),
        (down_ref, 0, 0, 0),
    ):
        slices = vol_ref[z * X_DEV : (z + Z_HALO) * X_DEV, :]
        rounded = slices.astype(jnp.bfloat16)
        out_ref[0:HALO_ROWS, :] = rounded
        left = slices - rounded.astype(jnp.float32)
        at = inner * X_DEV
        out_ref[HALO_ROWS:EDGE_AT, :] = left[at : at + INNER_ROWS].astype(jnp.bfloat16)
        for v in range(VIEWS):
            at = (v * ROWS_DEV + r) * SUBSETS
            row_ref[:, 0:COLS_DEV] = meas_ref[at : at + SUBSETS * M_HALO, :]
            row = row_ref[...]
            rounded = row.astype(jnp.bfloat16).astype(jnp.float32)
            both = pltpu.roll(rounded, MEAS_AT - 128, 1)
            both = both + pltpu.roll(row - rounded, MEAS_AT - 128 - COLS_DEV, 1)
            at = EDGE_AT + v * SUBSETS * M_HALO
            out_ref[at : at + SUBSETS * M_HALO, :] = both.astype(jnp.bfloat16)


def prepare_kernel(
    order_ref, vol_ref, meas_ref,
    w0_ref, w1_ref, own_ref, mown_ref, table_ref, u_ref, flat_ref, sem,
):
    xy = lax.axis_index("xy")
    chosen = iota((TABLE[0], ANGLES), 0) == iota((TABLE[0], ANGLES), 1)
    chosen = jnp.where(chosen, order_ref[...].astype(jnp.float32), 0.0)
    chosen = jnp.broadcast_to(jnp.sum(chosen, axis=1, keepdims=True), TABLE)
    angles = 2.0 * math.pi * chosen / ANGLES
    cosine = jnp.cos(angles)
    sine = jnp.sin(angles)
    flat_ref[...], own = fill_table(cosine, sine, xy)
    copy = pltpu.make_async_copy(flat_ref, table_ref, sem)
    copy.start()
    relay(vol_ref, own_ref, X_DEV)
    mown_ref[...] = jnp.zeros_like(mown_ref)
    for s in range(SUBSETS):
        for v in range(VIEWS):
            for at, count in ((0, 8), (8, 8), (16, 4)):
                rows = meas_ref[pl.ds((v * ROWS_DEV + at) * 2 + s, count, stride=2), :]
                mown_ref[s, v, at : at + count, MEAS_AT - 128 : 128] = rows
    copy.wait()
    for subset, w_ref in ((0, w0_ref), (1, w1_ref)):
        positions(u_ref, cosine, sine, own, subset, xy)

        def step(tt, nothing):
            for t in range(8):
                tile = tt * 8 + t
                w_ref[tile] = weights(u_ref, tile_offsets(table_ref, subset, tile), tile)
            return nothing

        lax.fori_loop(0, TILES // 8, step, 0)


def first_kernel(
    table_ref, w_ref, own_ref, mown_ref, low_ref, high_ref,
    out_ref, side_ref, m1_ref, halo_ref, acc_ref, raw_ref, m0_ref, edge_ref,
):
    gz = lax.axis_index("gz")
    for side, (sent_ref, inner) in enumerate(((low_ref, Z_HALO // 2), (high_ref, 0))):
        left_at = HALO_ROWS - inner * X_DEV
        for z in range(Z_HALO):
            at = z * X_DEV
            rows = sent_ref[at : at + X_DEV, :].astype(jnp.float32)
            if inner <= z < inner + Z_HALO // 2:
                rows = rows + sent_ref[left_at + at : left_at + at + X_DEV, :].astype(jnp.float32)
            at = (side * Z_HALO + z) * PITCH
            halo_ref[at : at + X_DEV, :] = rows
        edge = sent_ref[EDGE_AT:SENT_ROWS, :].astype(jnp.float32)
        edge = edge + pltpu.roll(edge, COLS_DEV, 1)
        edge_ref[side] = jnp.where(iota(edge.shape, 1) >= MEAS_AT - 128, edge, 0.0)
    for z in range(2 * Z_HALO, Z_DEV):
        value = 1.0 if z == ONES - Z_DEV else 0.0
        halo_ref[z * PITCH : z * PITCH + X_DEV, :] = jnp.full((X_DEV, NY), value, jnp.float32)
    relay(halo_ref, side_ref, PITCH)
    for s, m_ref in ((0, m0_ref), (1, m1_ref)):
        per = ROWS_PER[s]
        m_ref[...] = jnp.zeros_like(m_ref)
        for v in range(VIEWS):
            edge = pl.ds(v * 2 * M_HALO + s, M_HALO, stride=2)
            high = edge_ref[1, edge, :]
            joined = jnp.concatenate(
                (
                    edge_ref[0, edge, :],
                    mown_ref[s, v, 0:16, :],
                    jnp.concatenate((mown_ref[s, v, 16:20, :], high[0:4]), axis=0),
                    jnp.concatenate((high[4:8], jnp.zeros((4, 128), jnp.float32)), axis=0),
                ),
                axis=0,
            )
            raw_ref[s, v] = pltpu.roll(
                joined, M_ROWS + ((gz + 1) >> 1) - (M_HALO - ROWS_BELOW[s]), 0
            )
            for group in range(GROUPS):
                at = group * 2 * (per + 1) + per + 1
                m_ref[v, at : at + per, :] = raw_ref[s, v, group * per : (group + 1) * per, :]

    def slices(tile):
        return jnp.concatenate((own_ref[tile], side_ref[tile]), axis=0).astype(jnp.bfloat16)

    forward(w_ref, slices, acc_ref, m0_ref, table_ref, out_ref, 0, gz)


def middle_kernel(
    table_ref, recv_ref, own_ref, side_ref, m_ref, w0_ref, w1_ref,
    out_ref, new_ref, sm_ref, vb_ref, acc_ref,
):
    gz = lax.axis_index("gz")
    smear(recv_ref, sm_ref, gz)
    ones = iota((Z_PAD, VOXELS), 0) == ONES

    def old(tile):
        return jnp.concatenate((own_ref[tile], side_ref[tile]), axis=0)

    def store(tile, old, change):
        new = jnp.where(ones, 1.0, old + change)
        new_ref[tile] = new[0:Z_DEV]
        vb_ref[tile] = new.astype(jnp.bfloat16)

    backward(w0_ref, sm_ref, table_ref, old, store, 0, gz)
    forward(w1_ref, lambda tile: vb_ref[tile], acc_ref, m_ref, table_ref, out_ref, 1, gz)


def last_kernel(
    table_ref, recv_ref, old_ref, w_ref,
    out_ref, res_ref, sm_ref, new_ref, block_ref, own_ref, sems,
):
    gz = lax.axis_index("gz")
    smear_last(recv_ref, sm_ref, own_ref, gz)
    copies = [pltpu.make_async_copy(own_ref, res_ref, sems.at[X_DEV // TILE])]
    copies[0].start()

    def store(tile, old, change):
        new_ref[tile] = old + change[0:Z_DEV]

    backward(w_ref, sm_ref, table_ref, lambda tile: old_ref[tile], store, 1, gz)
    for xb in range(X_DEV // TILE):
        for half in range(2):
            for b in range(Z_DEV // 8):
                blocks = [
                    new_ref[xb * TILES_Y + q, b * 8 : b * 8 + 8, half * 128 : half * 128 + 128]
                    for q in range(TILES_Y)
                ]
                at = half * 8 + b * 8 * OUT_PITCH
                for i, row in enumerate(swap_blocks(blocks)):
                    block_ref[xb, pl.ds(at + i, 8, stride=OUT_PITCH), :] = row
        copies.append(
            pltpu.make_async_copy(
                block_ref.at[xb].reshape(Z_DEV, OUT_PITCH, NY).at[:, 0:TILE, :],
                out_ref.at[:, pl.ds(xb * TILE, TILE), :],
                sems.at[xb],
            )
        )
        copies[-1].start()
    for copy in copies:
        copy.wait()


def owner_kernel(table_ref, recv_ref, out_ref, acc_ref, sum_ref, mea_ref, *, subset):
    gz = lax.axis_index("gz")
    xy = lax.axis_index("xy")
    view = jnp.minimum(xy // GROUPS, VIEWS - 1)
    group = xy % GROUPS
    at = subset * VIEWS + view
    per = ROWS_PER[subset]
    half = per + 1
    lane = iota((8, 128), 1)
    sum_ref[...] = jnp.zeros_like(sum_ref)
    mea_ref[...] = jnp.zeros_like(mea_ref)
    end = N_XY * 2 * half - 8

    def upper(s):
        row = s * 2 * half + half
        last = recv_ref[min(row, end) : min(row, end) + 8, :]
        return pltpu.roll(last, 8 - (row - end), 0) if row > end else last

    for s in range(N_XY):
        column = s * COLS_DEV
        own = jnp.where(lane >= MEAS_AT - 128, upper(s), 0.0)
        own = pltpu.roll(own, (column + 256 - MEAS_AT) % 128, 1)
        block = column // 128 * 128
        offset = column - block
        mea_ref[:, block : block + 128] += jnp.where(lane >= offset, own, 0.0)
        if offset + COLS_DEV > 128:
            mea_ref[:, block + 128 : block + 256] += jnp.where(lane < offset, own, 0.0)
    for s in range(N_XY):
        base = pl.multiple_of(table_ref[at, s], 128)
        shift = table_ref[at, SHIFT_AT + s]
        row = s * 2 * half
        low = pltpu.roll(recv_ref[row : row + 8, :], shift, 1)
        high = pltpu.roll(jnp.where(lane < WIN - 128, upper(s), 0.0), shift, 1)
        wrapped = lane < shift
        part_ref = sum_ref.at[s % SUMS]
        part_ref[:, pl.ds(base, 128)] += jnp.where(wrapped, 0.0, low)
        part_ref[:, pl.ds(base + 128, 128)] += jnp.where(wrapped, low, high)
        part_ref[:, pl.ds(base + 256, 128)] += jnp.where(wrapped, high, 0.0)
    slot = iota((8, NZ), 0)
    row = first_row(gz, subset) + group * per + slot
    ray_rows = jnp.where(slot < per, hat(row, iota((8, NZ), 1)), 0.0)
    ray_rows = jnp.sum(ray_rows, axis=1, keepdims=True)
    sums = sum_ref[0]
    for part in range(1, SUMS):
        sums = sums + sum_ref[part]
    totals = sums[per : per + 1, :]
    acc_ref[...] = mea_ref[...] - sums / jnp.maximum(ray_rows * totals, 1.0)
    for t in range(N_XY):
        base = pl.multiple_of(table_ref[at, t], 128)
        shift = table_ref[at, SHIFT_AT + t]
        back = (128 - shift) & 127
        a = pltpu.roll(acc_ref[:, pl.ds(base, 128)], back, 1)
        b = pltpu.roll(acc_ref[:, pl.ds(base + 128, 128)], back, 1)
        c = pltpu.roll(acc_ref[:, pl.ds(base + 256, 128)], back, 1)
        kept = lane < 128 - shift
        low = jnp.where(kept, a, b)
        high = jnp.where(kept, b, c)
        if subset == 0:
            other = pltpu.roll(high, COLS_DEV, 1)
            even = jnp.where(
                slot == 5,
                pltpu.roll(high, 5, 0),
                jnp.where(slot == 6, pltpu.roll(high, 4, 0), pltpu.roll(high, 3, 0)),
            )
            odd = jnp.where(slot == 5, pltpu.roll(other, 4, 0), pltpu.roll(other, 3, 0))
            rest = jnp.where(lane < COLS_DEV, even, odd)
            out_ref[t] = jnp.where(slot < 5, low, rest).astype(jnp.bfloat16)
            continue
        column = t * COLS_DEV
        block = column // 128 * 128
        offset = column - block
        turn = (MEAS_AT - 128 - offset) % 128
        own = pltpu.roll(acc_ref[:, block : block + 128], turn, 1)
        if offset + COLS_DEV > 128:
            more = pltpu.roll(acc_ref[:, block + 128 : block + 256], turn, 1)
            own = jnp.where(lane < MEAS_AT - offset, own, more)
        high = jnp.where(lane >= MEAS_AT - 128, own, high)
        out_ref[t * 8 : (t + 1) * 8, :] = jnp.where(slot < 4, low, pltpu.roll(high, 4, 0))


def call(kernel, inputs, outs, scratch, name):
    vmem = pl.BlockSpec(memory_space=pltpu.VMEM)
    smem = pl.BlockSpec(memory_space=pltpu.SMEM)
    anywhere = pl.BlockSpec(memory_space=pl.ANY)

    def spec(x):
        if x.dtype == jnp.int32:
            return smem
        return anywhere if isinstance(x, jax.ShapeDtypeStruct) else vmem

    inputs = [
        x if x.dtype == jnp.int32 else pltpu.with_memory_space_constraint(x, pltpu.VMEM)
        for x in inputs
    ]
    return pl.pallas_call(
        kernel,
        in_specs=[spec(x) for x in inputs],
        out_specs=[spec(x) for x in outs],
        out_shape=outs,
        scratch_shapes=scratch,
        compiler_params=pltpu.CompilerParams(vmem_limit_bytes=12 * 1024 * 1024),
        name=name,
    )(*inputs)


def exchanged(parts, shape):
    sent = lax.all_to_all(
        parts.reshape(shape), "xy", split_axis=0, concat_axis=0, tiled=True
    )
    return sent.reshape(parts.shape)


def local(volume, measured, view_order):
    f32 = jnp.float32
    bf16 = jnp.bfloat16
    vmem = pltpu.VMEM
    flat = volume.reshape(Z_DEV * X_DEV, NY)
    order = view_order.reshape(1, ANGLES)
    rows = measured.transpose(1, 2, 0, 3).reshape(VIEWS * ROWS_DEV * SUBSETS, COLS_DEV)
    made = vmem((TILES, DEPTH, VOXELS), bf16)
    slices = vmem((TILES, Z_DEV, VOXELS), f32)
    sm_scratch = vmem((VIEWS, Z_PAD, LANES), f32)
    acc_scratch = vmem((VIEWS, WIN, 128), f32)
    row_scratch = vmem((8, FULL), f32)
    owner_scratch = [row_scratch, vmem((SUMS, 8, FULL), f32), row_scratch]

    sent = vmem((SENT_ROWS, 128), bf16)
    hbm = pl.BlockSpec(memory_space=pltpu.HBM)
    up, down, flat, rows, order = pl.pallas_call(
        pack_kernel,
        in_specs=[hbm] * 3,
        out_specs=[pl.BlockSpec(memory_space=vmem)] * 5,
        out_shape=[
            sent, sent, vmem(flat.shape, f32), vmem(rows.shape, f32), vmem((1, ANGLES), jnp.int32)
        ],
        scratch_shapes=[vmem((SUBSETS * M_HALO, 128), f32), pltpu.SemaphoreType.DMA((3,))],
        compiler_params=pltpu.CompilerParams(vmem_limit_bytes=12 * 1024 * 1024),
        name="pack",
    )(*(pltpu.with_memory_space_constraint(x, pltpu.HBM) for x in (flat, rows, order)))
    next_up = [(i, (i + 1) % N_GZ) for i in range(N_GZ)]
    low = lax.ppermute(up, "gz", next_up)
    high = lax.ppermute(down, "gz", [(j, i) for i, j in next_up])
    w0, w1, own, mown, table = pl.pallas_call(
        prepare_kernel,
        in_specs=[pl.BlockSpec(memory_space=vmem)] * 3,
        out_specs=[pl.BlockSpec(memory_space=m) for m in (vmem, vmem, vmem, vmem, pltpu.SMEM)],
        out_shape=[
            made, made, slices, vmem((SUBSETS, VIEWS, 24, 128), f32), pltpu.SMEM(TABLE, jnp.int32)
        ],
        scratch_shapes=[
            vmem((VIEWS, TILES, VOXELS), f32), vmem(TABLE, jnp.int32), pltpu.SemaphoreType.DMA
        ],
        compiler_params=pltpu.CompilerParams(vmem_limit_bytes=12 * 1024 * 1024),
        name="prepare",
    )(*(pltpu.with_memory_space_constraint(x, vmem) for x in (order, flat, rows)))
    partial, side, m1 = call(
        first_kernel,
        (table, w0, own, mown, low, high),
        [vmem((N_XY * 12, 128), f32), slices, vmem((VIEWS, 64, 128), f32)],
        [
            vmem((Z_DEV * PITCH, NY), f32),
            acc_scratch,
            vmem((SUBSETS, VIEWS, M_ROWS, 128), f32),
            vmem((VIEWS, 72, 128), f32),
            vmem((2, EDGE_ROWS, 128), f32),
        ],
        "first",
    )
    (rounded,) = call(
        functools.partial(owner_kernel, subset=0),
        (table, exchanged(partial, (N_XY, 3, 4, 128))),
        [vmem((N_XY, 8, 128), bf16)],
        owner_scratch,
        "owner_a",
    )
    partial, new = call(
        middle_kernel,
        (table, exchanged(rounded, rounded.shape), own, side, m1, w0, w1),
        [vmem((N_XY * 10, 128), f32), slices],
        [sm_scratch, vmem((TILES, Z_PAD, VOXELS), bf16), acc_scratch],
        "middle",
    )
    (final,) = call(
        functools.partial(owner_kernel, subset=1),
        (table, exchanged(partial, (N_XY, 5, 2, 128))),
        [vmem((N_XY * 8, 128), f32)],
        owner_scratch,
        "owner_b",
    )
    volume_out, residual = call(
        last_kernel,
        (table, exchanged(final, (N_XY, 8, 128)), new, w1),
        [
            jax.ShapeDtypeStruct(VOLUME, f32),
            jax.ShapeDtypeStruct((VIEWS, ROWS_DEV, COLS_DEV), f32),
        ],
        [
            sm_scratch,
            slices,
            vmem((X_DEV // TILE, Z_DEV * OUT_PITCH, NY), f32),
            vmem((VIEWS, ROWS_DEV, COLS_DEV), f32),
            pltpu.SemaphoreType.DMA((X_DEV // TILE + 1,)),
        ],
        "last",
    )
    return volume_out, residual


def solution(mesh):
    in_specs = (P("gz", "xy", None), P(None, None, "gz", "xy"), P())
    out_specs = (P("gz", "xy", None), P(None, "gz", "xy"))
    return jax.shard_map(local, mesh=mesh, in_specs=in_specs, out_specs=out_specs, check_vma=False)
```

```python
import functools
import math

import jax
import jax.numpy as jnp
from jax import lax
from jax.experimental import pallas as pl
from jax.experimental.pallas import tpu as pltpu
from jax.sharding import PartitionSpec as P

Z_DEV = 16
X_DEV = 48
NY = 128
COLS_DEV = 48
ROWS_DEV = 20
VIEWS = 5
SUBSETS = 2
ANGLES = 48
N_XY = 32
N_GZ = 8
NX = X_DEV * N_XY
NZ = Z_DEV * N_GZ
DR = ROWS_DEV * N_GZ
DC = COLS_DEV * N_XY

WIN = 176
LANES = 256
MEAS_AT = LANES - COLS_DEV
Z_HALO = 6
Z_ALL = Z_DEV + 2 * Z_HALO
ONES = Z_ALL
Z_PAD = 32
GROUPS = 6
GOT = GROUPS * 8
ROWS_PER = (5, 4)
ROWS_BELOW = (3, 0)
M_HALO = 8
M_ROWS = 40
FULL = 15 * 128
SUMS = 4
TILE = 16
TILES_Y = NY // TILE
TILES = X_DEV // TILE * TILES_Y
VOXELS = TILE * TILE
COLS_TILE = 40
VOLUME = (Z_DEV, X_DEV, NY)
PLACE = (0, 40, 80, 128, 168)
DEPTH = 208
HALO_ROWS = Z_HALO * X_DEV
INNER_ROWS = HALO_ROWS // 2
EDGE_AT = HALO_ROWS + INNER_ROWS
EDGE_ROWS = SUBSETS * VIEWS * M_HALO
SENT_ROWS = EDGE_AT + EDGE_ROWS
PITCH = 56
OUT_PITCH = 24
TABLE = (16, 128)
SHIFT_AT = 32
TILE_AT = 64


def iota(shape, dim):
    return lax.broadcasted_iota(jnp.int32, shape, dim)


def slice_of(i, gz):
    low = Z_DEV * gz - Z_HALO + (i - Z_DEV)
    high = Z_DEV * gz + Z_DEV + (i - Z_DEV - Z_HALO)
    return jnp.where(i < Z_DEV, Z_DEV * gz + i, jnp.where(i < Z_DEV + Z_HALO, low, high))


def hat(row, z):
    position = (DR - 1) / 2.0 + 0.96 * (DR / NZ) * (z.astype(jnp.float32) - (NZ - 1) / 2.0)
    value = jnp.maximum(0.0, 1.0 - jnp.abs(position - row.astype(jnp.float32)) / 2.0)
    ok = (row >= 0) & (row < DR) & (z >= 0) & (z < NZ)
    return jnp.where(ok, value, 0.0)


def first_row(gz, subset):
    return ROWS_DEV * gz - ROWS_BELOW[subset] - ((gz + 1) >> 1)


def slot_weights(group, slot, i, gz, subset):
    per = ROWS_PER[subset]
    row = first_row(gz, subset) + group * per + slot
    return jnp.where((slot < per) & (i < Z_ALL), hat(row, slice_of(i, gz)), 0.0)


def tile_offsets(table_ref, subset, tile):
    return [
        pl.multiple_of(table_ref[subset * VIEWS + v, TILE_AT + tile], 8) for v in range(VIEWS)
    ]


def coordinate(x, y, cosine, sine):
    xc = x - (NX - 1) / 2.0
    yc = y - (NY - 1) / 2.0
    source = 2.0 * NX
    along = xc * cosine + yc * sine
    depth = yc * cosine - xc * sine
    return (DC - 1) / 2.0 + 0.9 * (DC / NX) * along * source / (source + depth)


def fill_table(cosine, sine, xy):
    lane = iota(TABLE, 1)
    tile = lane - TILE_AT
    is_tile = lane >= TILE_AT
    strip = lane & (N_XY - 1)
    x = jnp.where(is_tile, xy * X_DEV + (tile >> 3) * TILE, strip * X_DEV).astype(jnp.float32)
    y = jnp.where(is_tile, (tile & 7) * TILE, 0).astype(jnp.float32)
    dx = jnp.where(is_tile, TILE - 1.0, X_DEV - 1.0)
    dy = jnp.where(is_tile, TILE - 1.0, NY - 1.0)
    least = jnp.minimum(
        jnp.minimum(coordinate(x, y, cosine, sine), coordinate(x + dx, y, cosine, sine)),
        jnp.minimum(coordinate(x, y + dy, cosine, sine), coordinate(x + dx, y + dy, cosine, sine)),
    )
    least = jnp.floor(least).astype(jnp.int32)
    start = least - 2
    own = jnp.sum(jnp.where(lane == xy, start, 0).astype(jnp.float32), axis=1, keepdims=True)
    tiles = jnp.maximum(least - 1 - own.astype(jnp.int32), 0) & ~7
    table = jnp.where(lane < SHIFT_AT, start & ~127, start & 127)
    return jnp.where(is_tile, tiles, table), own


def positions(u_ref, cosine, sine, own, subset, xy):
    t = iota((TILES, VOXELS), 0)
    l = iota((TILES, VOXELS), 1)
    x = ((t >> 3) * TILE + (l >> 4) + xy * X_DEV).astype(jnp.float32)
    y = ((t & 7) * TILE + (l & 15)).astype(jnp.float32)
    for v in range(VIEWS):
        at = subset * VIEWS + v
        u = coordinate(x, y, cosine[at : at + 1, 0:1], sine[at : at + 1, 0:1])
        u_ref[v] = u - own[at : at + 1, :]


def weights(u_ref, offsets, tile):
    c = iota((COLS_TILE, VOXELS), 0).astype(jnp.float32)
    pieces = []
    for v in range(VIEWS):
        u = u_ref[v, pl.ds(tile, 1), :] - offsets[v].astype(jnp.float32)
        pieces.append(jnp.maximum(0.0, 1.0 - jnp.abs(u - c)))
    pieces.insert(3, jnp.zeros((8, VOXELS), jnp.float32))
    return jnp.concatenate(pieces, axis=0).astype(jnp.bfloat16)


def forward(w_ref, slices, acc_refs, m_ref, table_ref, out_ref, subset, gz):
    for acc_ref in acc_refs:
        acc_ref[...] = jnp.zeros_like(acc_ref)
    for tile in range(TILES):
        offsets = tile_offsets(table_ref, subset, tile)
        part = lax.dot_general(
            w_ref[tile],
            jnp.concatenate([slices(tile)] * 4, axis=0),
            (((1,), (1,)), ((), ())),
            preferred_element_type=jnp.float32,
        )
        for v in range(VIEWS):
            acc_refs[v][pl.ds(offsets[v], COLS_TILE), :] += part[PLACE[v] : PLACE[v] + COLS_TILE]
    per = ROWS_PER[subset]
    half = per + 1
    size = GROUPS * 2 * half
    k = iota((size, 128), 0)
    lane = iota((size, 128), 1)
    i = lane & (Z_PAD - 1)
    group = (k * 43) >> 9 if half == 6 else (k * 205) >> 11
    slot = k - group * 2 * half
    is_low = slot < half
    slot = jnp.where(is_low, slot, slot - half)
    rows = slot_weights(group, slot, i, gz, subset)
    rows = jnp.where((slot == per) & (i == ONES), 1.0, rows)
    rounded = rows.astype(jnp.bfloat16).astype(jnp.float32)
    rows = jnp.where(lane < 2 * Z_PAD, rounded, rows - rounded).astype(jnp.bfloat16)
    left_over = (iota((WIN, 128), 1) & Z_PAD) != 0
    used = GROUPS * VIEWS * 2 * half
    out_ref[used:, :] = jnp.zeros((out_ref.shape[0] - used, 128), jnp.float32)
    for v in range(VIEWS):
        sums = acc_refs[v][...]
        rounded = sums.astype(jnp.bfloat16).astype(jnp.float32)
        sums = jnp.where(left_over, sums - rounded, rounded).astype(jnp.bfloat16)
        sums = lax.dot_general(
            rows, sums, (((1,), (1,)), ((), ())), preferred_element_type=jnp.float32
        )
        high = jnp.concatenate(
            (sums[:, 128:WIN], jnp.zeros((size, LANES - WIN), jnp.float32)), axis=1
        )
        part = jnp.where(is_low, sums[:, 0:128], high) + m_ref[v, 0:size, :]
        out_ref[v * size : (v + 1) * size, :] = part


def three_parts(x, third):
    first = x.astype(jnp.bfloat16).astype(jnp.float32)
    second = (x - first).astype(jnp.bfloat16).astype(jnp.float32)
    part = jnp.where(third == 0, first, jnp.where(third == 1, second, x - first - second))
    return part.astype(jnp.bfloat16)


def smear(recv_ref, sm_ref, gz):
    i = iota((3 * Z_PAD, 3 * GOT), 0)
    k = iota((3 * Z_PAD, 3 * GOT), 1)
    third = (k >= GOT).astype(jnp.int32) + (k >= 2 * GOT).astype(jnp.int32)
    k = k - GOT * third
    part = k & 7
    block = i >> 5
    slot = jnp.where(block == 0, part, 2 * (part - 5) + block - 1)
    rows = slot_weights(k >> 3, slot, i & (Z_PAD - 1), gz, 0)
    rows = three_parts(jnp.where((block == 0) == (part < 5), rows, 0.0), third)
    ones = iota((Z_PAD, LANES), 0) == ONES
    for v in range(VIEWS):
        got = recv_ref[v * GROUPS : (v + 1) * GROUPS].astype(jnp.float32)
        got = got.reshape(GOT, 128).astype(jnp.bfloat16)
        sums = jnp.dot(
            rows, jnp.concatenate((got, got, got), axis=0), preferred_element_type=jnp.float32
        )
        high = sums[Z_PAD : 2 * Z_PAD] + pltpu.roll(sums[2 * Z_PAD :], 128 - COLS_DEV, 1)
        smeared = jnp.concatenate((sums[0:Z_PAD], high), axis=1)
        sm_ref[v] = jnp.where(ones, 1.0, smeared).astype(jnp.bfloat16).astype(jnp.float32)


def smear_last(recv_ref, sm_ref, res_ref, gz):
    size = 2 * Z_PAD + 24
    i = iota((size, 3 * GOT), 0)
    k = iota((size, 3 * GOT), 1)
    third = (k >= GOT).astype(jnp.int32) + (k >= 2 * GOT).astype(jnp.int32)
    k = k - GOT * third
    part = k & 7
    rows = slot_weights(k >> 3, part & 3, i & (Z_PAD - 1), gz, 1)
    rows = three_parts(jnp.where((part >= 4) == (i >= Z_PAD), rows, 0.0), third)
    j = i - 2 * Z_PAD + ((gz + 1) >> 1)
    picked = jnp.where(k == ((j >> 2) << 3) + 4 + (j & 3), 1.0, 0.0).astype(jnp.bfloat16)
    rows = jnp.where(i >= 2 * Z_PAD, picked.astype(jnp.float32), rows.astype(jnp.float32))
    rows = rows.astype(jnp.bfloat16)
    ones = iota((Z_PAD, LANES), 0) == ONES
    part = iota((GOT, 128), 0) & 7
    exact = (part >= 4) & (iota((GOT, 128), 1) >= MEAS_AT - 128)
    for v in range(VIEWS):
        got = recv_ref[v * GOT : (v + 1) * GOT, :]
        first = got.astype(jnp.bfloat16).astype(jnp.float32)
        second = (got - first).astype(jnp.bfloat16).astype(jnp.float32)
        parts = (
            first,
            jnp.where(exact, second, first),
            jnp.where(exact, got - first - second, first),
        )
        sums = jnp.dot(
            rows,
            jnp.concatenate(parts, axis=0).astype(jnp.bfloat16),
            preferred_element_type=jnp.float32,
        )
        smeared = jnp.concatenate((sums[0:Z_PAD], sums[Z_PAD : 2 * Z_PAD]), axis=1)
        sm_ref[v] = jnp.where(ones, 1.0, smeared).astype(jnp.bfloat16).astype(jnp.float32)
        own = pltpu.roll(sums[2 * Z_PAD :], 256 - MEAS_AT, 1)
        res_ref[v] = own[0:ROWS_DEV, 0:COLS_DEV]


def windows(sm_ref, offsets):
    lane = iota((Z_PAD, 128), 1)
    placed = []
    for v in range(VIEWS):
        at = PLACE[v] & 127
        shift = (at - offsets[v]) & 127
        low = pltpu.roll(sm_ref[v, :, 0:128], shift, 1)
        high = pltpu.roll(sm_ref[v, :, 128:256], shift, 1)
        placed.append(jnp.where(lane < at + 128 - offsets[v], low, high))
    first = jnp.where(lane < 40, placed[0], jnp.where(lane < 80, placed[1], placed[2]))
    first = jnp.where(lane < 120, first, 0.0)
    second = jnp.where(lane < 40, placed[3], jnp.where(lane < 80, placed[4], 0.0))
    both = jnp.concatenate((first, second), axis=1)
    return both.astype(jnp.bfloat16)[:, 0:DEPTH]


def backward(w_ref, sm_ref, table_ref, old, store, subset, gz):
    zi = slice_of(iota((Z_PAD, LANES), 0), gz)
    inside = iota((Z_PAD, LANES), 0) < Z_ALL
    total = jnp.sum(jnp.where(inside, hat(iota((Z_PAD, LANES), 1), zi), 0.0), axis=1, keepdims=True)

    for tile in range(TILES):
        offsets = tile_offsets(table_ref, subset, tile)
        back = jnp.dot(
            windows(sm_ref, offsets), w_ref[tile], preferred_element_type=jnp.float32
        )
        norm = total * back[ONES : ONES + 1, :]
        store(tile, old(tile), back / jnp.maximum(norm, 1.0))


def swap_blocks(rows):
    block = iota((8, 128), 1) >> 4
    for d in (4, 2, 1):
        high = (block & d) != 0
        new = list(rows)
        for i in range(8):
            if i & d == 0:
                a, b = (rows[i], rows[i + d])
                new[i] = jnp.where(high, pltpu.roll(b, 16 * d, 1), a)
                new[i + d] = jnp.where(high, b, pltpu.roll(a, 128 - 16 * d, 1))
        rows = new
    return rows


def relay(source_ref, out_ref, pitch, unrolled):
    def step(xb, nothing):
        for half in range(2):
            for b in range(2):
                at = xb * TILE + half * 8 + b * 8 * pitch
                rows = [source_ref[pl.ds(at + i, 8, stride=pitch), :] for i in range(8)]
                for q, block in enumerate(swap_blocks(rows)):
                    out_ref[
                        xb * TILES_Y + q, b * 8 : b * 8 + 8, half * 128 : half * 128 + 128
                    ] = block
        return nothing

    if unrolled:
        for xb in range(X_DEV // TILE):
            step(xb, 0)
    else:
        lax.fori_loop(0, X_DEV // TILE, step, 0)


def pack_kernel(
    vol_hbm, meas_hbm, order_hbm, up_ref, down_ref, vol_ref, meas_ref, order_ref, row_ref, sems
):
    copies = [
        pltpu.make_async_copy(vol_hbm, vol_ref, sems.at[0]),
        pltpu.make_async_copy(meas_hbm, meas_ref, sems.at[1]),
        pltpu.make_async_copy(order_hbm, order_ref, sems.at[2]),
    ]
    for copy in copies:
        copy.start()
    row_ref[...] = jnp.zeros_like(row_ref)
    for copy in copies:
        copy.wait()
    for out_ref, z, inner, r in (
        (up_ref, Z_DEV - Z_HALO, Z_HALO // 2, ROWS_DEV - M_HALO),
        (down_ref, 0, 0, 0),
    ):
        slices = vol_ref[z * X_DEV : (z + Z_HALO) * X_DEV, :]
        rounded = slices.astype(jnp.bfloat16)
        out_ref[0:HALO_ROWS, :] = rounded
        left = slices - rounded.astype(jnp.float32)
        at = inner * X_DEV
        out_ref[HALO_ROWS:EDGE_AT, :] = left[at : at + INNER_ROWS].astype(jnp.bfloat16)
        for v in range(VIEWS):
            at = (v * ROWS_DEV + r) * SUBSETS
            row_ref[:, 0:COLS_DEV] = meas_ref[at : at + SUBSETS * M_HALO, :]
            row = row_ref[...]
            rounded = row.astype(jnp.bfloat16).astype(jnp.float32)
            both = pltpu.roll(rounded, MEAS_AT - 128, 1)
            both = both + pltpu.roll(row - rounded, MEAS_AT - 128 - COLS_DEV, 1)
            at = EDGE_AT + v * SUBSETS * M_HALO
            out_ref[at : at + SUBSETS * M_HALO, :] = both.astype(jnp.bfloat16)


def prepare_kernel(
    order_ref, vol_ref, meas_ref,
    w0_ref, w1_ref, own_ref, mown_ref, table_ref, u_ref, flat_ref, sem,
):
    xy = lax.axis_index("xy")
    chosen = iota((TABLE[0], ANGLES), 0) == iota((TABLE[0], ANGLES), 1)
    chosen = jnp.where(chosen, order_ref[...].astype(jnp.float32), 0.0)
    chosen = jnp.broadcast_to(jnp.sum(chosen, axis=1, keepdims=True), TABLE)
    angles = 2.0 * math.pi * chosen / ANGLES
    cosine = jnp.cos(angles)
    sine = jnp.sin(angles)
    flat_ref[...], own = fill_table(cosine, sine, xy)
    copy = pltpu.make_async_copy(flat_ref, table_ref, sem)
    copy.start()
    relay(vol_ref, own_ref, X_DEV, False)
    mown_ref[...] = jnp.zeros_like(mown_ref)
    for s in range(SUBSETS):
        for v in range(VIEWS):
            for at, count in ((0, 8), (8, 8), (16, 4)):
                rows = meas_ref[pl.ds((v * ROWS_DEV + at) * 2 + s, count, stride=2), :]
                mown_ref[s, v, at : at + count, MEAS_AT - 128 : 128] = rows
    copy.wait()
    for subset, w_ref in ((0, w0_ref), (1, w1_ref)):
        positions(u_ref, cosine, sine, own, subset, xy)

        def step(tt, nothing):
            for t in range(8):
                tile = tt * 8 + t
                w_ref[tile] = weights(u_ref, tile_offsets(table_ref, subset, tile), tile)
            return nothing

        lax.fori_loop(0, TILES // 8, step, 0)


def first_kernel(
    table_ref, w_ref, own_ref, mown_ref, low_ref, high_ref,
    out_ref, side_ref, m1_ref, halo_ref, raw_ref, m0_ref, edge_ref, *acc_refs,
):
    gz = lax.axis_index("gz")
    for side, (sent_ref, inner) in enumerate(((low_ref, Z_HALO // 2), (high_ref, 0))):
        left_at = HALO_ROWS - inner * X_DEV
        for z in range(Z_HALO):
            at = z * X_DEV
            rows = sent_ref[at : at + X_DEV, :].astype(jnp.float32)
            if inner <= z < inner + Z_HALO // 2:
                rows = rows + sent_ref[left_at + at : left_at + at + X_DEV, :].astype(jnp.float32)
            at = (side * Z_HALO + z) * PITCH
            halo_ref[at : at + X_DEV, :] = rows
        edge = sent_ref[EDGE_AT:SENT_ROWS, :].astype(jnp.float32)
        edge = edge + pltpu.roll(edge, COLS_DEV, 1)
        edge_ref[side] = jnp.where(iota(edge.shape, 1) >= MEAS_AT - 128, edge, 0.0)
    for z in range(2 * Z_HALO, Z_DEV):
        value = 1.0 if z == ONES - Z_DEV else 0.0
        halo_ref[z * PITCH : z * PITCH + X_DEV, :] = jnp.full((X_DEV, NY), value, jnp.float32)
    relay(halo_ref, side_ref, PITCH, True)
    for s, m_ref in ((0, m0_ref), (1, m1_ref)):
        per = ROWS_PER[s]
        m_ref[...] = jnp.zeros_like(m_ref)
        for v in range(VIEWS):
            edge = pl.ds(v * 2 * M_HALO + s, M_HALO, stride=2)
            high = edge_ref[1, edge, :]
            joined = jnp.concatenate(
                (
                    edge_ref[0, edge, :],
                    mown_ref[s, v, 0:16, :],
                    jnp.concatenate((mown_ref[s, v, 16:20, :], high[0:4]), axis=0),
                    jnp.concatenate((high[4:8], jnp.zeros((4, 128), jnp.float32)), axis=0),
                ),
                axis=0,
            )
            raw_ref[s, v] = pltpu.roll(
                joined, M_ROWS + ((gz + 1) >> 1) - (M_HALO - ROWS_BELOW[s]), 0
            )
            for group in range(GROUPS):
                at = group * 2 * (per + 1) + per + 1
                m_ref[v, at : at + per, :] = raw_ref[s, v, group * per : (group + 1) * per, :]

    def slices(tile):
        return jnp.concatenate((own_ref[tile], side_ref[tile]), axis=0).astype(jnp.bfloat16)

    forward(w_ref, slices, acc_refs, m0_ref, table_ref, out_ref, 0, gz)


def middle_kernel(
    table_ref, recv_ref, own_ref, side_ref, m_ref, w0_ref, w1_ref,
    out_ref, new_ref, sm_ref, vb_ref, *acc_refs,
):
    gz = lax.axis_index("gz")
    smear(recv_ref, sm_ref, gz)
    ones = iota((Z_PAD, VOXELS), 0) == ONES

    def old(tile):
        return jnp.concatenate((own_ref[tile], side_ref[tile]), axis=0)

    def store(tile, old, change):
        new = jnp.where(ones, 1.0, old + change)
        new_ref[tile] = new[0:Z_DEV]
        vb_ref[tile] = new.astype(jnp.bfloat16)

    backward(w0_ref, sm_ref, table_ref, old, store, 0, gz)
    forward(w1_ref, lambda tile: vb_ref[tile], acc_refs, m_ref, table_ref, out_ref, 1, gz)


def last_kernel(
    table_ref, recv_ref, old_ref, w_ref,
    out_ref, res_ref, sm_ref, new_ref, block_ref, own_ref, sems,
):
    gz = lax.axis_index("gz")
    smear_last(recv_ref, sm_ref, own_ref, gz)
    copies = [pltpu.make_async_copy(own_ref, res_ref, sems.at[X_DEV // TILE])]
    copies[0].start()

    def store(tile, old, change):
        new_ref[tile] = old + change[0:Z_DEV]

    backward(w_ref, sm_ref, table_ref, lambda tile: old_ref[tile], store, 1, gz)
    for xb in range(X_DEV // TILE):
        for half in range(2):
            for b in range(Z_DEV // 8):
                blocks = [
                    new_ref[xb * TILES_Y + q, b * 8 : b * 8 + 8, half * 128 : half * 128 + 128]
                    for q in range(TILES_Y)
                ]
                at = half * 8 + b * 8 * OUT_PITCH
                for i, row in enumerate(swap_blocks(blocks)):
                    block_ref[xb, pl.ds(at + i, 8, stride=OUT_PITCH), :] = row
        copies.append(
            pltpu.make_async_copy(
                block_ref.at[xb].reshape(Z_DEV, OUT_PITCH, NY).at[:, 0:TILE, :],
                out_ref.at[:, pl.ds(xb * TILE, TILE), :],
                sems.at[xb],
            )
        )
        copies[-1].start()
    for copy in copies:
        copy.wait()


def owner_kernel(table_ref, recv_ref, out_ref, acc_ref, mea_ref, *sum_refs, subset):
    gz = lax.axis_index("gz")
    xy = lax.axis_index("xy")
    view = jnp.minimum(xy // GROUPS, VIEWS - 1)
    group = xy % GROUPS
    at = subset * VIEWS + view
    per = ROWS_PER[subset]
    half = per + 1
    lane = iota((8, 128), 1)
    for sum_ref in sum_refs:
        sum_ref[...] = jnp.zeros_like(sum_ref)
    mea_ref[...] = jnp.zeros_like(mea_ref)
    end = N_XY * 2 * half - 8

    def upper(s):
        row = s * 2 * half + half
        last = recv_ref[min(row, end) : min(row, end) + 8, :]
        return pltpu.roll(last, 8 - (row - end), 0) if row > end else last

    for s in range(N_XY):
        column = s * COLS_DEV
        own = jnp.where(lane >= MEAS_AT - 128, upper(s), 0.0)
        own = pltpu.roll(own, (column + 256 - MEAS_AT) % 128, 1)
        block = column // 128 * 128
        offset = column - block
        mea_ref[:, block : block + 128] += jnp.where(lane >= offset, own, 0.0)
        if offset + COLS_DEV > 128:
            mea_ref[:, block + 128 : block + 256] += jnp.where(lane < offset, own, 0.0)
    for s in range(N_XY):
        base = pl.multiple_of(table_ref[at, s], 128)
        shift = table_ref[at, SHIFT_AT + s]
        row = s * 2 * half
        low = pltpu.roll(recv_ref[row : row + 8, :], shift, 1)
        high = pltpu.roll(jnp.where(lane < WIN - 128, upper(s), 0.0), shift, 1)
        wrapped = lane < shift
        part_ref = sum_refs[s % SUMS]
        part_ref[:, pl.ds(base, 128)] += jnp.where(wrapped, 0.0, low)
        part_ref[:, pl.ds(base + 128, 128)] += jnp.where(wrapped, low, high)
        part_ref[:, pl.ds(base + 256, 128)] += jnp.where(wrapped, high, 0.0)
    slot = iota((8, NZ), 0)
    row = first_row(gz, subset) + group * per + slot
    ray_rows = jnp.where(slot < per, hat(row, iota((8, NZ), 1)), 0.0)
    ray_rows = jnp.sum(ray_rows, axis=1, keepdims=True)
    sums = sum_refs[0][...]
    for part_ref in sum_refs[1:]:
        sums = sums + part_ref[...]
    totals = sums[per : per + 1, :]
    acc_ref[...] = mea_ref[...] - sums / jnp.maximum(ray_rows * totals, 1.0)
    for t in range(N_XY):
        base = pl.multiple_of(table_ref[at, t], 128)
        shift = table_ref[at, SHIFT_AT + t]
        back = (128 - shift) & 127
        a = pltpu.roll(acc_ref[:, pl.ds(base, 128)], back, 1)
        b = pltpu.roll(acc_ref[:, pl.ds(base + 128, 128)], back, 1)
        c = pltpu.roll(acc_ref[:, pl.ds(base + 256, 128)], back, 1)
        kept = lane < 128 - shift
        low = jnp.where(kept, a, b)
        high = jnp.where(kept, b, c)
        if subset == 0:
            other = pltpu.roll(high, COLS_DEV, 1)
            even = jnp.where(
                slot == 5,
                pltpu.roll(high, 5, 0),
                jnp.where(slot == 6, pltpu.roll(high, 4, 0), pltpu.roll(high, 3, 0)),
            )
            odd = jnp.where(slot == 5, pltpu.roll(other, 4, 0), pltpu.roll(other, 3, 0))
            rest = jnp.where(lane < COLS_DEV, even, odd)
            out_ref[t] = jnp.where(slot < 5, low, rest).astype(jnp.bfloat16)
            continue
        column = t * COLS_DEV
        block = column // 128 * 128
        offset = column - block
        turn = (MEAS_AT - 128 - offset) % 128
        own = pltpu.roll(acc_ref[:, block : block + 128], turn, 1)
        if offset + COLS_DEV > 128:
            more = pltpu.roll(acc_ref[:, block + 128 : block + 256], turn, 1)
            own = jnp.where(lane < MEAS_AT - offset, own, more)
        high = jnp.where(lane >= MEAS_AT - 128, own, high)
        out_ref[t * 8 : (t + 1) * 8, :] = jnp.where(slot < 4, low, pltpu.roll(high, 4, 0))


def call(kernel, inputs, outs, scratch, name):
    vmem = pl.BlockSpec(memory_space=pltpu.VMEM)
    smem = pl.BlockSpec(memory_space=pltpu.SMEM)
    anywhere = pl.BlockSpec(memory_space=pl.ANY)

    def spec(x):
        if x.dtype == jnp.int32:
            return smem
        return anywhere if isinstance(x, jax.ShapeDtypeStruct) else vmem

    inputs = [
        x if x.dtype == jnp.int32 else pltpu.with_memory_space_constraint(x, pltpu.VMEM)
        for x in inputs
    ]
    return pl.pallas_call(
        kernel,
        in_specs=[spec(x) for x in inputs],
        out_specs=[spec(x) for x in outs],
        out_shape=outs,
        scratch_shapes=scratch,
        compiler_params=pltpu.CompilerParams(vmem_limit_bytes=12 * 1024 * 1024),
        name=name,
    )(*inputs)


def exchanged(parts, shape):
    sent = lax.all_to_all(
        parts.reshape(shape), "xy", split_axis=0, concat_axis=0, tiled=True
    )
    return sent.reshape(parts.shape)


def local(volume, measured, view_order):
    f32 = jnp.float32
    bf16 = jnp.bfloat16
    vmem = pltpu.VMEM
    flat = volume.reshape(Z_DEV * X_DEV, NY)
    order = view_order.reshape(1, ANGLES)
    rows = measured.transpose(1, 2, 0, 3).reshape(VIEWS * ROWS_DEV * SUBSETS, COLS_DEV)
    made = vmem((TILES, DEPTH, VOXELS), bf16)
    slices = vmem((TILES, Z_DEV, VOXELS), f32)
    sm_scratch = vmem((VIEWS, Z_PAD, LANES), f32)
    acc_scratch = [vmem((WIN, 128), f32)] * VIEWS
    row_scratch = vmem((8, FULL), f32)
    owner_scratch = [row_scratch] * (2 + SUMS)

    sent = vmem((SENT_ROWS, 128), bf16)
    hbm = pl.BlockSpec(memory_space=pltpu.HBM)
    up, down, flat, rows, order = pl.pallas_call(
        pack_kernel,
        in_specs=[hbm] * 3,
        out_specs=[pl.BlockSpec(memory_space=vmem)] * 5,
        out_shape=[
            sent, sent, vmem(flat.shape, f32), vmem(rows.shape, f32), vmem((1, ANGLES), jnp.int32)
        ],
        scratch_shapes=[vmem((SUBSETS * M_HALO, 128), f32), pltpu.SemaphoreType.DMA((3,))],
        compiler_params=pltpu.CompilerParams(vmem_limit_bytes=12 * 1024 * 1024),
        name="pack",
    )(*(pltpu.with_memory_space_constraint(x, pltpu.HBM) for x in (flat, rows, order)))
    next_up = [(i, (i + 1) % N_GZ) for i in range(N_GZ)]
    low = lax.ppermute(up, "gz", next_up)
    high = lax.ppermute(down, "gz", [(j, i) for i, j in next_up])
    w0, w1, own, mown, table = pl.pallas_call(
        prepare_kernel,
        in_specs=[pl.BlockSpec(memory_space=vmem)] * 3,
        out_specs=[pl.BlockSpec(memory_space=m) for m in (vmem, vmem, vmem, vmem, pltpu.SMEM)],
        out_shape=[
            made, made, slices, vmem((SUBSETS, VIEWS, 24, 128), f32), pltpu.SMEM(TABLE, jnp.int32)
        ],
        scratch_shapes=[
            vmem((VIEWS, TILES, VOXELS), f32), vmem(TABLE, jnp.int32), pltpu.SemaphoreType.DMA
        ],
        compiler_params=pltpu.CompilerParams(vmem_limit_bytes=12 * 1024 * 1024),
        name="prepare",
    )(*(pltpu.with_memory_space_constraint(x, vmem) for x in (order, flat, rows)))
    partial, side, m1 = call(
        first_kernel,
        (table, w0, own, mown, low, high),
        [vmem((N_XY * 12, 128), f32), slices, vmem((VIEWS, 64, 128), f32)],
        [
            vmem((Z_DEV * PITCH, NY), f32),
            vmem((SUBSETS, VIEWS, M_ROWS, 128), f32),
            vmem((VIEWS, 72, 128), f32),
            vmem((2, EDGE_ROWS, 128), f32),
            *acc_scratch,
        ],
        "first",
    )
    (rounded,) = call(
        functools.partial(owner_kernel, subset=0),
        (table, exchanged(partial, (N_XY, 3, 4, 128))),
        [vmem((N_XY, 8, 128), bf16)],
        owner_scratch,
        "owner_a",
    )
    partial, new = call(
        middle_kernel,
        (table, exchanged(rounded, rounded.shape), own, side, m1, w0, w1),
        [vmem((N_XY * 10, 128), f32), slices],
        [sm_scratch, vmem((TILES, Z_PAD, VOXELS), bf16), *acc_scratch],
        "middle",
    )
    (final,) = call(
        functools.partial(owner_kernel, subset=1),
        (table, exchanged(partial, (N_XY, 5, 2, 128))),
        [vmem((N_XY * 8, 128), f32)],
        owner_scratch,
        "owner_b",
    )
    volume_out, residual = call(
        last_kernel,
        (table, exchanged(final, (N_XY, 8, 128)), new, w1),
        [
            jax.ShapeDtypeStruct(VOLUME, f32),
            jax.ShapeDtypeStruct((VIEWS, ROWS_DEV, COLS_DEV), f32),
        ],
        [
            sm_scratch,
            slices,
            vmem((X_DEV // TILE, Z_DEV * OUT_PITCH, NY), f32),
            vmem((VIEWS, ROWS_DEV, COLS_DEV), f32),
            pltpu.SemaphoreType.DMA((X_DEV // TILE + 1,)),
        ],
        "last",
    )
    return volume_out, residual


def solution(mesh):
    in_specs = (P("gz", "xy", None), P(None, None, "gz", "xy"), P())
    out_specs = (P("gz", "xy", None), P(None, "gz", "xy"))
    return jax.shard_map(local, mesh=mesh, in_specs=in_specs, out_specs=out_specs, check_vma=False)
```

```python
import functools
import math

import jax
import jax.numpy as jnp
from jax import lax
from jax.experimental import pallas as pl
from jax.experimental.pallas import tpu as pltpu
from jax.sharding import PartitionSpec as P

Z_DEV = 16
X_DEV = 48
NY = 128
COLS_DEV = 48
ROWS_DEV = 20
VIEWS = 5
SUBSETS = 2
ANGLES = 48
N_XY = 32
N_GZ = 8
NX = X_DEV * N_XY
NZ = Z_DEV * N_GZ
DR = ROWS_DEV * N_GZ
DC = COLS_DEV * N_XY

WIN = 176
LANES = 256
MEAS_AT = LANES - COLS_DEV
Z_HALO = 6
Z_ALL = Z_DEV + 2 * Z_HALO
ONES = Z_ALL
Z_PAD = 32
GROUPS = 6
GOT = GROUPS * 8
ROWS_PER = (5, 4)
ROWS_BELOW = (3, 0)
M_HALO = 8
M_ROWS = 40
FULL = 15 * 128
SUMS = 4
TILE = 16
TILES_Y = NY // TILE
TILES = X_DEV // TILE * TILES_Y
VOXELS = TILE * TILE
COLS_TILE = 40
VOLUME = (Z_DEV, X_DEV, NY)
PLACE = (0, 40, 80, 128, 168)
DEPTH = 208
HALO_ROWS = Z_HALO * X_DEV
INNER_ROWS = HALO_ROWS // 2
EDGE_AT = HALO_ROWS + INNER_ROWS
EDGE_ROWS = SUBSETS * VIEWS * M_HALO
SENT_ROWS = EDGE_AT + EDGE_ROWS
TABLE = (16, 128)
SHIFT_AT = 32
TILE_AT = 64


def iota(shape, dim):
    return lax.broadcasted_iota(jnp.int32, shape, dim)


def slice_of(i, gz):
    low = Z_DEV * gz - Z_HALO + (i - Z_DEV)
    high = Z_DEV * gz + Z_DEV + (i - Z_DEV - Z_HALO)
    return jnp.where(i < Z_DEV, Z_DEV * gz + i, jnp.where(i < Z_DEV + Z_HALO, low, high))


def hat(row, z):
    position = (DR - 1) / 2.0 + 0.96 * (DR / NZ) * (z.astype(jnp.float32) - (NZ - 1) / 2.0)
    value = jnp.maximum(0.0, 1.0 - jnp.abs(position - row.astype(jnp.float32)) / 2.0)
    ok = (row >= 0) & (row < DR) & (z >= 0) & (z < NZ)
    return jnp.where(ok, value, 0.0)


def first_row(gz, subset):
    return ROWS_DEV * gz - ROWS_BELOW[subset] - ((gz + 1) >> 1)


def slot_weights(group, slot, i, gz, subset):
    per = ROWS_PER[subset]
    row = first_row(gz, subset) + group * per + slot
    return jnp.where((slot < per) & (i < Z_ALL), hat(row, slice_of(i, gz)), 0.0)


def tile_offsets(table_ref, subset, tile):
    return [
        pl.multiple_of(table_ref[subset * VIEWS + v, TILE_AT + tile], 8) for v in range(VIEWS)
    ]


def coordinate(x, y, cosine, sine):
    xc = x - (NX - 1) / 2.0
    yc = y - (NY - 1) / 2.0
    source = 2.0 * NX
    along = xc * cosine + yc * sine
    depth = yc * cosine - xc * sine
    return (DC - 1) / 2.0 + 0.9 * (DC / NX) * along * source / (source + depth)


def fill_table(cosine, sine, xy):
    lane = iota(TABLE, 1)
    tile = lane - TILE_AT
    is_tile = lane >= TILE_AT
    strip = lane & (N_XY - 1)
    x = jnp.where(is_tile, xy * X_DEV + (tile >> 3) * TILE, strip * X_DEV).astype(jnp.float32)
    y = jnp.where(is_tile, (tile & 7) * TILE, 0).astype(jnp.float32)
    dx = jnp.where(is_tile, TILE - 1.0, X_DEV - 1.0)
    dy = jnp.where(is_tile, TILE - 1.0, NY - 1.0)
    least = jnp.minimum(
        jnp.minimum(coordinate(x, y, cosine, sine), coordinate(x + dx, y, cosine, sine)),
        jnp.minimum(coordinate(x, y + dy, cosine, sine), coordinate(x + dx, y + dy, cosine, sine)),
    )
    least = jnp.floor(least).astype(jnp.int32)
    start = least - 2
    own = jnp.sum(jnp.where(lane == xy, start, 0).astype(jnp.float32), axis=1, keepdims=True)
    tiles = jnp.maximum(least - 1 - own.astype(jnp.int32), 0) & ~7
    table = jnp.where(lane < SHIFT_AT, start & ~127, start & 127)
    return jnp.where(is_tile, tiles, table), own


def positions(u_ref, cosine, sine, own, subset, xy):
    t = iota((TILES, VOXELS), 0)
    l = iota((TILES, VOXELS), 1)
    x = ((t >> 3) * TILE + (l >> 4) + xy * X_DEV).astype(jnp.float32)
    y = ((t & 7) * TILE + (l & 15)).astype(jnp.float32)
    for v in range(VIEWS):
        at = subset * VIEWS + v
        u = coordinate(x, y, cosine[at : at + 1, 0:1], sine[at : at + 1, 0:1])
        u_ref[v] = u - own[at : at + 1, :]


def weights(u_ref, offsets, tile):
    c = iota((COLS_TILE, VOXELS), 0).astype(jnp.float32)
    pieces = []
    for v in range(VIEWS):
        u = u_ref[v, pl.ds(tile, 1), :] - offsets[v].astype(jnp.float32)
        pieces.append(jnp.maximum(0.0, 1.0 - jnp.abs(u - c)))
    pieces.insert(3, jnp.zeros((8, VOXELS), jnp.float32))
    return jnp.concatenate(pieces, axis=0).astype(jnp.bfloat16)


def forward(w_ref, slices, acc_refs, m_ref, table_ref, out_ref, subset, gz):
    for acc_ref in acc_refs:
        acc_ref[...] = jnp.zeros_like(acc_ref)
    for tile in range(TILES):
        offsets = tile_offsets(table_ref, subset, tile)
        part = lax.dot_general(
            w_ref[tile],
            jnp.concatenate([slices(tile)] * 4, axis=0),
            (((1,), (1,)), ((), ())),
            preferred_element_type=jnp.float32,
        )
        for v in range(VIEWS):
            acc_refs[v][pl.ds(offsets[v], COLS_TILE), :] += part[PLACE[v] : PLACE[v] + COLS_TILE]
    per = ROWS_PER[subset]
    half = per + 1
    size = GROUPS * 2 * half
    k = iota((size, 128), 0)
    lane = iota((size, 128), 1)
    i = lane & (Z_PAD - 1)
    group = (k * 43) >> 9 if half == 6 else (k * 205) >> 11
    slot = k - group * 2 * half
    is_low = slot < half
    slot = jnp.where(is_low, slot, slot - half)
    rows = slot_weights(group, slot, i, gz, subset)
    rows = jnp.where((slot == per) & (i == ONES), 1.0, rows)
    rounded = rows.astype(jnp.bfloat16).astype(jnp.float32)
    rows = jnp.where(lane < 2 * Z_PAD, rounded, rows - rounded).astype(jnp.bfloat16)
    left_over = (iota((WIN, 128), 1) & Z_PAD) != 0
    used = GROUPS * VIEWS * 2 * half
    out_ref[used:, :] = jnp.zeros((out_ref.shape[0] - used, 128), jnp.float32)
    for v in range(VIEWS):
        sums = acc_refs[v][...]
        rounded = sums.astype(jnp.bfloat16).astype(jnp.float32)
        sums = jnp.where(left_over, sums - rounded, rounded).astype(jnp.bfloat16)
        sums = lax.dot_general(
            rows, sums, (((1,), (1,)), ((), ())), preferred_element_type=jnp.float32
        )
        high = jnp.concatenate(
            (sums[:, 128:WIN], jnp.zeros((size, LANES - WIN), jnp.float32)), axis=1
        )
        part = jnp.where(is_low, sums[:, 0:128], high) + m_ref[v, 0:size, :]
        out_ref[v * size : (v + 1) * size, :] = part


def three_parts(x, third):
    first = x.astype(jnp.bfloat16).astype(jnp.float32)
    second = (x - first).astype(jnp.bfloat16).astype(jnp.float32)
    part = jnp.where(third == 0, first, jnp.where(third == 1, second, x - first - second))
    return part.astype(jnp.bfloat16)


def smear(recv_ref, sm_ref, gz):
    i = iota((3 * Z_PAD, 3 * GOT), 0)
    k = iota((3 * Z_PAD, 3 * GOT), 1)
    third = (k >= GOT).astype(jnp.int32) + (k >= 2 * GOT).astype(jnp.int32)
    k = k - GOT * third
    part = k & 7
    block = i >> 5
    slot = jnp.where(block == 0, part, 2 * (part - 5) + block - 1)
    rows = slot_weights(k >> 3, slot, i & (Z_PAD - 1), gz, 0)
    rows = three_parts(jnp.where((block == 0) == (part < 5), rows, 0.0), third)
    ones = iota((Z_PAD, LANES), 0) == ONES
    for v in range(VIEWS):
        got = recv_ref[v * GROUPS : (v + 1) * GROUPS].astype(jnp.float32)
        got = got.reshape(GOT, 128).astype(jnp.bfloat16)
        sums = jnp.dot(
            rows, jnp.concatenate((got, got, got), axis=0), preferred_element_type=jnp.float32
        )
        high = sums[Z_PAD : 2 * Z_PAD] + pltpu.roll(sums[2 * Z_PAD :], 128 - COLS_DEV, 1)
        smeared = jnp.concatenate((sums[0:Z_PAD], high), axis=1)
        sm_ref[v] = jnp.where(ones, 1.0, smeared).astype(jnp.bfloat16).astype(jnp.float32)


def smear_last(recv_ref, sm_ref, res_ref, gz):
    size = 2 * Z_PAD + 24
    i = iota((size, 3 * GOT), 0)
    k = iota((size, 3 * GOT), 1)
    third = (k >= GOT).astype(jnp.int32) + (k >= 2 * GOT).astype(jnp.int32)
    k = k - GOT * third
    part = k & 7
    rows = slot_weights(k >> 3, part & 3, i & (Z_PAD - 1), gz, 1)
    rows = three_parts(jnp.where((part >= 4) == (i >= Z_PAD), rows, 0.0), third)
    j = i - 2 * Z_PAD + ((gz + 1) >> 1)
    picked = jnp.where(k == ((j >> 2) << 3) + 4 + (j & 3), 1.0, 0.0).astype(jnp.bfloat16)
    rows = jnp.where(i >= 2 * Z_PAD, picked.astype(jnp.float32), rows.astype(jnp.float32))
    rows = rows.astype(jnp.bfloat16)
    ones = iota((Z_PAD, LANES), 0) == ONES
    part = iota((GOT, 128), 0) & 7
    exact = (part >= 4) & (iota((GOT, 128), 1) >= MEAS_AT - 128)
    for v in range(VIEWS):
        got = recv_ref[v * GOT : (v + 1) * GOT, :]
        first = got.astype(jnp.bfloat16).astype(jnp.float32)
        second = (got - first).astype(jnp.bfloat16).astype(jnp.float32)
        parts = (
            first,
            jnp.where(exact, second, first),
            jnp.where(exact, got - first - second, first),
        )
        sums = jnp.dot(
            rows,
            jnp.concatenate(parts, axis=0).astype(jnp.bfloat16),
            preferred_element_type=jnp.float32,
        )
        smeared = jnp.concatenate((sums[0:Z_PAD], sums[Z_PAD : 2 * Z_PAD]), axis=1)
        sm_ref[v] = jnp.where(ones, 1.0, smeared).astype(jnp.bfloat16).astype(jnp.float32)
        own = pltpu.roll(sums[2 * Z_PAD :], 256 - MEAS_AT, 1)
        res_ref[v] = own[0:ROWS_DEV, 0:COLS_DEV]


def windows(sm_ref, offsets):
    lane = iota((Z_PAD, 128), 1)
    placed = []
    for v in range(VIEWS):
        at = PLACE[v] & 127
        shift = (at - offsets[v]) & 127
        low = pltpu.roll(sm_ref[v, :, 0:128], shift, 1)
        high = pltpu.roll(sm_ref[v, :, 128:256], shift, 1)
        placed.append(jnp.where(lane < at + 128 - offsets[v], low, high))
    first = jnp.where(lane < 40, placed[0], jnp.where(lane < 80, placed[1], placed[2]))
    first = jnp.where(lane < 120, first, 0.0)
    second = jnp.where(lane < 40, placed[3], jnp.where(lane < 80, placed[4], 0.0))
    both = jnp.concatenate((first, second), axis=1)
    return both.astype(jnp.bfloat16)[:, 0:DEPTH]


def backward(w_ref, sm_ref, table_ref, old, store, subset, gz):
    zi = slice_of(iota((Z_PAD, LANES), 0), gz)
    inside = iota((Z_PAD, LANES), 0) < Z_ALL
    total = jnp.sum(jnp.where(inside, hat(iota((Z_PAD, LANES), 1), zi), 0.0), axis=1, keepdims=True)

    for tile in range(TILES):
        offsets = tile_offsets(table_ref, subset, tile)
        back = jnp.dot(
            windows(sm_ref, offsets), w_ref[tile], preferred_element_type=jnp.float32
        )
        norm = total * back[ONES : ONES + 1, :]
        store(tile, old(tile), back / jnp.maximum(norm, 1.0))


def swapped(rows, index, turn, axis):
    for d in (4, 2, 1):
        high = (index & d) != 0
        new = list(rows)
        for i in range(8):
            if i & d == 0:
                a, b = (rows[i], rows[i + d])
                new[i] = jnp.where(high, pltpu.roll(b, turn * d, axis), a)
                new[i + d] = jnp.where(high, b, pltpu.roll(a, turn * (8 - d), axis))
        rows = new
    return rows


def swap_blocks(rows):
    return swapped(rows, iota((8, 128), 1) >> 4, 16, 1)


def swap_sublanes(rows):
    return swapped(rows, iota((8, 128), 0), 1, 0)


def relay(read, out_ref, unrolled):
    def step(xb, nothing):
        for half in range(2):
            for b in range(2):
                x = xb * TILE + half * 8
                rows = swap_sublanes([read(b * 8 + z, x) for z in range(8)])
                for q, block in enumerate(swap_blocks(rows)):
                    out_ref[
                        xb * TILES_Y + q, b * 8 : b * 8 + 8, half * 128 : half * 128 + 128
                    ] = block
        return nothing

    if unrolled:
        for xb in range(X_DEV // TILE):
            step(xb, 0)
    else:
        lax.fori_loop(0, X_DEV // TILE, step, 0)


def pack_kernel(
    vol_hbm, meas_hbm, order_hbm, up_ref, down_ref, vol_ref, meas_ref, order_ref, row_ref, sems
):
    copies = [
        pltpu.make_async_copy(vol_hbm, vol_ref, sems.at[0]),
        pltpu.make_async_copy(meas_hbm, meas_ref, sems.at[1]),
        pltpu.make_async_copy(order_hbm, order_ref, sems.at[2]),
    ]
    for copy in copies:
        copy.start()
    row_ref[...] = jnp.zeros_like(row_ref)
    for copy in copies:
        copy.wait()
    for out_ref, z, inner, r in (
        (up_ref, Z_DEV - Z_HALO, Z_HALO // 2, ROWS_DEV - M_HALO),
        (down_ref, 0, 0, 0),
    ):
        slices = vol_ref[z * X_DEV : (z + Z_HALO) * X_DEV, :]
        rounded = slices.astype(jnp.bfloat16)
        out_ref[0:HALO_ROWS, :] = rounded
        left = slices - rounded.astype(jnp.float32)
        at = inner * X_DEV
        out_ref[HALO_ROWS:EDGE_AT, :] = left[at : at + INNER_ROWS].astype(jnp.bfloat16)
        for v in range(VIEWS):
            at = (v * ROWS_DEV + r) * SUBSETS
            row_ref[:, 0:COLS_DEV] = meas_ref[at : at + SUBSETS * M_HALO, :]
            row = row_ref[...]
            rounded = row.astype(jnp.bfloat16).astype(jnp.float32)
            both = pltpu.roll(rounded, MEAS_AT - 128, 1)
            both = both + pltpu.roll(row - rounded, MEAS_AT - 128 - COLS_DEV, 1)
            at = EDGE_AT + v * SUBSETS * M_HALO
            out_ref[at : at + SUBSETS * M_HALO, :] = both.astype(jnp.bfloat16)


def prepare_kernel(
    order_ref, vol_ref, meas_ref,
    w0_ref, w1_ref, own_ref, mown_ref, table_ref, u_ref, flat_ref, sem,
):
    xy = lax.axis_index("xy")
    chosen = iota((TABLE[0], ANGLES), 0) == iota((TABLE[0], ANGLES), 1)
    chosen = jnp.where(chosen, order_ref[...].astype(jnp.float32), 0.0)
    chosen = jnp.broadcast_to(jnp.sum(chosen, axis=1, keepdims=True), TABLE)
    angles = 2.0 * math.pi * chosen / ANGLES
    cosine = jnp.cos(angles)
    sine = jnp.sin(angles)
    flat_ref[...], own = fill_table(cosine, sine, xy)
    copy = pltpu.make_async_copy(flat_ref, table_ref, sem)
    copy.start()
    relay(
        lambda z, x: vol_ref[pl.ds(pl.multiple_of(z * X_DEV + x, 8), 8), :], own_ref, False
    )
    mown_ref[...] = jnp.zeros_like(mown_ref)
    for s in range(SUBSETS):
        for v in range(VIEWS):
            for at, count in ((0, 8), (8, 8), (16, 4)):
                rows = meas_ref[pl.ds((v * ROWS_DEV + at) * 2 + s, count, stride=2), :]
                mown_ref[s, v, at : at + count, MEAS_AT - 128 : 128] = rows
    copy.wait()
    for subset, w_ref in ((0, w0_ref), (1, w1_ref)):
        positions(u_ref, cosine, sine, own, subset, xy)

        def step(tt, nothing):
            for t in range(8):
                tile = tt * 8 + t
                w_ref[tile] = weights(u_ref, tile_offsets(table_ref, subset, tile), tile)
            return nothing

        lax.fori_loop(0, TILES // 8, step, 0)


def first_kernel(
    table_ref, w_ref, own_ref, mown_ref, low_ref, high_ref,
    out_ref, side_ref, m1_ref, raw_ref, m0_ref, edge_ref, *acc_refs,
):
    gz = lax.axis_index("gz")
    for side, sent_ref in enumerate((low_ref, high_ref)):
        edge = sent_ref[EDGE_AT:SENT_ROWS, :].astype(jnp.float32)
        edge = edge + pltpu.roll(edge, COLS_DEV, 1)
        edge_ref[side] = jnp.where(iota(edge.shape, 1) >= MEAS_AT - 128, edge, 0.0)

    def read(z, x):
        if z >= 2 * Z_HALO:
            return jnp.full((8, NY), 1.0 if z == ONES - Z_DEV else 0.0, jnp.float32)
        sent_ref, inner = (low_ref, Z_HALO // 2) if z < Z_HALO else (high_ref, 0)
        z = z % Z_HALO
        at = z * X_DEV + x
        rows = sent_ref[at : at + 8, :].astype(jnp.float32)
        if inner <= z < inner + Z_HALO // 2:
            at = at + HALO_ROWS - inner * X_DEV
            rows = rows + sent_ref[at : at + 8, :].astype(jnp.float32)
        return rows

    relay(read, side_ref, True)
    for s, m_ref in ((0, m0_ref), (1, m1_ref)):
        per = ROWS_PER[s]
        m_ref[...] = jnp.zeros_like(m_ref)
        for v in range(VIEWS):
            edge = pl.ds(v * 2 * M_HALO + s, M_HALO, stride=2)
            high = edge_ref[1, edge, :]
            joined = jnp.concatenate(
                (
                    edge_ref[0, edge, :],
                    mown_ref[s, v, 0:16, :],
                    jnp.concatenate((mown_ref[s, v, 16:20, :], high[0:4]), axis=0),
                    jnp.concatenate((high[4:8], jnp.zeros((4, 128), jnp.float32)), axis=0),
                ),
                axis=0,
            )
            raw_ref[s, v] = pltpu.roll(
                joined, M_ROWS + ((gz + 1) >> 1) - (M_HALO - ROWS_BELOW[s]), 0
            )
            for group in range(GROUPS):
                at = group * 2 * (per + 1) + per + 1
                m_ref[v, at : at + per, :] = raw_ref[s, v, group * per : (group + 1) * per, :]

    def slices(tile):
        return jnp.concatenate((own_ref[tile], side_ref[tile]), axis=0).astype(jnp.bfloat16)

    forward(w_ref, slices, acc_refs, m0_ref, table_ref, out_ref, 0, gz)


def middle_kernel(
    table_ref, recv_ref, own_ref, side_ref, m_ref, w0_ref, w1_ref,
    out_ref, new_ref, sm_ref, vb_ref, *acc_refs,
):
    gz = lax.axis_index("gz")
    smear(recv_ref, sm_ref, gz)
    ones = iota((Z_PAD, VOXELS), 0) == ONES

    def old(tile):
        return jnp.concatenate((own_ref[tile], side_ref[tile]), axis=0)

    def store(tile, old, change):
        new = jnp.where(ones, 1.0, old + change)
        new_ref[tile] = new[0:Z_DEV]
        vb_ref[tile] = new.astype(jnp.bfloat16)

    backward(w0_ref, sm_ref, table_ref, old, store, 0, gz)
    forward(w1_ref, lambda tile: vb_ref[tile], acc_refs, m_ref, table_ref, out_ref, 1, gz)


def last_kernel(
    table_ref, recv_ref, old_ref, w_ref,
    out_ref, res_ref, sm_ref, new_ref, block_ref, own_ref, sems,
):
    gz = lax.axis_index("gz")
    smear_last(recv_ref, sm_ref, own_ref, gz)
    copies = [pltpu.make_async_copy(own_ref, res_ref, sems.at[X_DEV // TILE])]
    copies[0].start()

    def store(tile, old, change):
        new_ref[tile] = old + change[0:Z_DEV]

    backward(w_ref, sm_ref, table_ref, lambda tile: old_ref[tile], store, 1, gz)
    for xb in range(X_DEV // TILE):
        for half in range(2):
            for b in range(Z_DEV // 8):
                blocks = [
                    new_ref[xb * TILES_Y + q, b * 8 : b * 8 + 8, half * 128 : half * 128 + 128]
                    for q in range(TILES_Y)
                ]
                x = xb * TILE + half * 8
                for z, row in enumerate(swap_sublanes(swap_blocks(blocks))):
                    block_ref[b * 8 + z, x : x + 8, :] = row
        columns = pl.ds(xb * TILE, TILE)
        copies.append(
            pltpu.make_async_copy(
                block_ref.at[:, columns, :], out_ref.at[:, columns, :], sems.at[xb]
            )
        )
        copies[-1].start()
    for copy in copies:
        copy.wait()


def owner_kernel(table_ref, recv_ref, out_ref, acc_ref, mea_ref, *sum_refs, subset):
    gz = lax.axis_index("gz")
    xy = lax.axis_index("xy")
    view = jnp.minimum(xy // GROUPS, VIEWS - 1)
    group = xy % GROUPS
    at = subset * VIEWS + view
    per = ROWS_PER[subset]
    half = per + 1
    lane = iota((8, 128), 1)
    for sum_ref in sum_refs:
        sum_ref[...] = jnp.zeros_like(sum_ref)
    mea_ref[...] = jnp.zeros_like(mea_ref)
    end = N_XY * 2 * half - 8

    def upper(s):
        row = s * 2 * half + half
        last = recv_ref[min(row, end) : min(row, end) + 8, :]
        return pltpu.roll(last, 8 - (row - end), 0) if row > end else last

    for s in range(N_XY):
        column = s * COLS_DEV
        own = jnp.where(lane >= MEAS_AT - 128, upper(s), 0.0)
        own = pltpu.roll(own, (column + 256 - MEAS_AT) % 128, 1)
        block = column // 128 * 128
        offset = column - block
        mea_ref[:, block : block + 128] += jnp.where(lane >= offset, own, 0.0)
        if offset + COLS_DEV > 128:
            mea_ref[:, block + 128 : block + 256] += jnp.where(lane < offset, own, 0.0)
    for s in range(N_XY):
        base = pl.multiple_of(table_ref[at, s], 128)
        shift = table_ref[at, SHIFT_AT + s]
        row = s * 2 * half
        low = pltpu.roll(recv_ref[row : row + 8, :], shift, 1)
        high = pltpu.roll(jnp.where(lane < WIN - 128, upper(s), 0.0), shift, 1)
        wrapped = lane < shift
        part_ref = sum_refs[s % SUMS]
        part_ref[:, pl.ds(base, 128)] += jnp.where(wrapped, 0.0, low)
        part_ref[:, pl.ds(base + 128, 128)] += jnp.where(wrapped, low, high)
        part_ref[:, pl.ds(base + 256, 128)] += jnp.where(wrapped, high, 0.0)
    slot = iota((8, NZ), 0)
    row = first_row(gz, subset) + group * per + slot
    ray_rows = jnp.where(slot < per, hat(row, iota((8, NZ), 1)), 0.0)
    ray_rows = jnp.sum(ray_rows, axis=1, keepdims=True)
    sums = sum_refs[0][...]
    for part_ref in sum_refs[1:]:
        sums = sums + part_ref[...]
    totals = sums[per : per + 1, :]
    acc_ref[...] = mea_ref[...] - sums / jnp.maximum(ray_rows * totals, 1.0)
    for t in range(N_XY):
        base = pl.multiple_of(table_ref[at, t], 128)
        shift = table_ref[at, SHIFT_AT + t]
        back = (128 - shift) & 127
        a = pltpu.roll(acc_ref[:, pl.ds(base, 128)], back, 1)
        b = pltpu.roll(acc_ref[:, pl.ds(base + 128, 128)], back, 1)
        c = pltpu.roll(acc_ref[:, pl.ds(base + 256, 128)], back, 1)
        kept = lane < 128 - shift
        low = jnp.where(kept, a, b)
        high = jnp.where(kept, b, c)
        if subset == 0:
            other = pltpu.roll(high, COLS_DEV, 1)
            even = jnp.where(
                slot == 5,
                pltpu.roll(high, 5, 0),
                jnp.where(slot == 6, pltpu.roll(high, 4, 0), pltpu.roll(high, 3, 0)),
            )
            odd = jnp.where(slot == 5, pltpu.roll(other, 4, 0), pltpu.roll(other, 3, 0))
            rest = jnp.where(lane < COLS_DEV, even, odd)
            out_ref[t] = jnp.where(slot < 5, low, rest).astype(jnp.bfloat16)
            continue
        column = t * COLS_DEV
        block = column // 128 * 128
        offset = column - block
        turn = (MEAS_AT - 128 - offset) % 128
        own = pltpu.roll(acc_ref[:, block : block + 128], turn, 1)
        if offset + COLS_DEV > 128:
            more = pltpu.roll(acc_ref[:, block + 128 : block + 256], turn, 1)
            own = jnp.where(lane < MEAS_AT - offset, own, more)
        high = jnp.where(lane >= MEAS_AT - 128, own, high)
        out_ref[t * 8 : (t + 1) * 8, :] = jnp.where(slot < 4, low, pltpu.roll(high, 4, 0))


def call(kernel, inputs, outs, scratch, name):
    vmem = pl.BlockSpec(memory_space=pltpu.VMEM)
    smem = pl.BlockSpec(memory_space=pltpu.SMEM)
    anywhere = pl.BlockSpec(memory_space=pl.ANY)

    def spec(x):
        if x.dtype == jnp.int32:
            return smem
        return anywhere if isinstance(x, jax.ShapeDtypeStruct) else vmem

    inputs = [
        x if x.dtype == jnp.int32 else pltpu.with_memory_space_constraint(x, pltpu.VMEM)
        for x in inputs
    ]
    return pl.pallas_call(
        kernel,
        in_specs=[spec(x) for x in inputs],
        out_specs=[spec(x) for x in outs],
        out_shape=outs,
        scratch_shapes=scratch,
        compiler_params=pltpu.CompilerParams(vmem_limit_bytes=12 * 1024 * 1024),
        name=name,
    )(*inputs)


def exchanged(parts, shape):
    sent = lax.all_to_all(
        parts.reshape(shape), "xy", split_axis=0, concat_axis=0, tiled=True
    )
    return sent.reshape(parts.shape)


def local(volume, measured, view_order):
    f32 = jnp.float32
    bf16 = jnp.bfloat16
    vmem = pltpu.VMEM
    flat = volume.reshape(Z_DEV * X_DEV, NY)
    order = view_order.reshape(1, ANGLES)
    rows = measured.transpose(1, 2, 0, 3).reshape(VIEWS * ROWS_DEV * SUBSETS, COLS_DEV)
    made = vmem((TILES, DEPTH, VOXELS), bf16)
    slices = vmem((TILES, Z_DEV, VOXELS), f32)
    sm_scratch = vmem((VIEWS, Z_PAD, LANES), f32)
    acc_scratch = [vmem((WIN, 128), f32)] * VIEWS
    row_scratch = vmem((8, FULL), f32)
    owner_scratch = [row_scratch] * (2 + SUMS)

    sent = vmem((SENT_ROWS, 128), bf16)
    hbm = pl.BlockSpec(memory_space=pltpu.HBM)
    up, down, flat, rows, order = pl.pallas_call(
        pack_kernel,
        in_specs=[hbm] * 3,
        out_specs=[pl.BlockSpec(memory_space=vmem)] * 5,
        out_shape=[
            sent, sent, vmem(flat.shape, f32), vmem(rows.shape, f32), vmem((1, ANGLES), jnp.int32)
        ],
        scratch_shapes=[vmem((SUBSETS * M_HALO, 128), f32), pltpu.SemaphoreType.DMA((3,))],
        compiler_params=pltpu.CompilerParams(vmem_limit_bytes=12 * 1024 * 1024),
        name="pack",
    )(*(pltpu.with_memory_space_constraint(x, pltpu.HBM) for x in (flat, rows, order)))
    next_up = [(i, (i + 1) % N_GZ) for i in range(N_GZ)]
    low = lax.ppermute(up, "gz", next_up)
    high = lax.ppermute(down, "gz", [(j, i) for i, j in next_up])
    w0, w1, own, mown, table = pl.pallas_call(
        prepare_kernel,
        in_specs=[pl.BlockSpec(memory_space=vmem)] * 3,
        out_specs=[pl.BlockSpec(memory_space=m) for m in (vmem, vmem, vmem, vmem, pltpu.SMEM)],
        out_shape=[
            made, made, slices, vmem((SUBSETS, VIEWS, 24, 128), f32), pltpu.SMEM(TABLE, jnp.int32)
        ],
        scratch_shapes=[
            vmem((VIEWS, TILES, VOXELS), f32), vmem(TABLE, jnp.int32), pltpu.SemaphoreType.DMA
        ],
        compiler_params=pltpu.CompilerParams(vmem_limit_bytes=12 * 1024 * 1024),
        name="prepare",
    )(*(pltpu.with_memory_space_constraint(x, vmem) for x in (order, flat, rows)))
    partial, side, m1 = call(
        first_kernel,
        (table, w0, own, mown, low, high),
        [vmem((N_XY * 12, 128), f32), slices, vmem((VIEWS, 64, 128), f32)],
        [
            vmem((SUBSETS, VIEWS, M_ROWS, 128), f32),
            vmem((VIEWS, 72, 128), f32),
            vmem((2, EDGE_ROWS, 128), f32),
            *acc_scratch,
        ],
        "first",
    )
    (rounded,) = call(
        functools.partial(owner_kernel, subset=0),
        (table, exchanged(partial, (N_XY, 3, 4, 128))),
        [vmem((N_XY, 8, 128), bf16)],
        owner_scratch,
        "owner_a",
    )
    partial, new = call(
        middle_kernel,
        (table, exchanged(rounded, rounded.shape), own, side, m1, w0, w1),
        [vmem((N_XY * 10, 128), f32), slices],
        [sm_scratch, vmem((TILES, Z_PAD, VOXELS), bf16), *acc_scratch],
        "middle",
    )
    (final,) = call(
        functools.partial(owner_kernel, subset=1),
        (table, exchanged(partial, (N_XY, 5, 2, 128))),
        [vmem((N_XY * 8, 128), f32)],
        owner_scratch,
        "owner_b",
    )
    volume_out, residual = call(
        last_kernel,
        (table, exchanged(final, (N_XY, 8, 128)), new, w1),
        [
            jax.ShapeDtypeStruct(VOLUME, f32),
            jax.ShapeDtypeStruct((VIEWS, ROWS_DEV, COLS_DEV), f32),
        ],
        [
            sm_scratch,
            slices,
            vmem(VOLUME, f32),
            vmem((VIEWS, ROWS_DEV, COLS_DEV), f32),
            pltpu.SemaphoreType.DMA((X_DEV // TILE + 1,)),
        ],
        "last",
    )
    return volume_out, residual


def solution(mesh):
    in_specs = (P("gz", "xy", None), P(None, None, "gz", "xy"), P())
    out_specs = (P("gz", "xy", None), P(None, "gz", "xy"))
    return jax.shard_map(local, mesh=mesh, in_specs=in_specs, out_specs=out_specs, check_vma=False)
```

```python
import functools
import math

import jax
import jax.numpy as jnp
from jax import lax
from jax.experimental import pallas as pl
from jax.experimental.pallas import tpu as pltpu
from jax.sharding import PartitionSpec as P

Z_DEV = 16
X_DEV = 48
NY = 128
COLS_DEV = 48
ROWS_DEV = 20
VIEWS = 5
SUBSETS = 2
ANGLES = 48
N_XY = 32
N_GZ = 8
NX = X_DEV * N_XY
NZ = Z_DEV * N_GZ
DR = ROWS_DEV * N_GZ
DC = COLS_DEV * N_XY

WIN = 176
LANES = 256
MEAS_AT = LANES - COLS_DEV
Z_HALO = 6
Z_ALL = Z_DEV + 2 * Z_HALO
ONES = Z_ALL
Z_PAD = 32
GROUPS = 6
GOT = GROUPS * 8
ROWS_PER = (5, 4)
ROWS_BELOW = (3, 0)
M_HALO = 8
M_ROWS = 40
FULL = 15 * 128
SUMS = 4
TILE = 16
TILES_Y = NY // TILE
TILES = X_DEV // TILE * TILES_Y
VOXELS = TILE * TILE
COLS_TILE = 40
VOLUME = (Z_DEV, X_DEV, NY)
PLACE = (0, 40, 80, 128, 168)
DEPTH = 208
HALO_ROWS = Z_HALO * X_DEV
INNER_ROWS = HALO_ROWS // 2
EDGE_AT = HALO_ROWS + INNER_ROWS
EDGE_ROWS = SUBSETS * VIEWS * M_HALO
SENT_ROWS = EDGE_AT + EDGE_ROWS
TABLE = (16, 128)
SHIFT_AT = 32
TILE_AT = 64


def iota(shape, dim):
    return lax.broadcasted_iota(jnp.int32, shape, dim)


def slice_of(i, gz):
    low = Z_DEV * gz - Z_HALO + (i - Z_DEV)
    high = Z_DEV * gz + Z_DEV + (i - Z_DEV - Z_HALO)
    return jnp.where(i < Z_DEV, Z_DEV * gz + i, jnp.where(i < Z_DEV + Z_HALO, low, high))


def hat(row, z):
    position = (DR - 1) / 2.0 + 0.96 * (DR / NZ) * (z.astype(jnp.float32) - (NZ - 1) / 2.0)
    value = jnp.maximum(0.0, 1.0 - jnp.abs(position - row.astype(jnp.float32)) / 2.0)
    ok = (row >= 0) & (row < DR) & (z >= 0) & (z < NZ)
    return jnp.where(ok, value, 0.0)


def first_row(gz, subset):
    return ROWS_DEV * gz - ROWS_BELOW[subset] - ((gz + 1) >> 1)


def slot_weights(group, slot, i, gz, subset):
    per = ROWS_PER[subset]
    row = first_row(gz, subset) + group * per + slot
    return jnp.where((slot < per) & (i < Z_ALL), hat(row, slice_of(i, gz)), 0.0)


def tile_offsets(table_ref, subset, tile):
    return [
        pl.multiple_of(table_ref[subset * VIEWS + v, TILE_AT + tile], 8) for v in range(VIEWS)
    ]


def coordinate(x, y, cosine, sine):
    xc = x - (NX - 1) / 2.0
    yc = y - (NY - 1) / 2.0
    source = 2.0 * NX
    along = xc * cosine + yc * sine
    depth = yc * cosine - xc * sine
    return (DC - 1) / 2.0 + 0.9 * (DC / NX) * along * source / (source + depth)


def fill_table(cosine, sine, xy):
    lane = iota(TABLE, 1)
    tile = lane - TILE_AT
    is_tile = lane >= TILE_AT
    strip = lane & (N_XY - 1)
    x = jnp.where(is_tile, xy * X_DEV + (tile >> 3) * TILE, strip * X_DEV).astype(jnp.float32)
    y = jnp.where(is_tile, (tile & 7) * TILE, 0).astype(jnp.float32)
    dx = jnp.where(is_tile, TILE - 1.0, X_DEV - 1.0)
    dy = jnp.where(is_tile, TILE - 1.0, NY - 1.0)
    least = jnp.minimum(
        jnp.minimum(coordinate(x, y, cosine, sine), coordinate(x + dx, y, cosine, sine)),
        jnp.minimum(coordinate(x, y + dy, cosine, sine), coordinate(x + dx, y + dy, cosine, sine)),
    )
    least = jnp.floor(least).astype(jnp.int32)
    start = least - 2
    own = jnp.sum(jnp.where(lane == xy, start, 0).astype(jnp.float32), axis=1, keepdims=True)
    tiles = jnp.maximum(least - 1 - own.astype(jnp.int32), 0) & ~7
    table = jnp.where(lane < SHIFT_AT, start & ~127, start & 127)
    return jnp.where(is_tile, tiles, table), own


def positions(u_ref, cosine, sine, own, subset, xy):
    t = iota((TILES, VOXELS), 0)
    l = iota((TILES, VOXELS), 1)
    x = ((t >> 3) * TILE + (l >> 4) + xy * X_DEV).astype(jnp.float32)
    y = ((t & 7) * TILE + (l & 15)).astype(jnp.float32)
    for v in range(VIEWS):
        at = subset * VIEWS + v
        u = coordinate(x, y, cosine[at : at + 1, 0:1], sine[at : at + 1, 0:1])
        u_ref[v] = u - own[at : at + 1, :]


def weights(u_ref, offsets, tile):
    c = iota((COLS_TILE, VOXELS), 0).astype(jnp.float32)
    pieces = []
    for v in range(VIEWS):
        u = u_ref[v, pl.ds(tile, 1), :] - offsets[v].astype(jnp.float32)
        pieces.append(jnp.maximum(0.0, 1.0 - jnp.abs(u - c)))
    pieces.insert(3, jnp.zeros((8, VOXELS), jnp.float32))
    return jnp.concatenate(pieces, axis=0).astype(jnp.bfloat16)


def forward(w_ref, slices, acc_refs, m_ref, table_ref, out_ref, subset, gz):
    for acc_ref in acc_refs:
        acc_ref[...] = jnp.zeros_like(acc_ref)
    for tile in range(TILES):
        offsets = tile_offsets(table_ref, subset, tile)
        part = lax.dot_general(
            w_ref[tile],
            jnp.concatenate([slices(tile)] * 4, axis=0),
            (((1,), (1,)), ((), ())),
            preferred_element_type=jnp.float32,
        )
        for v in range(VIEWS):
            acc_refs[v][pl.ds(offsets[v], COLS_TILE), :] += part[PLACE[v] : PLACE[v] + COLS_TILE]
    per = ROWS_PER[subset]
    half = per + 1
    size = GROUPS * 2 * half
    k = iota((size, 128), 0)
    lane = iota((size, 128), 1)
    i = lane & (Z_PAD - 1)
    group = (k * 43) >> 9 if half == 6 else (k * 205) >> 11
    slot = k - group * 2 * half
    is_low = slot < half
    slot = jnp.where(is_low, slot, slot - half)
    rows = slot_weights(group, slot, i, gz, subset)
    rows = jnp.where((slot == per) & (i == ONES), 1.0, rows)
    rounded = rows.astype(jnp.bfloat16).astype(jnp.float32)
    rows = jnp.where(lane < 2 * Z_PAD, rounded, rows - rounded).astype(jnp.bfloat16)
    left_over = (iota((WIN, 128), 1) & Z_PAD) != 0
    used = GROUPS * VIEWS * 2 * half
    out_ref[used:, :] = jnp.zeros((out_ref.shape[0] - used, 128), jnp.float32)
    for v in range(VIEWS):
        sums = acc_refs[v][...]
        rounded = sums.astype(jnp.bfloat16).astype(jnp.float32)
        sums = jnp.where(left_over, sums - rounded, rounded).astype(jnp.bfloat16)
        sums = lax.dot_general(
            rows, sums, (((1,), (1,)), ((), ())), preferred_element_type=jnp.float32
        )
        high = jnp.concatenate(
            (sums[:, 128:WIN], jnp.zeros((size, LANES - WIN), jnp.float32)), axis=1
        )
        part = jnp.where(is_low, sums[:, 0:128], high) + m_ref[v, 0:size, :]
        out_ref[v * size : (v + 1) * size, :] = part


def three_parts(x, third):
    first = x.astype(jnp.bfloat16).astype(jnp.float32)
    second = (x - first).astype(jnp.bfloat16).astype(jnp.float32)
    part = jnp.where(third == 0, first, jnp.where(third == 1, second, x - first - second))
    return part.astype(jnp.bfloat16)


def smear(recv_ref, sm_ref, gz):
    i = iota((3 * Z_PAD, 3 * GOT), 0)
    k = iota((3 * Z_PAD, 3 * GOT), 1)
    third = (k >= GOT).astype(jnp.int32) + (k >= 2 * GOT).astype(jnp.int32)
    k = k - GOT * third
    part = k & 7
    block = i >> 5
    slot = jnp.where(block == 0, part, 2 * (part - 5) + block - 1)
    rows = slot_weights(k >> 3, slot, i & (Z_PAD - 1), gz, 0)
    rows = three_parts(jnp.where((block == 0) == (part < 5), rows, 0.0), third)
    ones = iota((Z_PAD, LANES), 0) == ONES
    for v in range(VIEWS):
        got = recv_ref[v * GROUPS : (v + 1) * GROUPS].astype(jnp.float32)
        got = got.reshape(GOT, 128).astype(jnp.bfloat16)
        sums = jnp.dot(
            rows, jnp.concatenate((got, got, got), axis=0), preferred_element_type=jnp.float32
        )
        high = sums[Z_PAD : 2 * Z_PAD] + pltpu.roll(sums[2 * Z_PAD :], 128 - COLS_DEV, 1)
        smeared = jnp.concatenate((sums[0:Z_PAD], high), axis=1)
        sm_ref[v] = jnp.where(ones, 1.0, smeared).astype(jnp.bfloat16).astype(jnp.float32)


def smear_last(recv_ref, sm_ref, res_ref, gz):
    size = 2 * Z_PAD + 24
    i = iota((size, 3 * GOT), 0)
    k = iota((size, 3 * GOT), 1)
    third = (k >= GOT).astype(jnp.int32) + (k >= 2 * GOT).astype(jnp.int32)
    k = k - GOT * third
    part = k & 7
    rows = slot_weights(k >> 3, part & 3, i & (Z_PAD - 1), gz, 1)
    rows = three_parts(jnp.where((part >= 4) == (i >= Z_PAD), rows, 0.0), third)
    j = i - 2 * Z_PAD + ((gz + 1) >> 1)
    picked = jnp.where(k == ((j >> 2) << 3) + 4 + (j & 3), 1.0, 0.0).astype(jnp.bfloat16)
    rows = jnp.where(i >= 2 * Z_PAD, picked.astype(jnp.float32), rows.astype(jnp.float32))
    rows = rows.astype(jnp.bfloat16)
    ones = iota((Z_PAD, LANES), 0) == ONES
    part = iota((GOT, 128), 0) & 7
    exact = (part >= 4) & (iota((GOT, 128), 1) >= MEAS_AT - 128)
    for v in range(VIEWS):
        got = recv_ref[v * GOT : (v + 1) * GOT, :]
        first = got.astype(jnp.bfloat16).astype(jnp.float32)
        second = (got - first).astype(jnp.bfloat16).astype(jnp.float32)
        parts = (
            first,
            jnp.where(exact, second, first),
            jnp.where(exact, got - first - second, first),
        )
        sums = jnp.dot(
            rows,
            jnp.concatenate(parts, axis=0).astype(jnp.bfloat16),
            preferred_element_type=jnp.float32,
        )
        smeared = jnp.concatenate((sums[0:Z_PAD], sums[Z_PAD : 2 * Z_PAD]), axis=1)
        sm_ref[v] = jnp.where(ones, 1.0, smeared).astype(jnp.bfloat16).astype(jnp.float32)
        own = pltpu.roll(sums[2 * Z_PAD :], 256 - MEAS_AT, 1)
        res_ref[v] = own[0:ROWS_DEV, 0:COLS_DEV]


def windows(sm_ref, offsets):
    lane = iota((Z_PAD, 128), 1)
    placed = []
    for v in range(VIEWS):
        at = PLACE[v] & 127
        shift = (at - offsets[v]) & 127
        low = pltpu.roll(sm_ref[v, :, 0:128], shift, 1)
        high = pltpu.roll(sm_ref[v, :, 128:256], shift, 1)
        placed.append(jnp.where(lane < at + 128 - offsets[v], low, high))
    first = jnp.where(lane < 40, placed[0], jnp.where(lane < 80, placed[1], placed[2]))
    first = jnp.where(lane < 120, first, 0.0)
    second = jnp.where(lane < 40, placed[3], jnp.where(lane < 80, placed[4], 0.0))
    both = jnp.concatenate((first, second), axis=1)
    return both.astype(jnp.bfloat16)[:, 0:DEPTH]


def backward(w_ref, sm_ref, table_ref, old, store, subset, gz):
    zi = slice_of(iota((Z_PAD, LANES), 0), gz)
    inside = iota((Z_PAD, LANES), 0) < Z_ALL
    total = jnp.sum(jnp.where(inside, hat(iota((Z_PAD, LANES), 1), zi), 0.0), axis=1, keepdims=True)

    for tile in range(TILES):
        offsets = tile_offsets(table_ref, subset, tile)
        back = jnp.dot(
            windows(sm_ref, offsets), w_ref[tile], preferred_element_type=jnp.float32
        )
        norm = total * back[ONES : ONES + 1, :]
        store(tile, old(tile), back / jnp.maximum(norm, 1.0))


def swapped(rows, index, turn, axis):
    for d in (4, 2, 1):
        high = (index & d) != 0
        new = list(rows)
        for i in range(8):
            if i & d == 0:
                a, b = (rows[i], rows[i + d])
                new[i] = jnp.where(high, pltpu.roll(b, turn * d, axis), a)
                new[i + d] = jnp.where(high, b, pltpu.roll(a, turn * (8 - d), axis))
        rows = new
    return rows


def swap_blocks(rows):
    return swapped(rows, iota((8, 128), 1) >> 4, 16, 1)


def swap_sublanes(rows):
    return swapped(rows, iota((8, 128), 0), 1, 0)


def relay(read, out_ref, unrolled):
    def step(xb, nothing):
        for half in range(2):
            for b in range(2):
                x = xb * TILE + half * 8
                rows = swap_sublanes([read(b * 8 + z, x) for z in range(8)])
                for q, block in enumerate(swap_blocks(rows)):
                    out_ref[
                        xb * TILES_Y + q, b * 8 : b * 8 + 8, half * 128 : half * 128 + 128
                    ] = block
        return nothing

    if unrolled:
        for xb in range(X_DEV // TILE):
            step(xb, 0)
    else:
        lax.fori_loop(0, X_DEV // TILE, step, 0)


def pack_kernel(
    vol_hbm, meas_hbm, order_hbm, up_ref, down_ref, vol_ref, meas_ref, order_ref, row_ref, sems
):
    copies = [
        pltpu.make_async_copy(vol_hbm, vol_ref, sems.at[0]),
        pltpu.make_async_copy(meas_hbm, meas_ref, sems.at[1]),
        pltpu.make_async_copy(order_hbm, order_ref, sems.at[2]),
    ]
    for copy in copies:
        copy.start()
    row_ref[...] = jnp.zeros_like(row_ref)
    for copy in copies:
        copy.wait()
    for out_ref, z, inner, r in (
        (up_ref, Z_DEV - Z_HALO, Z_HALO // 2, ROWS_DEV - M_HALO),
        (down_ref, 0, 0, 0),
    ):
        slices = vol_ref[z * X_DEV : (z + Z_HALO) * X_DEV, :]
        rounded = slices.astype(jnp.bfloat16)
        out_ref[0:HALO_ROWS, :] = rounded
        left = slices - rounded.astype(jnp.float32)
        at = inner * X_DEV
        out_ref[HALO_ROWS:EDGE_AT, :] = left[at : at + INNER_ROWS].astype(jnp.bfloat16)
        for v in range(VIEWS):
            at = (v * ROWS_DEV + r) * SUBSETS
            row_ref[:, 0:COLS_DEV] = meas_ref[at : at + SUBSETS * M_HALO, :]
            row = row_ref[...]
            rounded = row.astype(jnp.bfloat16).astype(jnp.float32)
            both = pltpu.roll(rounded, MEAS_AT - 128, 1)
            both = both + pltpu.roll(row - rounded, MEAS_AT - 128 - COLS_DEV, 1)
            at = EDGE_AT + v * SUBSETS * M_HALO
            out_ref[at : at + SUBSETS * M_HALO, :] = both.astype(jnp.bfloat16)


def prepare_kernel(
    order_ref, vol_ref, meas_ref,
    w0_ref, w1_ref, own_ref, mown_ref, table_ref, u_ref, flat_ref, sem,
):
    xy = lax.axis_index("xy")
    chosen = iota((TABLE[0], ANGLES), 0) == iota((TABLE[0], ANGLES), 1)
    chosen = jnp.where(chosen, order_ref[...].astype(jnp.float32), 0.0)
    chosen = jnp.broadcast_to(jnp.sum(chosen, axis=1, keepdims=True), TABLE)
    angles = 2.0 * math.pi * chosen / ANGLES
    cosine = jnp.cos(angles)
    sine = jnp.sin(angles)
    flat_ref[...], own = fill_table(cosine, sine, xy)
    copy = pltpu.make_async_copy(flat_ref, table_ref, sem)
    copy.start()
    relay(
        lambda z, x: vol_ref[pl.ds(pl.multiple_of(z * X_DEV + x, 8), 8), :], own_ref, False
    )
    mown_ref[...] = jnp.zeros_like(mown_ref)
    for s in range(SUBSETS):
        for v in range(VIEWS):
            for at, count in ((0, 8), (8, 8), (16, 4)):
                rows = meas_ref[pl.ds((v * ROWS_DEV + at) * 2 + s, count, stride=2), :]
                mown_ref[s, v, at : at + count, MEAS_AT - 128 : 128] = rows
    copy.wait()
    for subset, w_ref in ((0, w0_ref), (1, w1_ref)):
        positions(u_ref, cosine, sine, own, subset, xy)

        def step(tt, nothing):
            for t in range(8):
                tile = tt * 8 + t
                w_ref[tile] = weights(u_ref, tile_offsets(table_ref, subset, tile), tile)
            return nothing

        lax.fori_loop(0, TILES // 8, step, 0)


def first_kernel(
    table_ref, w_ref, own_ref, mown_ref, low_ref, high_ref,
    out_ref, side_ref, m1_ref, raw_ref, m0_ref, edge_ref, *acc_refs,
):
    gz = lax.axis_index("gz")
    for side, sent_ref in enumerate((low_ref, high_ref)):
        edge = sent_ref[EDGE_AT:SENT_ROWS, :].astype(jnp.float32)
        edge = edge + pltpu.roll(edge, COLS_DEV, 1)
        edge_ref[side] = jnp.where(iota(edge.shape, 1) >= MEAS_AT - 128, edge, 0.0)

    def read(z, x):
        if z >= 2 * Z_HALO:
            return jnp.full((8, NY), 1.0 if z == ONES - Z_DEV else 0.0, jnp.float32)
        sent_ref, inner = (low_ref, Z_HALO // 2) if z < Z_HALO else (high_ref, 0)
        z = z % Z_HALO
        at = z * X_DEV + x
        rows = sent_ref[at : at + 8, :].astype(jnp.float32)
        if inner <= z < inner + Z_HALO // 2:
            at = at + HALO_ROWS - inner * X_DEV
            rows = rows + sent_ref[at : at + 8, :].astype(jnp.float32)
        return rows

    relay(read, side_ref, True)
    for s, m_ref in ((0, m0_ref), (1, m1_ref)):
        per = ROWS_PER[s]
        m_ref[...] = jnp.zeros_like(m_ref)
        for v in range(VIEWS):
            edge = pl.ds(v * 2 * M_HALO + s, M_HALO, stride=2)
            high = edge_ref[1, edge, :]
            joined = jnp.concatenate(
                (
                    edge_ref[0, edge, :],
                    mown_ref[s, v, 0:16, :],
                    jnp.concatenate((mown_ref[s, v, 16:20, :], high[0:4]), axis=0),
                    jnp.concatenate((high[4:8], jnp.zeros((4, 128), jnp.float32)), axis=0),
                ),
                axis=0,
            )
            raw_ref[s, v] = pltpu.roll(
                joined, M_ROWS + ((gz + 1) >> 1) - (M_HALO - ROWS_BELOW[s]), 0
            )
            for group in range(GROUPS):
                at = group * 2 * (per + 1) + per + 1
                m_ref[v, at : at + per, :] = raw_ref[s, v, group * per : (group + 1) * per, :]

    def slices(tile):
        return jnp.concatenate((own_ref[tile], side_ref[tile]), axis=0).astype(jnp.bfloat16)

    forward(w_ref, slices, acc_refs, m0_ref, table_ref, out_ref, 0, gz)


def middle_kernel(
    table_ref, recv_ref, own_ref, side_ref, m_ref, w0_ref, w1_ref,
    out_ref, new_ref, sm_ref, vb_ref, *acc_refs,
):
    gz = lax.axis_index("gz")
    smear(recv_ref, sm_ref, gz)
    ones = iota((Z_PAD, VOXELS), 0) == ONES

    def old(tile):
        return jnp.concatenate((own_ref[tile], side_ref[tile]), axis=0)

    def store(tile, old, change):
        new = jnp.where(ones, 1.0, old + change)
        new_ref[tile] = new[0:Z_DEV]
        vb_ref[tile] = new.astype(jnp.bfloat16)

    backward(w0_ref, sm_ref, table_ref, old, store, 0, gz)
    forward(w1_ref, lambda tile: vb_ref[tile], acc_refs, m_ref, table_ref, out_ref, 1, gz)


def last_kernel(
    table_ref, recv_ref, old_ref, w_ref,
    out_ref, res_ref, sm_ref, new_ref, block_ref, own_ref, sems,
):
    gz = lax.axis_index("gz")
    smear_last(recv_ref, sm_ref, own_ref, gz)
    copies = [pltpu.make_async_copy(own_ref, res_ref, sems.at[X_DEV // TILE])]
    copies[0].start()

    def store(tile, old, change):
        new_ref[tile] = old + change[0:Z_DEV]
        xb = tile // TILES_Y
        if tile % TILES_Y < TILES_Y - 1:
            return
        for half in range(2):
            for b in range(Z_DEV // 8):
                blocks = [
                    new_ref[xb * TILES_Y + q, b * 8 : b * 8 + 8, half * 128 : half * 128 + 128]
                    for q in range(TILES_Y)
                ]
                x = xb * TILE + half * 8
                for z, row in enumerate(swap_sublanes(swap_blocks(blocks))):
                    block_ref[b * 8 + z, x : x + 8, :] = row
        columns = pl.ds(xb * TILE, TILE)
        copies.append(
            pltpu.make_async_copy(
                block_ref.at[:, columns, :], out_ref.at[:, columns, :], sems.at[xb]
            )
        )
        copies[-1].start()

    backward(w_ref, sm_ref, table_ref, lambda tile: old_ref[tile], store, 1, gz)
    for copy in copies:
        copy.wait()


def owner_kernel(table_ref, recv_ref, out_ref, acc_ref, mea_ref, *sum_refs, subset):
    gz = lax.axis_index("gz")
    xy = lax.axis_index("xy")
    view = jnp.minimum(xy // GROUPS, VIEWS - 1)
    group = xy % GROUPS
    at = subset * VIEWS + view
    per = ROWS_PER[subset]
    half = per + 1
    lane = iota((8, 128), 1)
    for sum_ref in sum_refs:
        sum_ref[...] = jnp.zeros_like(sum_ref)
    mea_ref[...] = jnp.zeros_like(mea_ref)
    end = N_XY * 2 * half - 8

    def upper(s):
        row = s * 2 * half + half
        last = recv_ref[min(row, end) : min(row, end) + 8, :]
        return pltpu.roll(last, 8 - (row - end), 0) if row > end else last

    for s in range(N_XY):
        column = s * COLS_DEV
        own = jnp.where(lane >= MEAS_AT - 128, upper(s), 0.0)
        own = pltpu.roll(own, (column + 256 - MEAS_AT) % 128, 1)
        block = column // 128 * 128
        offset = column - block
        mea_ref[:, block : block + 128] += jnp.where(lane >= offset, own, 0.0)
        if offset + COLS_DEV > 128:
            mea_ref[:, block + 128 : block + 256] += jnp.where(lane < offset, own, 0.0)
    for s in range(N_XY):
        base = pl.multiple_of(table_ref[at, s], 128)
        shift = table_ref[at, SHIFT_AT + s]
        row = s * 2 * half
        low = pltpu.roll(recv_ref[row : row + 8, :], shift, 1)
        high = pltpu.roll(jnp.where(lane < WIN - 128, upper(s), 0.0), shift, 1)
        wrapped = lane < shift
        part_ref = sum_refs[s % SUMS]
        part_ref[:, pl.ds(base, 128)] += jnp.where(wrapped, 0.0, low)
        part_ref[:, pl.ds(base + 128, 128)] += jnp.where(wrapped, low, high)
        part_ref[:, pl.ds(base + 256, 128)] += jnp.where(wrapped, high, 0.0)
    slot = iota((8, NZ), 0)
    row = first_row(gz, subset) + group * per + slot
    ray_rows = jnp.where(slot < per, hat(row, iota((8, NZ), 1)), 0.0)
    ray_rows = jnp.sum(ray_rows, axis=1, keepdims=True)
    sums = sum_refs[0][...]
    for part_ref in sum_refs[1:]:
        sums = sums + part_ref[...]
    totals = sums[per : per + 1, :]
    acc_ref[...] = mea_ref[...] - sums / jnp.maximum(ray_rows * totals, 1.0)
    for t in range(N_XY):
        base = pl.multiple_of(table_ref[at, t], 128)
        shift = table_ref[at, SHIFT_AT + t]
        back = (128 - shift) & 127
        a = pltpu.roll(acc_ref[:, pl.ds(base, 128)], back, 1)
        b = pltpu.roll(acc_ref[:, pl.ds(base + 128, 128)], back, 1)
        c = pltpu.roll(acc_ref[:, pl.ds(base + 256, 128)], back, 1)
        kept = lane < 128 - shift
        low = jnp.where(kept, a, b)
        high = jnp.where(kept, b, c)
        if subset == 0:
            other = pltpu.roll(high, COLS_DEV, 1)
            even = jnp.where(
                slot == 5,
                pltpu.roll(high, 5, 0),
                jnp.where(slot == 6, pltpu.roll(high, 4, 0), pltpu.roll(high, 3, 0)),
            )
            odd = jnp.where(slot == 5, pltpu.roll(other, 4, 0), pltpu.roll(other, 3, 0))
            rest = jnp.where(lane < COLS_DEV, even, odd)
            out_ref[t] = jnp.where(slot < 5, low, rest).astype(jnp.bfloat16)
            continue
        column = t * COLS_DEV
        block = column // 128 * 128
        offset = column - block
        turn = (MEAS_AT - 128 - offset) % 128
        own = pltpu.roll(acc_ref[:, block : block + 128], turn, 1)
        if offset + COLS_DEV > 128:
            more = pltpu.roll(acc_ref[:, block + 128 : block + 256], turn, 1)
            own = jnp.where(lane < MEAS_AT - offset, own, more)
        high = jnp.where(lane >= MEAS_AT - 128, own, high)
        out_ref[t * 8 : (t + 1) * 8, :] = jnp.where(slot < 4, low, pltpu.roll(high, 4, 0))


def call(kernel, inputs, outs, scratch, name):
    vmem = pl.BlockSpec(memory_space=pltpu.VMEM)
    smem = pl.BlockSpec(memory_space=pltpu.SMEM)
    anywhere = pl.BlockSpec(memory_space=pl.ANY)

    def spec(x):
        if x.dtype == jnp.int32:
            return smem
        return anywhere if isinstance(x, jax.ShapeDtypeStruct) else vmem

    inputs = [
        x if x.dtype == jnp.int32 else pltpu.with_memory_space_constraint(x, pltpu.VMEM)
        for x in inputs
    ]
    return pl.pallas_call(
        kernel,
        in_specs=[spec(x) for x in inputs],
        out_specs=[spec(x) for x in outs],
        out_shape=outs,
        scratch_shapes=scratch,
        compiler_params=pltpu.CompilerParams(vmem_limit_bytes=12 * 1024 * 1024),
        name=name,
    )(*inputs)


def exchanged(parts, shape):
    sent = lax.all_to_all(
        parts.reshape(shape), "xy", split_axis=0, concat_axis=0, tiled=True
    )
    return sent.reshape(parts.shape)


def local(volume, measured, view_order):
    f32 = jnp.float32
    bf16 = jnp.bfloat16
    vmem = pltpu.VMEM
    flat = volume.reshape(Z_DEV * X_DEV, NY)
    order = view_order.reshape(1, ANGLES)
    rows = measured.transpose(1, 2, 0, 3).reshape(VIEWS * ROWS_DEV * SUBSETS, COLS_DEV)
    made = vmem((TILES, DEPTH, VOXELS), bf16)
    slices = vmem((TILES, Z_DEV, VOXELS), f32)
    sm_scratch = vmem((VIEWS, Z_PAD, LANES), f32)
    acc_scratch = [vmem((WIN, 128), f32)] * VIEWS
    row_scratch = vmem((8, FULL), f32)
    owner_scratch = [row_scratch] * (2 + SUMS)

    sent = vmem((SENT_ROWS, 128), bf16)
    hbm = pl.BlockSpec(memory_space=pltpu.HBM)
    up, down, flat, rows, order = pl.pallas_call(
        pack_kernel,
        in_specs=[hbm] * 3,
        out_specs=[pl.BlockSpec(memory_space=vmem)] * 5,
        out_shape=[
            sent, sent, vmem(flat.shape, f32), vmem(rows.shape, f32), vmem((1, ANGLES), jnp.int32)
        ],
        scratch_shapes=[vmem((SUBSETS * M_HALO, 128), f32), pltpu.SemaphoreType.DMA((3,))],
        compiler_params=pltpu.CompilerParams(vmem_limit_bytes=12 * 1024 * 1024),
        name="pack",
    )(*(pltpu.with_memory_space_constraint(x, pltpu.HBM) for x in (flat, rows, order)))
    next_up = [(i, (i + 1) % N_GZ) for i in range(N_GZ)]
    low = lax.ppermute(up, "gz", next_up)
    high = lax.ppermute(down, "gz", [(j, i) for i, j in next_up])
    w0, w1, own, mown, table = pl.pallas_call(
        prepare_kernel,
        in_specs=[pl.BlockSpec(memory_space=vmem)] * 3,
        out_specs=[pl.BlockSpec(memory_space=m) for m in (vmem, vmem, vmem, vmem, pltpu.SMEM)],
        out_shape=[
            made, made, slices, vmem((SUBSETS, VIEWS, 24, 128), f32), pltpu.SMEM(TABLE, jnp.int32)
        ],
        scratch_shapes=[
            vmem((VIEWS, TILES, VOXELS), f32), vmem(TABLE, jnp.int32), pltpu.SemaphoreType.DMA
        ],
        compiler_params=pltpu.CompilerParams(vmem_limit_bytes=12 * 1024 * 1024),
        name="prepare",
    )(*(pltpu.with_memory_space_constraint(x, vmem) for x in (order, flat, rows)))
    partial, side, m1 = call(
        first_kernel,
        (table, w0, own, mown, low, high),
        [vmem((N_XY * 12, 128), f32), slices, vmem((VIEWS, 64, 128), f32)],
        [
            vmem((SUBSETS, VIEWS, M_ROWS, 128), f32),
            vmem((VIEWS, 72, 128), f32),
            vmem((2, EDGE_ROWS, 128), f32),
            *acc_scratch,
        ],
        "first",
    )
    (rounded,) = call(
        functools.partial(owner_kernel, subset=0),
        (table, exchanged(partial, (N_XY, 3, 4, 128))),
        [vmem((N_XY, 8, 128), bf16)],
        owner_scratch,
        "owner_a",
    )
    partial, new = call(
        middle_kernel,
        (table, exchanged(rounded, rounded.shape), own, side, m1, w0, w1),
        [vmem((N_XY * 10, 128), f32), slices],
        [sm_scratch, vmem((TILES, Z_PAD, VOXELS), bf16), *acc_scratch],
        "middle",
    )
    (final,) = call(
        functools.partial(owner_kernel, subset=1),
        (table, exchanged(partial, (N_XY, 5, 2, 128))),
        [vmem((N_XY * 8, 128), f32)],
        owner_scratch,
        "owner_b",
    )
    volume_out, residual = call(
        last_kernel,
        (table, exchanged(final, (N_XY, 8, 128)), new, w1),
        [
            jax.ShapeDtypeStruct(VOLUME, f32),
            jax.ShapeDtypeStruct((VIEWS, ROWS_DEV, COLS_DEV), f32),
        ],
        [
            sm_scratch,
            slices,
            vmem(VOLUME, f32),
            vmem((VIEWS, ROWS_DEV, COLS_DEV), f32),
            pltpu.SemaphoreType.DMA((X_DEV // TILE + 1,)),
        ],
        "last",
    )
    return volume_out, residual


def solution(mesh):
    in_specs = (P("gz", "xy", None), P(None, None, "gz", "xy"), P())
    out_specs = (P("gz", "xy", None), P(None, "gz", "xy"))
    return jax.shard_map(local, mesh=mesh, in_specs=in_specs, out_specs=out_specs, check_vma=False)
```

```python
import functools
import math

import jax
import jax.numpy as jnp
from jax import lax
from jax.experimental import pallas as pl
from jax.experimental.pallas import tpu as pltpu
from jax.sharding import PartitionSpec as P

Z_DEV = 16
X_DEV = 48
NY = 128
COLS_DEV = 48
ROWS_DEV = 20
VIEWS = 5
SUBSETS = 2
ANGLES = 48
N_XY = 32
N_GZ = 8
NX = X_DEV * N_XY
NZ = Z_DEV * N_GZ
DR = ROWS_DEV * N_GZ
DC = COLS_DEV * N_XY

WIN = 176
LANES = 256
MEAS_AT = LANES - COLS_DEV
Z_HALO = 6
Z_ALL = Z_DEV + 2 * Z_HALO
ONES = Z_ALL
Z_PAD = 32
GROUPS = 6
GOT = GROUPS * 8
ROWS_PER = (5, 4)
ROWS_BELOW = (3, 0)
M_HALO = 8
M_ROWS = 40
FULL = 15 * 128
SUMS = 4
TILE = 16
TILES_Y = NY // TILE
TILES = X_DEV // TILE * TILES_Y
VOXELS = TILE * TILE
COLS_TILE = 40
VOLUME = (Z_DEV, X_DEV, NY)
PLACE = (0, 40, 80, 128, 168)
DEPTH = 208
HALO_ROWS = Z_HALO * X_DEV
EDGE_AT = HALO_ROWS
EDGE_ROWS = SUBSETS * VIEWS * M_HALO
SENT_ROWS = EDGE_AT + EDGE_ROWS
TABLE = (16, 128)
SHIFT_AT = 32
TILE_AT = 64


def iota(shape, dim):
    return lax.broadcasted_iota(jnp.int32, shape, dim)


def slice_of(i, gz):
    low = Z_DEV * gz - Z_HALO + (i - Z_DEV)
    high = Z_DEV * gz + Z_DEV + (i - Z_DEV - Z_HALO)
    return jnp.where(i < Z_DEV, Z_DEV * gz + i, jnp.where(i < Z_DEV + Z_HALO, low, high))


def hat(row, z):
    position = (DR - 1) / 2.0 + 0.96 * (DR / NZ) * (z.astype(jnp.float32) - (NZ - 1) / 2.0)
    value = jnp.maximum(0.0, 1.0 - jnp.abs(position - row.astype(jnp.float32)) / 2.0)
    ok = (row >= 0) & (row < DR) & (z >= 0) & (z < NZ)
    return jnp.where(ok, value, 0.0)


def first_row(gz, subset):
    return ROWS_DEV * gz - ROWS_BELOW[subset] - ((gz + 1) >> 1)


def slot_weights(group, slot, i, gz, subset):
    per = ROWS_PER[subset]
    row = first_row(gz, subset) + group * per + slot
    return jnp.where((slot < per) & (i < Z_ALL), hat(row, slice_of(i, gz)), 0.0)


def tile_offsets(table_ref, subset, tile):
    return [
        pl.multiple_of(table_ref[subset * VIEWS + v, TILE_AT + tile], 8) for v in range(VIEWS)
    ]


def coordinate(x, y, cosine, sine):
    xc = x - (NX - 1) / 2.0
    yc = y - (NY - 1) / 2.0
    source = 2.0 * NX
    along = xc * cosine + yc * sine
    depth = yc * cosine - xc * sine
    return (DC - 1) / 2.0 + 0.9 * (DC / NX) * along * source / (source + depth)


def fill_table(cosine, sine, xy):
    lane = iota(TABLE, 1)
    tile = lane - TILE_AT
    is_tile = lane >= TILE_AT
    strip = lane & (N_XY - 1)
    x = jnp.where(is_tile, xy * X_DEV + (tile >> 3) * TILE, strip * X_DEV).astype(jnp.float32)
    y = jnp.where(is_tile, (tile & 7) * TILE, 0).astype(jnp.float32)
    dx = jnp.where(is_tile, TILE - 1.0, X_DEV - 1.0)
    dy = jnp.where(is_tile, TILE - 1.0, NY - 1.0)
    least = jnp.minimum(
        jnp.minimum(coordinate(x, y, cosine, sine), coordinate(x + dx, y, cosine, sine)),
        jnp.minimum(coordinate(x, y + dy, cosine, sine), coordinate(x + dx, y + dy, cosine, sine)),
    )
    least = jnp.floor(least).astype(jnp.int32)
    start = least - 2
    own = jnp.sum(jnp.where(lane == xy, start, 0).astype(jnp.float32), axis=1, keepdims=True)
    tiles = jnp.maximum(least - 1 - own.astype(jnp.int32), 0) & ~7
    table = jnp.where(lane < SHIFT_AT, start & ~127, start & 127)
    return jnp.where(is_tile, tiles, table), own


def positions(u_ref, cosine, sine, own, subset, xy):
    t = iota((TILES, VOXELS), 0)
    l = iota((TILES, VOXELS), 1)
    x = ((t >> 3) * TILE + (l >> 4) + xy * X_DEV).astype(jnp.float32)
    y = ((t & 7) * TILE + (l & 15)).astype(jnp.float32)
    for v in range(VIEWS):
        at = subset * VIEWS + v
        u = coordinate(x, y, cosine[at : at + 1, 0:1], sine[at : at + 1, 0:1])
        u_ref[v] = u - own[at : at + 1, :]


def weights(u_ref, offsets, tile):
    c = iota((COLS_TILE, VOXELS), 0).astype(jnp.float32)
    pieces = []
    for v in range(VIEWS):
        u = u_ref[v, pl.ds(tile, 1), :] - offsets[v].astype(jnp.float32)
        pieces.append(jnp.maximum(0.0, 1.0 - jnp.abs(u - c)))
    pieces.insert(3, jnp.zeros((8, VOXELS), jnp.float32))
    return jnp.concatenate(pieces, axis=0).astype(jnp.bfloat16)


def forward(w_ref, slices, acc_refs, m_ref, table_ref, out_ref, subset, gz):
    for acc_ref in acc_refs:
        acc_ref[...] = jnp.zeros_like(acc_ref)
    for tile in range(TILES):
        offsets = tile_offsets(table_ref, subset, tile)
        part = lax.dot_general(
            w_ref[tile],
            jnp.concatenate([slices(tile)] * 4, axis=0),
            (((1,), (1,)), ((), ())),
            preferred_element_type=jnp.float32,
        )
        for v in range(VIEWS):
            acc_refs[v][pl.ds(offsets[v], COLS_TILE), :] += part[PLACE[v] : PLACE[v] + COLS_TILE]
    per = ROWS_PER[subset]
    half = per + 1
    size = GROUPS * 2 * half
    k = iota((size, 128), 0)
    lane = iota((size, 128), 1)
    i = lane & (Z_PAD - 1)
    group = (k * 43) >> 9 if half == 6 else (k * 205) >> 11
    slot = k - group * 2 * half
    is_low = slot < half
    slot = jnp.where(is_low, slot, slot - half)
    rows = slot_weights(group, slot, i, gz, subset)
    rows = jnp.where((slot == per) & (i == ONES), 1.0, rows)
    rounded = rows.astype(jnp.bfloat16).astype(jnp.float32)
    rows = jnp.where(lane < 2 * Z_PAD, rounded, rows - rounded).astype(jnp.bfloat16)
    left_over = (iota((WIN, 128), 1) & Z_PAD) != 0
    used = GROUPS * VIEWS * 2 * half
    out_ref[used:, :] = jnp.zeros((out_ref.shape[0] - used, 128), jnp.float32)
    for v in range(VIEWS):
        sums = acc_refs[v][...]
        rounded = sums.astype(jnp.bfloat16).astype(jnp.float32)
        sums = jnp.where(left_over, sums - rounded, rounded).astype(jnp.bfloat16)
        sums = lax.dot_general(
            rows, sums, (((1,), (1,)), ((), ())), preferred_element_type=jnp.float32
        )
        high = jnp.concatenate(
            (sums[:, 128:WIN], jnp.zeros((size, LANES - WIN), jnp.float32)), axis=1
        )
        part = jnp.where(is_low, sums[:, 0:128], high) + m_ref[v, 0:size, :]
        out_ref[v * size : (v + 1) * size, :] = part


def three_parts(x, third):
    first = x.astype(jnp.bfloat16).astype(jnp.float32)
    second = (x - first).astype(jnp.bfloat16).astype(jnp.float32)
    part = jnp.where(third == 0, first, jnp.where(third == 1, second, x - first - second))
    return part.astype(jnp.bfloat16)


def smear(recv_ref, sm_ref, gz):
    i = iota((3 * Z_PAD, 3 * GOT), 0)
    k = iota((3 * Z_PAD, 3 * GOT), 1)
    third = (k >= GOT).astype(jnp.int32) + (k >= 2 * GOT).astype(jnp.int32)
    k = k - GOT * third
    part = k & 7
    block = i >> 5
    slot = jnp.where(block == 0, part, 2 * (part - 5) + block - 1)
    rows = slot_weights(k >> 3, slot, i & (Z_PAD - 1), gz, 0)
    rows = three_parts(jnp.where((block == 0) == (part < 5), rows, 0.0), third)
    ones = iota((Z_PAD, LANES), 0) == ONES
    for v in range(VIEWS):
        got = recv_ref[v * GROUPS : (v + 1) * GROUPS].astype(jnp.float32)
        got = got.reshape(GOT, 128).astype(jnp.bfloat16)
        sums = jnp.dot(
            rows, jnp.concatenate((got, got, got), axis=0), preferred_element_type=jnp.float32
        )
        high = sums[Z_PAD : 2 * Z_PAD] + pltpu.roll(sums[2 * Z_PAD :], 128 - COLS_DEV, 1)
        smeared = jnp.concatenate((sums[0:Z_PAD], high), axis=1)
        sm_ref[v] = jnp.where(ones, 1.0, smeared).astype(jnp.bfloat16).astype(jnp.float32)


def smear_last(recv_ref, sm_ref, res_ref, gz):
    size = 2 * Z_PAD + 24
    i = iota((size, 3 * GOT), 0)
    k = iota((size, 3 * GOT), 1)
    third = (k >= GOT).astype(jnp.int32) + (k >= 2 * GOT).astype(jnp.int32)
    k = k - GOT * third
    part = k & 7
    rows = slot_weights(k >> 3, part & 3, i & (Z_PAD - 1), gz, 1)
    rows = three_parts(jnp.where((part >= 4) == (i >= Z_PAD), rows, 0.0), third)
    j = i - 2 * Z_PAD + ((gz + 1) >> 1)
    picked = jnp.where(k == ((j >> 2) << 3) + 4 + (j & 3), 1.0, 0.0).astype(jnp.bfloat16)
    rows = jnp.where(i >= 2 * Z_PAD, picked.astype(jnp.float32), rows.astype(jnp.float32))
    rows = rows.astype(jnp.bfloat16)
    ones = iota((Z_PAD, LANES), 0) == ONES
    part = iota((GOT, 128), 0) & 7
    exact = (part >= 4) & (iota((GOT, 128), 1) >= MEAS_AT - 128)
    for v in range(VIEWS):
        got = recv_ref[v * GOT : (v + 1) * GOT, :]
        first = got.astype(jnp.bfloat16).astype(jnp.float32)
        second = (got - first).astype(jnp.bfloat16).astype(jnp.float32)
        parts = (
            first,
            jnp.where(exact, second, first),
            jnp.where(exact, got - first - second, first),
        )
        sums = jnp.dot(
            rows,
            jnp.concatenate(parts, axis=0).astype(jnp.bfloat16),
            preferred_element_type=jnp.float32,
        )
        smeared = jnp.concatenate((sums[0:Z_PAD], sums[Z_PAD : 2 * Z_PAD]), axis=1)
        sm_ref[v] = jnp.where(ones, 1.0, smeared).astype(jnp.bfloat16).astype(jnp.float32)
        own = pltpu.roll(sums[2 * Z_PAD :], 256 - MEAS_AT, 1)
        res_ref[v] = own[0:ROWS_DEV, 0:COLS_DEV]


def windows(sm_ref, offsets):
    lane = iota((Z_PAD, 128), 1)
    placed = []
    for v in range(VIEWS):
        at = PLACE[v] & 127
        shift = (at - offsets[v]) & 127
        low = pltpu.roll(sm_ref[v, :, 0:128], shift, 1)
        high = pltpu.roll(sm_ref[v, :, 128:256], shift, 1)
        placed.append(jnp.where(lane < at + 128 - offsets[v], low, high))
    first = jnp.where(lane < 40, placed[0], jnp.where(lane < 80, placed[1], placed[2]))
    first = jnp.where(lane < 120, first, 0.0)
    second = jnp.where(lane < 40, placed[3], jnp.where(lane < 80, placed[4], 0.0))
    both = jnp.concatenate((first, second), axis=1)
    return both.astype(jnp.bfloat16)[:, 0:DEPTH]


def backward(w_ref, sm_ref, table_ref, old, store, subset, gz):
    zi = slice_of(iota((Z_PAD, LANES), 0), gz)
    inside = iota((Z_PAD, LANES), 0) < Z_ALL
    total = jnp.sum(jnp.where(inside, hat(iota((Z_PAD, LANES), 1), zi), 0.0), axis=1, keepdims=True)

    for tile in range(TILES):
        offsets = tile_offsets(table_ref, subset, tile)
        back = jnp.dot(
            windows(sm_ref, offsets), w_ref[tile], preferred_element_type=jnp.float32
        )
        norm = total * back[ONES : ONES + 1, :]
        store(tile, old(tile), back / jnp.maximum(norm, 1.0))


def swapped(rows, index, turn, axis):
    for d in (4, 2, 1):
        high = (index & d) != 0
        new = list(rows)
        for i in range(8):
            if i & d == 0:
                a, b = (rows[i], rows[i + d])
                new[i] = jnp.where(high, pltpu.roll(b, turn * d, axis), a)
                new[i + d] = jnp.where(high, b, pltpu.roll(a, turn * (8 - d), axis))
        rows = new
    return rows


def swap_blocks(rows):
    return swapped(rows, iota((8, 128), 1) >> 4, 16, 1)


def swap_sublanes(rows):
    return swapped(rows, iota((8, 128), 0), 1, 0)


def relay(read, out_ref, unrolled):
    def step(xb, nothing):
        for half in range(2):
            for b in range(2):
                x = xb * TILE + half * 8
                rows = swap_sublanes([read(b * 8 + z, x) for z in range(8)])
                for q, block in enumerate(swap_blocks(rows)):
                    out_ref[
                        xb * TILES_Y + q, b * 8 : b * 8 + 8, half * 128 : half * 128 + 128
                    ] = block
        return nothing

    if unrolled:
        for xb in range(X_DEV // TILE):
            step(xb, 0)
    else:
        lax.fori_loop(0, X_DEV // TILE, step, 0)


def pack_kernel(
    vol_hbm, meas_hbm, order_hbm, up_ref, down_ref, vol_ref, meas_ref, order_ref, row_ref, sems
):
    copies = [
        pltpu.make_async_copy(vol_hbm, vol_ref, sems.at[0]),
        pltpu.make_async_copy(meas_hbm, meas_ref, sems.at[1]),
        pltpu.make_async_copy(order_hbm, order_ref, sems.at[2]),
    ]
    for copy in copies:
        copy.start()
    row_ref[...] = jnp.zeros_like(row_ref)
    for copy in copies:
        copy.wait()
    for out_ref, z, r in (
        (up_ref, Z_DEV - Z_HALO, ROWS_DEV - M_HALO),
        (down_ref, 0, 0),
    ):
        slices = vol_ref[z * X_DEV : (z + Z_HALO) * X_DEV, :]
        out_ref[0:HALO_ROWS, :] = slices.astype(jnp.bfloat16)
        for v in range(VIEWS):
            at = (v * ROWS_DEV + r) * SUBSETS
            row_ref[:, 0:COLS_DEV] = meas_ref[at : at + SUBSETS * M_HALO, :]
            row = row_ref[...]
            rounded = row.astype(jnp.bfloat16).astype(jnp.float32)
            both = pltpu.roll(rounded, MEAS_AT - 128, 1)
            both = both + pltpu.roll(row - rounded, MEAS_AT - 128 - COLS_DEV, 1)
            at = EDGE_AT + v * SUBSETS * M_HALO
            out_ref[at : at + SUBSETS * M_HALO, :] = both.astype(jnp.bfloat16)


def prepare_kernel(
    order_ref, vol_ref, meas_ref,
    w0_ref, w1_ref, own_ref, mown_ref, table_ref, u_ref, flat_ref, sem,
):
    xy = lax.axis_index("xy")
    chosen = iota((TABLE[0], ANGLES), 0) == iota((TABLE[0], ANGLES), 1)
    chosen = jnp.where(chosen, order_ref[...].astype(jnp.float32), 0.0)
    chosen = jnp.broadcast_to(jnp.sum(chosen, axis=1, keepdims=True), TABLE)
    angles = 2.0 * math.pi * chosen / ANGLES
    cosine = jnp.cos(angles)
    sine = jnp.sin(angles)
    flat_ref[...], own = fill_table(cosine, sine, xy)
    copy = pltpu.make_async_copy(flat_ref, table_ref, sem)
    copy.start()
    relay(
        lambda z, x: vol_ref[pl.ds(pl.multiple_of(z * X_DEV + x, 8), 8), :], own_ref, False
    )
    mown_ref[...] = jnp.zeros_like(mown_ref)
    for s in range(SUBSETS):
        for v in range(VIEWS):
            for at, count in ((0, 8), (8, 8), (16, 4)):
                rows = meas_ref[pl.ds((v * ROWS_DEV + at) * 2 + s, count, stride=2), :]
                mown_ref[s, v, at : at + count, MEAS_AT - 128 : 128] = rows
    copy.wait()
    for subset, w_ref in ((0, w0_ref), (1, w1_ref)):
        positions(u_ref, cosine, sine, own, subset, xy)

        def step(tt, nothing):
            for t in range(8):
                tile = tt * 8 + t
                w_ref[tile] = weights(u_ref, tile_offsets(table_ref, subset, tile), tile)
            return nothing

        lax.fori_loop(0, TILES // 8, step, 0)


def first_kernel(
    table_ref, w_ref, own_ref, mown_ref, low_ref, high_ref,
    out_ref, side_ref, m1_ref, raw_ref, m0_ref, edge_ref, *acc_refs,
):
    gz = lax.axis_index("gz")
    for side, sent_ref in enumerate((low_ref, high_ref)):
        edge = sent_ref[EDGE_AT:SENT_ROWS, :].astype(jnp.float32)
        edge = edge + pltpu.roll(edge, COLS_DEV, 1)
        edge_ref[side] = jnp.where(iota(edge.shape, 1) >= MEAS_AT - 128, edge, 0.0)

    def read(z, x):
        if z >= 2 * Z_HALO:
            return jnp.full((8, NY), 1.0 if z == ONES - Z_DEV else 0.0, jnp.float32)
        sent_ref = low_ref if z < Z_HALO else high_ref
        at = z % Z_HALO * X_DEV + x
        return sent_ref[at : at + 8, :].astype(jnp.float32)

    relay(read, side_ref, True)
    for s, m_ref in ((0, m0_ref), (1, m1_ref)):
        per = ROWS_PER[s]
        m_ref[...] = jnp.zeros_like(m_ref)
        for v in range(VIEWS):
            edge = pl.ds(v * 2 * M_HALO + s, M_HALO, stride=2)
            high = edge_ref[1, edge, :]
            joined = jnp.concatenate(
                (
                    edge_ref[0, edge, :],
                    mown_ref[s, v, 0:16, :],
                    jnp.concatenate((mown_ref[s, v, 16:20, :], high[0:4]), axis=0),
                    jnp.concatenate((high[4:8], jnp.zeros((4, 128), jnp.float32)), axis=0),
                ),
                axis=0,
            )
            raw_ref[s, v] = pltpu.roll(
                joined, M_ROWS + ((gz + 1) >> 1) - (M_HALO - ROWS_BELOW[s]), 0
            )
            for group in range(GROUPS):
                at = group * 2 * (per + 1) + per + 1
                m_ref[v, at : at + per, :] = raw_ref[s, v, group * per : (group + 1) * per, :]

    def slices(tile):
        return jnp.concatenate((own_ref[tile], side_ref[tile]), axis=0).astype(jnp.bfloat16)

    forward(w_ref, slices, acc_refs, m0_ref, table_ref, out_ref, 0, gz)


def middle_kernel(
    table_ref, recv_ref, own_ref, side_ref, m_ref, w0_ref, w1_ref,
    out_ref, new_ref, sm_ref, vb_ref, *acc_refs,
):
    gz = lax.axis_index("gz")
    smear(recv_ref, sm_ref, gz)
    ones = iota((Z_PAD, VOXELS), 0) == ONES

    def old(tile):
        return jnp.concatenate((own_ref[tile], side_ref[tile]), axis=0)

    def store(tile, old, change):
        new = jnp.where(ones, 1.0, old + change)
        new_ref[tile] = new[0:Z_DEV]
        vb_ref[tile] = new.astype(jnp.bfloat16)

    backward(w0_ref, sm_ref, table_ref, old, store, 0, gz)
    forward(w1_ref, lambda tile: vb_ref[tile], acc_refs, m_ref, table_ref, out_ref, 1, gz)


def last_kernel(
    table_ref, recv_ref, old_ref, w_ref,
    out_ref, res_ref, sm_ref, new_ref, block_ref, own_ref, sems,
):
    gz = lax.axis_index("gz")
    smear_last(recv_ref, sm_ref, own_ref, gz)
    copies = [pltpu.make_async_copy(own_ref, res_ref, sems.at[X_DEV // TILE])]
    copies[0].start()

    def store(tile, old, change):
        new_ref[tile] = old + change[0:Z_DEV]
        xb = tile // TILES_Y
        if tile % TILES_Y < TILES_Y - 1:
            return
        for half in range(2):
            for b in range(Z_DEV // 8):
                blocks = [
                    new_ref[xb * TILES_Y + q, b * 8 : b * 8 + 8, half * 128 : half * 128 + 128]
                    for q in range(TILES_Y)
                ]
                x = xb * TILE + half * 8
                for z, row in enumerate(swap_sublanes(swap_blocks(blocks))):
                    block_ref[b * 8 + z, x : x + 8, :] = row
        columns = pl.ds(xb * TILE, TILE)
        copies.append(
            pltpu.make_async_copy(
                block_ref.at[:, columns, :], out_ref.at[:, columns, :], sems.at[xb]
            )
        )
        copies[-1].start()

    backward(w_ref, sm_ref, table_ref, lambda tile: old_ref[tile], store, 1, gz)
    for copy in copies:
        copy.wait()


def owner_kernel(table_ref, recv_ref, out_ref, acc_ref, mea_ref, *sum_refs, subset):
    gz = lax.axis_index("gz")
    xy = lax.axis_index("xy")
    view = jnp.minimum(xy // GROUPS, VIEWS - 1)
    group = xy % GROUPS
    at = subset * VIEWS + view
    per = ROWS_PER[subset]
    half = per + 1
    lane = iota((8, 128), 1)
    for sum_ref in sum_refs:
        sum_ref[...] = jnp.zeros_like(sum_ref)
    mea_ref[...] = jnp.zeros_like(mea_ref)
    end = N_XY * 2 * half - 8

    def upper(s):
        row = s * 2 * half + half
        last = recv_ref[min(row, end) : min(row, end) + 8, :]
        return pltpu.roll(last, 8 - (row - end), 0) if row > end else last

    for s in range(N_XY):
        column = s * COLS_DEV
        own = jnp.where(lane >= MEAS_AT - 128, upper(s), 0.0)
        own = pltpu.roll(own, (column + 256 - MEAS_AT) % 128, 1)
        block = column // 128 * 128
        offset = column - block
        mea_ref[:, block : block + 128] += jnp.where(lane >= offset, own, 0.0)
        if offset + COLS_DEV > 128:
            mea_ref[:, block + 128 : block + 256] += jnp.where(lane < offset, own, 0.0)
    for s in range(N_XY):
        base = pl.multiple_of(table_ref[at, s], 128)
        shift = table_ref[at, SHIFT_AT + s]
        row = s * 2 * half
        low = pltpu.roll(recv_ref[row : row + 8, :], shift, 1)
        high = pltpu.roll(jnp.where(lane < WIN - 128, upper(s), 0.0), shift, 1)
        wrapped = lane < shift
        part_ref = sum_refs[s % SUMS]
        part_ref[:, pl.ds(base, 128)] += jnp.where(wrapped, 0.0, low)
        part_ref[:, pl.ds(base + 128, 128)] += jnp.where(wrapped, low, high)
        part_ref[:, pl.ds(base + 256, 128)] += jnp.where(wrapped, high, 0.0)
    slot = iota((8, NZ), 0)
    row = first_row(gz, subset) + group * per + slot
    ray_rows = jnp.where(slot < per, hat(row, iota((8, NZ), 1)), 0.0)
    ray_rows = jnp.sum(ray_rows, axis=1, keepdims=True)
    sums = sum_refs[0][...]
    for part_ref in sum_refs[1:]:
        sums = sums + part_ref[...]
    totals = sums[per : per + 1, :]
    acc_ref[...] = mea_ref[...] - sums / jnp.maximum(ray_rows * totals, 1.0)
    for t in range(N_XY):
        base = pl.multiple_of(table_ref[at, t], 128)
        shift = table_ref[at, SHIFT_AT + t]
        back = (128 - shift) & 127
        a = pltpu.roll(acc_ref[:, pl.ds(base, 128)], back, 1)
        b = pltpu.roll(acc_ref[:, pl.ds(base + 128, 128)], back, 1)
        c = pltpu.roll(acc_ref[:, pl.ds(base + 256, 128)], back, 1)
        kept = lane < 128 - shift
        low = jnp.where(kept, a, b)
        high = jnp.where(kept, b, c)
        if subset == 0:
            other = pltpu.roll(high, COLS_DEV, 1)
            even = jnp.where(
                slot == 5,
                pltpu.roll(high, 5, 0),
                jnp.where(slot == 6, pltpu.roll(high, 4, 0), pltpu.roll(high, 3, 0)),
            )
            odd = jnp.where(slot == 5, pltpu.roll(other, 4, 0), pltpu.roll(other, 3, 0))
            rest = jnp.where(lane < COLS_DEV, even, odd)
            out_ref[t] = jnp.where(slot < 5, low, rest).astype(jnp.bfloat16)
            continue
        column = t * COLS_DEV
        block = column // 128 * 128
        offset = column - block
        turn = (MEAS_AT - 128 - offset) % 128
        own = pltpu.roll(acc_ref[:, block : block + 128], turn, 1)
        if offset + COLS_DEV > 128:
            more = pltpu.roll(acc_ref[:, block + 128 : block + 256], turn, 1)
            own = jnp.where(lane < MEAS_AT - offset, own, more)
        high = jnp.where(lane >= MEAS_AT - 128, own, high)
        out_ref[t * 8 : (t + 1) * 8, :] = jnp.where(slot < 4, low, pltpu.roll(high, 4, 0))


def call(kernel, inputs, outs, scratch, name):
    vmem = pl.BlockSpec(memory_space=pltpu.VMEM)
    smem = pl.BlockSpec(memory_space=pltpu.SMEM)
    anywhere = pl.BlockSpec(memory_space=pl.ANY)

    def spec(x):
        if x.dtype == jnp.int32:
            return smem
        return anywhere if isinstance(x, jax.ShapeDtypeStruct) else vmem

    inputs = [
        x if x.dtype == jnp.int32 else pltpu.with_memory_space_constraint(x, pltpu.VMEM)
        for x in inputs
    ]
    return pl.pallas_call(
        kernel,
        in_specs=[spec(x) for x in inputs],
        out_specs=[spec(x) for x in outs],
        out_shape=outs,
        scratch_shapes=scratch,
        compiler_params=pltpu.CompilerParams(vmem_limit_bytes=12 * 1024 * 1024),
        name=name,
    )(*inputs)


def exchanged(parts, shape):
    sent = lax.all_to_all(
        parts.reshape(shape), "xy", split_axis=0, concat_axis=0, tiled=True
    )
    return sent.reshape(parts.shape)


def local(volume, measured, view_order):
    f32 = jnp.float32
    bf16 = jnp.bfloat16
    vmem = pltpu.VMEM
    flat = volume.reshape(Z_DEV * X_DEV, NY)
    order = view_order.reshape(1, ANGLES)
    rows = measured.transpose(1, 2, 0, 3).reshape(VIEWS * ROWS_DEV * SUBSETS, COLS_DEV)
    made = vmem((TILES, DEPTH, VOXELS), bf16)
    slices = vmem((TILES, Z_DEV, VOXELS), f32)
    sm_scratch = vmem((VIEWS, Z_PAD, LANES), f32)
    acc_scratch = [vmem((WIN, 128), f32)] * VIEWS
    row_scratch = vmem((8, FULL), f32)
    owner_scratch = [row_scratch] * (2 + SUMS)

    sent = vmem((SENT_ROWS, 128), bf16)
    hbm = pl.BlockSpec(memory_space=pltpu.HBM)
    up, down, flat, rows, order = pl.pallas_call(
        pack_kernel,
        in_specs=[hbm] * 3,
        out_specs=[pl.BlockSpec(memory_space=vmem)] * 5,
        out_shape=[
            sent, sent, vmem(flat.shape, f32), vmem(rows.shape, f32), vmem((1, ANGLES), jnp.int32)
        ],
        scratch_shapes=[vmem((SUBSETS * M_HALO, 128), f32), pltpu.SemaphoreType.DMA((3,))],
        compiler_params=pltpu.CompilerParams(vmem_limit_bytes=12 * 1024 * 1024),
        name="pack",
    )(*(pltpu.with_memory_space_constraint(x, pltpu.HBM) for x in (flat, rows, order)))
    next_up = [(i, (i + 1) % N_GZ) for i in range(N_GZ)]
    low = lax.ppermute(up, "gz", next_up)
    high = lax.ppermute(down, "gz", [(j, i) for i, j in next_up])
    w0, w1, own, mown, table = pl.pallas_call(
        prepare_kernel,
        in_specs=[pl.BlockSpec(memory_space=vmem)] * 3,
        out_specs=[pl.BlockSpec(memory_space=m) for m in (vmem, vmem, vmem, vmem, pltpu.SMEM)],
        out_shape=[
            made, made, slices, vmem((SUBSETS, VIEWS, 24, 128), f32), pltpu.SMEM(TABLE, jnp.int32)
        ],
        scratch_shapes=[
            vmem((VIEWS, TILES, VOXELS), f32), vmem(TABLE, jnp.int32), pltpu.SemaphoreType.DMA
        ],
        compiler_params=pltpu.CompilerParams(vmem_limit_bytes=12 * 1024 * 1024),
        name="prepare",
    )(*(pltpu.with_memory_space_constraint(x, vmem) for x in (order, flat, rows)))
    partial, side, m1 = call(
        first_kernel,
        (table, w0, own, mown, low, high),
        [vmem((N_XY * 12, 128), f32), slices, vmem((VIEWS, 64, 128), f32)],
        [
            vmem((SUBSETS, VIEWS, M_ROWS, 128), f32),
            vmem((VIEWS, 72, 128), f32),
            vmem((2, EDGE_ROWS, 128), f32),
            *acc_scratch,
        ],
        "first",
    )
    (rounded,) = call(
        functools.partial(owner_kernel, subset=0),
        (table, exchanged(partial, (N_XY, 3, 4, 128))),
        [vmem((N_XY, 8, 128), bf16)],
        owner_scratch,
        "owner_a",
    )
    partial, new = call(
        middle_kernel,
        (table, exchanged(rounded, rounded.shape), own, side, m1, w0, w1),
        [vmem((N_XY * 10, 128), f32), slices],
        [sm_scratch, vmem((TILES, Z_PAD, VOXELS), bf16), *acc_scratch],
        "middle",
    )
    (final,) = call(
        functools.partial(owner_kernel, subset=1),
        (table, exchanged(partial, (N_XY, 5, 2, 128))),
        [vmem((N_XY * 8, 128), f32)],
        owner_scratch,
        "owner_b",
    )
    volume_out, residual = call(
        last_kernel,
        (table, exchanged(final, (N_XY, 8, 128)), new, w1),
        [
            jax.ShapeDtypeStruct(VOLUME, f32),
            jax.ShapeDtypeStruct((VIEWS, ROWS_DEV, COLS_DEV), f32),
        ],
        [
            sm_scratch,
            slices,
            vmem(VOLUME, f32),
            vmem((VIEWS, ROWS_DEV, COLS_DEV), f32),
            pltpu.SemaphoreType.DMA((X_DEV // TILE + 1,)),
        ],
        "last",
    )
    return volume_out, residual


def solution(mesh):
    in_specs = (P("gz", "xy", None), P(None, None, "gz", "xy"), P())
    out_specs = (P("gz", "xy", None), P(None, "gz", "xy"))
    return jax.shard_map(local, mesh=mesh, in_specs=in_specs, out_specs=out_specs, check_vma=False)
```

```python
import functools
import math

import jax
import jax.numpy as jnp
from jax import lax
from jax.experimental import pallas as pl
from jax.experimental.pallas import tpu as pltpu
from jax.sharding import PartitionSpec as P

Z_DEV = 16
X_DEV = 48
NY = 128
COLS_DEV = 48
ROWS_DEV = 20
VIEWS = 5
SUBSETS = 2
ANGLES = 48
N_XY = 32
N_GZ = 8
NX = X_DEV * N_XY
NZ = Z_DEV * N_GZ
DR = ROWS_DEV * N_GZ
DC = COLS_DEV * N_XY

WIN = 176
LANES = 256
MEAS_AT = LANES - COLS_DEV
Z_HALO = 6
Z_ALL = Z_DEV + 2 * Z_HALO
ONES = Z_ALL
Z_PAD = 32
GROUPS = 6
GOT = GROUPS * 8
ROWS_PER = (5, 4)
ROWS_BELOW = (3, 0)
M_HALO = 8
M_ROWS = 40
FULL = 15 * 128
SUMS = 4
TILE = 16
TILES_Y = NY // TILE
TILES = X_DEV // TILE * TILES_Y
VOXELS = TILE * TILE
COLS_TILE = 40
VOLUME = (Z_DEV, X_DEV, NY)
PLACE = (0, 40, 80, 128, 168)
DEPTH = 208
HALO_ROWS = Z_HALO * X_DEV
EDGE_AT = HALO_ROWS
EDGE_ROWS = SUBSETS * VIEWS * M_HALO
SENT_ROWS = EDGE_AT + EDGE_ROWS
TABLE = (16, 128)
SHIFT_AT = 32
TILE_AT = 64


def iota(shape, dim):
    return lax.broadcasted_iota(jnp.int32, shape, dim)


def slice_of(i, gz):
    low = Z_DEV * gz - Z_HALO + (i - Z_DEV)
    high = Z_DEV * gz + Z_DEV + (i - Z_DEV - Z_HALO)
    return jnp.where(i < Z_DEV, Z_DEV * gz + i, jnp.where(i < Z_DEV + Z_HALO, low, high))


def hat(row, z):
    position = (DR - 1) / 2.0 + 0.96 * (DR / NZ) * (z.astype(jnp.float32) - (NZ - 1) / 2.0)
    value = jnp.maximum(0.0, 1.0 - jnp.abs(position - row.astype(jnp.float32)) / 2.0)
    ok = (row >= 0) & (row < DR) & (z >= 0) & (z < NZ)
    return jnp.where(ok, value, 0.0)


def first_row(gz, subset):
    return ROWS_DEV * gz - ROWS_BELOW[subset] - ((gz + 1) >> 1)


def slot_weights(group, slot, i, gz, subset):
    per = ROWS_PER[subset]
    row = first_row(gz, subset) + group * per + slot
    return jnp.where((slot < per) & (i < Z_ALL), hat(row, slice_of(i, gz)), 0.0)


def tile_offsets(table_ref, subset, tile):
    return [
        pl.multiple_of(table_ref[subset * VIEWS + v, TILE_AT + tile], 8) for v in range(VIEWS)
    ]


def coordinate(x, y, cosine, sine):
    xc = x - (NX - 1) / 2.0
    yc = y - (NY - 1) / 2.0
    source = 2.0 * NX
    along = xc * cosine + yc * sine
    depth = yc * cosine - xc * sine
    return (DC - 1) / 2.0 + 0.9 * (DC / NX) * along * source / (source + depth)


def fill_table(cosine, sine, xy):
    lane = iota(TABLE, 1)
    tile = lane - TILE_AT
    is_tile = lane >= TILE_AT
    strip = lane & (N_XY - 1)
    x = jnp.where(is_tile, xy * X_DEV + (tile >> 3) * TILE, strip * X_DEV).astype(jnp.float32)
    y = jnp.where(is_tile, (tile & 7) * TILE, 0).astype(jnp.float32)
    dx = jnp.where(is_tile, TILE - 1.0, X_DEV - 1.0)
    dy = jnp.where(is_tile, TILE - 1.0, NY - 1.0)
    least = jnp.minimum(
        jnp.minimum(coordinate(x, y, cosine, sine), coordinate(x + dx, y, cosine, sine)),
        jnp.minimum(coordinate(x, y + dy, cosine, sine), coordinate(x + dx, y + dy, cosine, sine)),
    )
    least = jnp.floor(least).astype(jnp.int32)
    start = least - 2
    own = jnp.sum(jnp.where(lane == xy, start, 0).astype(jnp.float32), axis=1, keepdims=True)
    tiles = jnp.maximum(least - 1 - own.astype(jnp.int32), 0) & ~7
    table = jnp.where(lane < SHIFT_AT, start & ~127, start & 127)
    return jnp.where(is_tile, tiles, table), own


def positions(u_ref, cosine, sine, own, subset, xy):
    t = iota((TILES, VOXELS), 0)
    l = iota((TILES, VOXELS), 1)
    x = ((t >> 3) * TILE + (l >> 4) + xy * X_DEV).astype(jnp.float32)
    y = ((t & 7) * TILE + (l & 15)).astype(jnp.float32)
    for v in range(VIEWS):
        at = subset * VIEWS + v
        u = coordinate(x, y, cosine[at : at + 1, 0:1], sine[at : at + 1, 0:1])
        u_ref[v] = u - own[at : at + 1, :]


def weights(u_ref, offsets, tile):
    c = iota((COLS_TILE, VOXELS), 0).astype(jnp.float32)
    pieces = []
    for v in range(VIEWS):
        u = u_ref[v, pl.ds(tile, 1), :] - offsets[v].astype(jnp.float32)
        pieces.append(jnp.maximum(0.0, 1.0 - jnp.abs(u - c)))
    pieces.insert(3, jnp.zeros((8, VOXELS), jnp.float32))
    return jnp.concatenate(pieces, axis=0).astype(jnp.bfloat16)


def forward(w_ref, slices, acc_refs, m_ref, table_ref, out_ref, subset, gz):
    for acc_ref in acc_refs:
        acc_ref[...] = jnp.zeros_like(acc_ref)
    for tile in range(TILES):
        offsets = tile_offsets(table_ref, subset, tile)
        part = lax.dot_general(
            w_ref[tile],
            jnp.concatenate([slices(tile)] * 4, axis=0),
            (((1,), (1,)), ((), ())),
            preferred_element_type=jnp.float32,
        )
        for v in range(VIEWS):
            acc_refs[v][pl.ds(offsets[v], COLS_TILE), :] += part[PLACE[v] : PLACE[v] + COLS_TILE]
    per = ROWS_PER[subset]
    half = per + 1
    size = GROUPS * 2 * half
    k = iota((size, 128), 0)
    lane = iota((size, 128), 1)
    i = lane & (Z_PAD - 1)
    group = (k * 43) >> 9 if half == 6 else (k * 205) >> 11
    slot = k - group * 2 * half
    is_low = slot < half
    slot = jnp.where(is_low, slot, slot - half)
    rows = slot_weights(group, slot, i, gz, subset)
    rows = jnp.where((slot == per) & (i == ONES), 1.0, rows)
    rounded = rows.astype(jnp.bfloat16).astype(jnp.float32)
    rows = jnp.where(lane < 2 * Z_PAD, rounded, rows - rounded).astype(jnp.bfloat16)
    left_over = (iota((WIN, 128), 1) & Z_PAD) != 0
    used = GROUPS * VIEWS * 2 * half
    out_ref[used:, :] = jnp.zeros((out_ref.shape[0] - used, 128), jnp.float32)
    for v in range(VIEWS):
        sums = acc_refs[v][...]
        rounded = sums.astype(jnp.bfloat16).astype(jnp.float32)
        sums = jnp.where(left_over, sums - rounded, rounded).astype(jnp.bfloat16)
        sums = lax.dot_general(
            rows, sums, (((1,), (1,)), ((), ())), preferred_element_type=jnp.float32
        )
        high = jnp.concatenate(
            (sums[:, 128:WIN], jnp.zeros((size, LANES - WIN), jnp.float32)), axis=1
        )
        part = jnp.where(is_low, sums[:, 0:128], high) + m_ref[v, 0:size, :]
        out_ref[v * size : (v + 1) * size, :] = part


def three_parts(x, third):
    first = x.astype(jnp.bfloat16).astype(jnp.float32)
    second = (x - first).astype(jnp.bfloat16).astype(jnp.float32)
    part = jnp.where(third == 0, first, jnp.where(third == 1, second, x - first - second))
    return part.astype(jnp.bfloat16)


def smear(recv_ref, sm_ref, gz):
    i = iota((3 * Z_PAD, 3 * GOT), 0)
    k = iota((3 * Z_PAD, 3 * GOT), 1)
    third = (k >= GOT).astype(jnp.int32) + (k >= 2 * GOT).astype(jnp.int32)
    k = k - GOT * third
    part = k & 7
    block = i >> 5
    slot = jnp.where(block == 0, part, 2 * (part - 5) + block - 1)
    rows = slot_weights(k >> 3, slot, i & (Z_PAD - 1), gz, 0)
    rows = three_parts(jnp.where((block == 0) == (part < 5), rows, 0.0), third)
    ones = iota((Z_PAD, LANES), 0) == ONES
    for v in range(VIEWS):
        got = recv_ref[v * GROUPS : (v + 1) * GROUPS].astype(jnp.float32)
        got = got.reshape(GOT, 128).astype(jnp.bfloat16)
        sums = jnp.dot(
            rows, jnp.concatenate((got, got, got), axis=0), preferred_element_type=jnp.float32
        )
        high = sums[Z_PAD : 2 * Z_PAD] + pltpu.roll(sums[2 * Z_PAD :], 128 - COLS_DEV, 1)
        smeared = jnp.concatenate((sums[0:Z_PAD], high), axis=1)
        sm_ref[v] = jnp.where(ones, 1.0, smeared).astype(jnp.bfloat16).astype(jnp.float32)


def smear_last(recv_ref, sm_ref, res_ref, gz):
    size = 2 * Z_PAD + 24
    i = iota((size, 3 * GOT), 0)
    k = iota((size, 3 * GOT), 1)
    third = (k >= GOT).astype(jnp.int32) + (k >= 2 * GOT).astype(jnp.int32)
    k = k - GOT * third
    part = k & 7
    rows = slot_weights(k >> 3, part & 3, i & (Z_PAD - 1), gz, 1)
    rows = three_parts(jnp.where((part >= 4) == (i >= Z_PAD), rows, 0.0), third)
    j = i - 2 * Z_PAD + ((gz + 1) >> 1)
    picked = jnp.where(k == ((j >> 2) << 3) + 4 + (j & 3), 1.0, 0.0).astype(jnp.bfloat16)
    rows = jnp.where(i >= 2 * Z_PAD, picked.astype(jnp.float32), rows.astype(jnp.float32))
    rows = rows.astype(jnp.bfloat16)
    ones = iota((Z_PAD, LANES), 0) == ONES
    part = iota((GOT, 128), 0) & 7
    exact = (part >= 4) & (iota((GOT, 128), 1) >= MEAS_AT - 128)
    for v in range(VIEWS):
        got = recv_ref[v * GOT : (v + 1) * GOT, :]
        first = got.astype(jnp.bfloat16).astype(jnp.float32)
        second = (got - first).astype(jnp.bfloat16).astype(jnp.float32)
        parts = (
            first,
            jnp.where(exact, second, first),
            jnp.where(exact, got - first - second, first),
        )
        sums = jnp.dot(
            rows,
            jnp.concatenate(parts, axis=0).astype(jnp.bfloat16),
            preferred_element_type=jnp.float32,
        )
        smeared = jnp.concatenate((sums[0:Z_PAD], sums[Z_PAD : 2 * Z_PAD]), axis=1)
        sm_ref[v] = jnp.where(ones, 1.0, smeared).astype(jnp.bfloat16).astype(jnp.float32)
        own = pltpu.roll(sums[2 * Z_PAD :], 256 - MEAS_AT, 1)
        res_ref[v] = own[0:ROWS_DEV, 0:COLS_DEV]


def windows(sm_ref, offsets):
    lane = iota((Z_PAD, 128), 1)
    placed = []
    for v in range(VIEWS):
        at = PLACE[v] & 127
        shift = (at - offsets[v]) & 127
        low = pltpu.roll(sm_ref[v, :, 0:128], shift, 1)
        high = pltpu.roll(sm_ref[v, :, 128:256], shift, 1)
        placed.append(jnp.where(lane < at + 128 - offsets[v], low, high))
    first = jnp.where(lane < 40, placed[0], jnp.where(lane < 80, placed[1], placed[2]))
    first = jnp.where(lane < 120, first, 0.0)
    second = jnp.where(lane < 40, placed[3], jnp.where(lane < 80, placed[4], 0.0))
    both = jnp.concatenate((first, second), axis=1)
    return both.astype(jnp.bfloat16)[:, 0:DEPTH]


def backward(w_ref, sm_ref, table_ref, old, store, subset, gz):
    zi = slice_of(iota((Z_PAD, LANES), 0), gz)
    inside = iota((Z_PAD, LANES), 0) < Z_ALL
    total = jnp.sum(jnp.where(inside, hat(iota((Z_PAD, LANES), 1), zi), 0.0), axis=1, keepdims=True)

    for tile in range(TILES):
        offsets = tile_offsets(table_ref, subset, tile)
        back = jnp.dot(
            windows(sm_ref, offsets), w_ref[tile], preferred_element_type=jnp.float32
        )
        norm = total * back[ONES : ONES + 1, :]
        store(tile, old(tile), back / jnp.maximum(norm, 1.0))


def swapped(rows, index, turn, axis):
    for d in (4, 2, 1):
        high = (index & d) != 0
        new = list(rows)
        for i in range(8):
            if i & d == 0:
                a, b = (rows[i], rows[i + d])
                new[i] = jnp.where(high, pltpu.roll(b, turn * d, axis), a)
                new[i + d] = jnp.where(high, b, pltpu.roll(a, turn * (8 - d), axis))
        rows = new
    return rows


def swap_blocks(rows):
    return swapped(rows, iota((8, 128), 1) >> 4, 16, 1)


def swap_sublanes(rows):
    return swapped(rows, iota((8, 128), 0), 1, 0)


def relay(read, out_ref, unrolled):
    def step(xb, nothing):
        for half in range(2):
            for b in range(2):
                x = xb * TILE + half * 8
                rows = swap_sublanes([read(b * 8 + z, x) for z in range(8)])
                for q, block in enumerate(swap_blocks(rows)):
                    out_ref[
                        xb * TILES_Y + q, b * 8 : b * 8 + 8, half * 128 : half * 128 + 128
                    ] = block
        return nothing

    if unrolled:
        for xb in range(X_DEV // TILE):
            step(xb, 0)
    else:
        lax.fori_loop(0, X_DEV // TILE, step, 0)


def pack_kernel(
    vol_hbm, meas_hbm, order_hbm, up_ref, down_ref, meas_ref, order_ref, row_ref, edge_ref, sems
):
    copies = [
        pltpu.make_async_copy(
            vol_hbm.at[pl.ds((Z_DEV - Z_HALO) * X_DEV, HALO_ROWS)], edge_ref.at[0], sems.at[0]
        ),
        pltpu.make_async_copy(vol_hbm.at[pl.ds(0, HALO_ROWS)], edge_ref.at[1], sems.at[3]),
        pltpu.make_async_copy(meas_hbm, meas_ref, sems.at[1]),
        pltpu.make_async_copy(order_hbm, order_ref, sems.at[2]),
    ]
    for copy in copies:
        copy.start()
    row_ref[...] = jnp.zeros_like(row_ref)
    for copy in copies:
        copy.wait()
    for side, (out_ref, r) in enumerate(((up_ref, ROWS_DEV - M_HALO), (down_ref, 0))):
        out_ref[0:HALO_ROWS, :] = edge_ref[side].astype(jnp.bfloat16)
        for v in range(VIEWS):
            at = (v * ROWS_DEV + r) * SUBSETS
            row_ref[:, 0:COLS_DEV] = meas_ref[at : at + SUBSETS * M_HALO, :]
            row = row_ref[...]
            rounded = row.astype(jnp.bfloat16).astype(jnp.float32)
            both = pltpu.roll(rounded, MEAS_AT - 128, 1)
            both = both + pltpu.roll(row - rounded, MEAS_AT - 128 - COLS_DEV, 1)
            at = EDGE_AT + v * SUBSETS * M_HALO
            out_ref[at : at + SUBSETS * M_HALO, :] = both.astype(jnp.bfloat16)


def prepare_kernel(
    order_ref, meas_ref, vol_hbm,
    w0_ref, w1_ref, own_ref, mown_ref, table_ref, u_ref, flat_ref, vol_ref, sem, vol_sem,
):
    xy = lax.axis_index("xy")
    volume = pltpu.make_async_copy(vol_hbm, vol_ref, vol_sem)
    volume.start()
    chosen = iota((TABLE[0], ANGLES), 0) == iota((TABLE[0], ANGLES), 1)
    chosen = jnp.where(chosen, order_ref[...].astype(jnp.float32), 0.0)
    chosen = jnp.broadcast_to(jnp.sum(chosen, axis=1, keepdims=True), TABLE)
    angles = 2.0 * math.pi * chosen / ANGLES
    cosine = jnp.cos(angles)
    sine = jnp.sin(angles)
    flat_ref[...], own = fill_table(cosine, sine, xy)
    copy = pltpu.make_async_copy(flat_ref, table_ref, sem)
    copy.start()
    mown_ref[...] = jnp.zeros_like(mown_ref)
    for s in range(SUBSETS):
        for v in range(VIEWS):
            for at, count in ((0, 8), (8, 8), (16, 4)):
                rows = meas_ref[pl.ds((v * ROWS_DEV + at) * 2 + s, count, stride=2), :]
                mown_ref[s, v, at : at + count, MEAS_AT - 128 : 128] = rows
    copy.wait()
    for subset, w_ref in ((0, w0_ref), (1, w1_ref)):
        positions(u_ref, cosine, sine, own, subset, xy)

        def step(tt, nothing):
            for t in range(8):
                tile = tt * 8 + t
                w_ref[tile] = weights(u_ref, tile_offsets(table_ref, subset, tile), tile)
            return nothing

        lax.fori_loop(0, TILES // 8, step, 0)
    volume.wait()
    relay(
        lambda z, x: vol_ref[pl.ds(pl.multiple_of(z * X_DEV + x, 8), 8), :], own_ref, False
    )


def first_kernel(
    table_ref, w_ref, own_ref, mown_ref, low_ref, high_ref,
    out_ref, side_ref, m1_ref, raw_ref, m0_ref, edge_ref, *acc_refs,
):
    gz = lax.axis_index("gz")
    for side, sent_ref in enumerate((low_ref, high_ref)):
        edge = sent_ref[EDGE_AT:SENT_ROWS, :].astype(jnp.float32)
        edge = edge + pltpu.roll(edge, COLS_DEV, 1)
        edge_ref[side] = jnp.where(iota(edge.shape, 1) >= MEAS_AT - 128, edge, 0.0)

    def read(z, x):
        if z >= 2 * Z_HALO:
            return jnp.full((8, NY), 1.0 if z == ONES - Z_DEV else 0.0, jnp.float32)
        sent_ref = low_ref if z < Z_HALO else high_ref
        at = z % Z_HALO * X_DEV + x
        return sent_ref[at : at + 8, :].astype(jnp.float32)

    relay(read, side_ref, True)
    for s, m_ref in ((0, m0_ref), (1, m1_ref)):
        per = ROWS_PER[s]
        m_ref[...] = jnp.zeros_like(m_ref)
        for v in range(VIEWS):
            edge = pl.ds(v * 2 * M_HALO + s, M_HALO, stride=2)
            high = edge_ref[1, edge, :]
            joined = jnp.concatenate(
                (
                    edge_ref[0, edge, :],
                    mown_ref[s, v, 0:16, :],
                    jnp.concatenate((mown_ref[s, v, 16:20, :], high[0:4]), axis=0),
                    jnp.concatenate((high[4:8], jnp.zeros((4, 128), jnp.float32)), axis=0),
                ),
                axis=0,
            )
            raw_ref[s, v] = pltpu.roll(
                joined, M_ROWS + ((gz + 1) >> 1) - (M_HALO - ROWS_BELOW[s]), 0
            )
            for group in range(GROUPS):
                at = group * 2 * (per + 1) + per + 1
                m_ref[v, at : at + per, :] = raw_ref[s, v, group * per : (group + 1) * per, :]

    def slices(tile):
        return jnp.concatenate((own_ref[tile], side_ref[tile]), axis=0).astype(jnp.bfloat16)

    forward(w_ref, slices, acc_refs, m0_ref, table_ref, out_ref, 0, gz)


def middle_kernel(
    table_ref, recv_ref, own_ref, side_ref, m_ref, w0_ref, w1_ref,
    out_ref, new_ref, sm_ref, vb_ref, *acc_refs,
):
    gz = lax.axis_index("gz")
    smear(recv_ref, sm_ref, gz)
    ones = iota((Z_PAD, VOXELS), 0) == ONES

    def old(tile):
        return jnp.concatenate((own_ref[tile], side_ref[tile]), axis=0)

    def store(tile, old, change):
        new = jnp.where(ones, 1.0, old + change)
        new_ref[tile] = new[0:Z_DEV]
        vb_ref[tile] = new.astype(jnp.bfloat16)

    backward(w0_ref, sm_ref, table_ref, old, store, 0, gz)
    forward(w1_ref, lambda tile: vb_ref[tile], acc_refs, m_ref, table_ref, out_ref, 1, gz)


def last_kernel(
    table_ref, recv_ref, old_ref, w_ref,
    out_ref, res_ref, sm_ref, new_ref, block_ref, own_ref, sems,
):
    gz = lax.axis_index("gz")
    smear_last(recv_ref, sm_ref, own_ref, gz)
    copies = [pltpu.make_async_copy(own_ref, res_ref, sems.at[X_DEV // TILE])]
    copies[0].start()

    def store(tile, old, change):
        new_ref[tile] = old + change[0:Z_DEV]
        xb = tile // TILES_Y
        if tile % TILES_Y < TILES_Y - 1:
            return
        for half in range(2):
            for b in range(Z_DEV // 8):
                blocks = [
                    new_ref[xb * TILES_Y + q, b * 8 : b * 8 + 8, half * 128 : half * 128 + 128]
                    for q in range(TILES_Y)
                ]
                x = xb * TILE + half * 8
                for z, row in enumerate(swap_sublanes(swap_blocks(blocks))):
                    block_ref[b * 8 + z, x : x + 8, :] = row
        columns = pl.ds(xb * TILE, TILE)
        copies.append(
            pltpu.make_async_copy(
                block_ref.at[:, columns, :], out_ref.at[:, columns, :], sems.at[xb]
            )
        )
        copies[-1].start()

    backward(w_ref, sm_ref, table_ref, lambda tile: old_ref[tile], store, 1, gz)
    for copy in copies:
        copy.wait()


def owner_kernel(table_ref, recv_ref, out_ref, acc_ref, mea_ref, *sum_refs, subset):
    gz = lax.axis_index("gz")
    xy = lax.axis_index("xy")
    view = jnp.minimum(xy // GROUPS, VIEWS - 1)
    group = xy % GROUPS
    at = subset * VIEWS + view
    per = ROWS_PER[subset]
    half = per + 1
    lane = iota((8, 128), 1)
    for sum_ref in sum_refs:
        sum_ref[...] = jnp.zeros_like(sum_ref)
    mea_ref[...] = jnp.zeros_like(mea_ref)
    end = N_XY * 2 * half - 8

    def upper(s):
        row = s * 2 * half + half
        last = recv_ref[min(row, end) : min(row, end) + 8, :]
        return pltpu.roll(last, 8 - (row - end), 0) if row > end else last

    for s in range(N_XY):
        column = s * COLS_DEV
        own = jnp.where(lane >= MEAS_AT - 128, upper(s), 0.0)
        own = pltpu.roll(own, (column + 256 - MEAS_AT) % 128, 1)
        block = column // 128 * 128
        offset = column - block
        mea_ref[:, block : block + 128] += jnp.where(lane >= offset, own, 0.0)
        if offset + COLS_DEV > 128:
            mea_ref[:, block + 128 : block + 256] += jnp.where(lane < offset, own, 0.0)
    for s in range(N_XY):
        base = pl.multiple_of(table_ref[at, s], 128)
        shift = table_ref[at, SHIFT_AT + s]
        row = s * 2 * half
        low = pltpu.roll(recv_ref[row : row + 8, :], shift, 1)
        high = pltpu.roll(jnp.where(lane < WIN - 128, upper(s), 0.0), shift, 1)
        wrapped = lane < shift
        part_ref = sum_refs[s % SUMS]
        part_ref[:, pl.ds(base, 128)] += jnp.where(wrapped, 0.0, low)
        part_ref[:, pl.ds(base + 128, 128)] += jnp.where(wrapped, low, high)
        part_ref[:, pl.ds(base + 256, 128)] += jnp.where(wrapped, high, 0.0)
    slot = iota((8, NZ), 0)
    row = first_row(gz, subset) + group * per + slot
    ray_rows = jnp.where(slot < per, hat(row, iota((8, NZ), 1)), 0.0)
    ray_rows = jnp.sum(ray_rows, axis=1, keepdims=True)
    sums = sum_refs[0][...]
    for part_ref in sum_refs[1:]:
        sums = sums + part_ref[...]
    totals = sums[per : per + 1, :]
    acc_ref[...] = mea_ref[...] - sums / jnp.maximum(ray_rows * totals, 1.0)
    for t in range(N_XY):
        base = pl.multiple_of(table_ref[at, t], 128)
        shift = table_ref[at, SHIFT_AT + t]
        back = (128 - shift) & 127
        a = pltpu.roll(acc_ref[:, pl.ds(base, 128)], back, 1)
        b = pltpu.roll(acc_ref[:, pl.ds(base + 128, 128)], back, 1)
        c = pltpu.roll(acc_ref[:, pl.ds(base + 256, 128)], back, 1)
        kept = lane < 128 - shift
        low = jnp.where(kept, a, b)
        high = jnp.where(kept, b, c)
        if subset == 0:
            other = pltpu.roll(high, COLS_DEV, 1)
            even = jnp.where(
                slot == 5,
                pltpu.roll(high, 5, 0),
                jnp.where(slot == 6, pltpu.roll(high, 4, 0), pltpu.roll(high, 3, 0)),
            )
            odd = jnp.where(slot == 5, pltpu.roll(other, 4, 0), pltpu.roll(other, 3, 0))
            rest = jnp.where(lane < COLS_DEV, even, odd)
            out_ref[t] = jnp.where(slot < 5, low, rest).astype(jnp.bfloat16)
            continue
        column = t * COLS_DEV
        block = column // 128 * 128
        offset = column - block
        turn = (MEAS_AT - 128 - offset) % 128
        own = pltpu.roll(acc_ref[:, block : block + 128], turn, 1)
        if offset + COLS_DEV > 128:
            more = pltpu.roll(acc_ref[:, block + 128 : block + 256], turn, 1)
            own = jnp.where(lane < MEAS_AT - offset, own, more)
        high = jnp.where(lane >= MEAS_AT - 128, own, high)
        out_ref[t * 8 : (t + 1) * 8, :] = jnp.where(slot < 4, low, pltpu.roll(high, 4, 0))


def call(kernel, inputs, outs, scratch, name):
    vmem = pl.BlockSpec(memory_space=pltpu.VMEM)
    smem = pl.BlockSpec(memory_space=pltpu.SMEM)
    anywhere = pl.BlockSpec(memory_space=pl.ANY)

    def spec(x):
        if x.dtype == jnp.int32:
            return smem
        return anywhere if isinstance(x, jax.ShapeDtypeStruct) else vmem

    inputs = [
        x if x.dtype == jnp.int32 else pltpu.with_memory_space_constraint(x, pltpu.VMEM)
        for x in inputs
    ]
    return pl.pallas_call(
        kernel,
        in_specs=[spec(x) for x in inputs],
        out_specs=[spec(x) for x in outs],
        out_shape=outs,
        scratch_shapes=scratch,
        compiler_params=pltpu.CompilerParams(vmem_limit_bytes=12 * 1024 * 1024),
        name=name,
    )(*inputs)


def exchanged(parts, shape):
    sent = lax.all_to_all(
        parts.reshape(shape), "xy", split_axis=0, concat_axis=0, tiled=True
    )
    return sent.reshape(parts.shape)


def local(volume, measured, view_order):
    f32 = jnp.float32
    bf16 = jnp.bfloat16
    vmem = pltpu.VMEM
    flat = volume.reshape(Z_DEV * X_DEV, NY)
    order = view_order.reshape(1, ANGLES)
    rows = measured.transpose(1, 2, 0, 3).reshape(VIEWS * ROWS_DEV * SUBSETS, COLS_DEV)
    made = vmem((TILES, DEPTH, VOXELS), bf16)
    slices = vmem((TILES, Z_DEV, VOXELS), f32)
    sm_scratch = vmem((VIEWS, Z_PAD, LANES), f32)
    acc_scratch = [vmem((WIN, 128), f32)] * VIEWS
    row_scratch = vmem((8, FULL), f32)
    owner_scratch = [row_scratch] * (2 + SUMS)

    sent = vmem((SENT_ROWS, 128), bf16)
    hbm = pl.BlockSpec(memory_space=pltpu.HBM)
    up, down, rows, order = pl.pallas_call(
        pack_kernel,
        in_specs=[hbm] * 3,
        out_specs=[pl.BlockSpec(memory_space=vmem)] * 4,
        out_shape=[sent, sent, vmem(rows.shape, f32), vmem((1, ANGLES), jnp.int32)],
        scratch_shapes=[
            vmem((SUBSETS * M_HALO, 128), f32),
            vmem((2, HALO_ROWS, NY), f32),
            pltpu.SemaphoreType.DMA((4,)),
        ],
        compiler_params=pltpu.CompilerParams(vmem_limit_bytes=12 * 1024 * 1024),
        name="pack",
    )(*(pltpu.with_memory_space_constraint(x, pltpu.HBM) for x in (flat, rows, order)))
    next_up = [(i, (i + 1) % N_GZ) for i in range(N_GZ)]
    low = lax.ppermute(up, "gz", next_up)
    high = lax.ppermute(down, "gz", [(j, i) for i, j in next_up])
    w0, w1, own, mown, table = pl.pallas_call(
        prepare_kernel,
        in_specs=[pl.BlockSpec(memory_space=vmem)] * 2 + [hbm],
        out_specs=[pl.BlockSpec(memory_space=m) for m in (vmem, vmem, vmem, vmem, pltpu.SMEM)],
        out_shape=[
            made, made, slices, vmem((SUBSETS, VIEWS, 24, 128), f32), pltpu.SMEM(TABLE, jnp.int32)
        ],
        scratch_shapes=[
            vmem((VIEWS, TILES, VOXELS), f32),
            vmem(TABLE, jnp.int32),
            vmem((Z_DEV * X_DEV, NY), f32),
            pltpu.SemaphoreType.DMA,
            pltpu.SemaphoreType.DMA,
        ],
        compiler_params=pltpu.CompilerParams(vmem_limit_bytes=12 * 1024 * 1024),
        name="prepare",
    )(
        *(pltpu.with_memory_space_constraint(x, vmem) for x in (order, rows)),
        pltpu.with_memory_space_constraint(flat, pltpu.HBM),
    )
    partial, side, m1 = call(
        first_kernel,
        (table, w0, own, mown, low, high),
        [vmem((N_XY * 12, 128), f32), slices, vmem((VIEWS, 64, 128), f32)],
        [
            vmem((SUBSETS, VIEWS, M_ROWS, 128), f32),
            vmem((VIEWS, 72, 128), f32),
            vmem((2, EDGE_ROWS, 128), f32),
            *acc_scratch,
        ],
        "first",
    )
    (rounded,) = call(
        functools.partial(owner_kernel, subset=0),
        (table, exchanged(partial, (N_XY, 3, 4, 128))),
        [vmem((N_XY, 8, 128), bf16)],
        owner_scratch,
        "owner_a",
    )
    partial, new = call(
        middle_kernel,
        (table, exchanged(rounded, rounded.shape), own, side, m1, w0, w1),
        [vmem((N_XY * 10, 128), f32), slices],
        [sm_scratch, vmem((TILES, Z_PAD, VOXELS), bf16), *acc_scratch],
        "middle",
    )
    (final,) = call(
        functools.partial(owner_kernel, subset=1),
        (table, exchanged(partial, (N_XY, 5, 2, 128))),
        [vmem((N_XY * 8, 128), f32)],
        owner_scratch,
        "owner_b",
    )
    volume_out, residual = call(
        last_kernel,
        (table, exchanged(final, (N_XY, 8, 128)), new, w1),
        [
            jax.ShapeDtypeStruct(VOLUME, f32),
            jax.ShapeDtypeStruct((VIEWS, ROWS_DEV, COLS_DEV), f32),
        ],
        [
            sm_scratch,
            slices,
            vmem(VOLUME, f32),
            vmem((VIEWS, ROWS_DEV, COLS_DEV), f32),
            pltpu.SemaphoreType.DMA((X_DEV // TILE + 1,)),
        ],
        "last",
    )
    return volume_out, residual


def solution(mesh):
    in_specs = (P("gz", "xy", None), P(None, None, "gz", "xy"), P())
    out_specs = (P("gz", "xy", None), P(None, "gz", "xy"))
    return jax.shard_map(local, mesh=mesh, in_specs=in_specs, out_specs=out_specs, check_vma=False)
```

```python
import functools
import math

import jax
import jax.numpy as jnp
from jax import lax
from jax.experimental import pallas as pl
from jax.experimental.pallas import tpu as pltpu
from jax.sharding import PartitionSpec as P

Z_DEV = 16
X_DEV = 48
NY = 128
COLS_DEV = 48
ROWS_DEV = 20
VIEWS = 5
SUBSETS = 2
ANGLES = 48
N_XY = 32
N_GZ = 8
NX = X_DEV * N_XY
NZ = Z_DEV * N_GZ
DR = ROWS_DEV * N_GZ
DC = COLS_DEV * N_XY

WIN = 176
LANES = 256
MEAS_AT = LANES - COLS_DEV
Z_HALO = 6
Z_ALL = Z_DEV + 2 * Z_HALO
ONES = Z_ALL
Z_PAD = 32
GROUPS = 6
GOT = GROUPS * 8
ROWS_PER = (5, 4)
ROWS_BELOW = (3, 0)
M_HALO = 8
M_ROWS = 40
FULL = 15 * 128
SUMS = 4
TILE = 16
TILES_Y = NY // TILE
TILES = X_DEV // TILE * TILES_Y
VOXELS = TILE * TILE
COLS_TILE = 40
VOLUME = (Z_DEV, X_DEV, NY)
PLACE = (0, 40, 80, 128, 168)
DEPTH = 208
HALO_ROWS = Z_HALO * X_DEV
EDGE_AT = HALO_ROWS
EDGE_ROWS = SUBSETS * VIEWS * M_HALO
SENT_ROWS = EDGE_AT + EDGE_ROWS
TABLE = (16, 128)
SHIFT_AT = 32
TILE_AT = 64


def iota(shape, dim):
    return lax.broadcasted_iota(jnp.int32, shape, dim)


def slice_of(i, gz):
    low = Z_DEV * gz - Z_HALO + (i - Z_DEV)
    high = Z_DEV * gz + Z_DEV + (i - Z_DEV - Z_HALO)
    return jnp.where(i < Z_DEV, Z_DEV * gz + i, jnp.where(i < Z_DEV + Z_HALO, low, high))


def hat(row, z):
    position = (DR - 1) / 2.0 + 0.96 * (DR / NZ) * (z.astype(jnp.float32) - (NZ - 1) / 2.0)
    value = jnp.maximum(0.0, 1.0 - jnp.abs(position - row.astype(jnp.float32)) / 2.0)
    ok = (row >= 0) & (row < DR) & (z >= 0) & (z < NZ)
    return jnp.where(ok, value, 0.0)


def first_row(gz, subset):
    return ROWS_DEV * gz - ROWS_BELOW[subset] - ((gz + 1) >> 1)


def slot_weights(group, slot, i, gz, subset):
    per = ROWS_PER[subset]
    row = first_row(gz, subset) + group * per + slot
    return jnp.where((slot < per) & (i < Z_ALL), hat(row, slice_of(i, gz)), 0.0)


def tile_offsets(table_ref, subset, tile):
    return [
        pl.multiple_of(table_ref[subset * VIEWS + v, TILE_AT + tile], 8) for v in range(VIEWS)
    ]


def coordinate(x, y, cosine, sine):
    xc = x - (NX - 1) / 2.0
    yc = y - (NY - 1) / 2.0
    source = 2.0 * NX
    along = xc * cosine + yc * sine
    depth = yc * cosine - xc * sine
    return (DC - 1) / 2.0 + 0.9 * (DC / NX) * along * source / (source + depth)


def fill_table(cosine, sine, xy):
    lane = iota(TABLE, 1)
    tile = lane - TILE_AT
    is_tile = lane >= TILE_AT
    strip = lane & (N_XY - 1)
    x = jnp.where(is_tile, xy * X_DEV + (tile >> 3) * TILE, strip * X_DEV).astype(jnp.float32)
    y = jnp.where(is_tile, (tile & 7) * TILE, 0).astype(jnp.float32)
    dx = jnp.where(is_tile, TILE - 1.0, X_DEV - 1.0)
    dy = jnp.where(is_tile, TILE - 1.0, NY - 1.0)
    least = jnp.minimum(
        jnp.minimum(coordinate(x, y, cosine, sine), coordinate(x + dx, y, cosine, sine)),
        jnp.minimum(coordinate(x, y + dy, cosine, sine), coordinate(x + dx, y + dy, cosine, sine)),
    )
    least = jnp.floor(least).astype(jnp.int32)
    start = least - 2
    own = jnp.sum(jnp.where(lane == xy, start, 0).astype(jnp.float32), axis=1, keepdims=True)
    tiles = jnp.maximum(least - 1 - own.astype(jnp.int32), 0) & ~7
    table = jnp.where(lane < SHIFT_AT, start & ~127, start & 127)
    return jnp.where(is_tile, tiles, table), own


def positions(u_ref, cosine, sine, own, subset, xy):
    t = iota((TILES, VOXELS), 0)
    l = iota((TILES, VOXELS), 1)
    x = ((t >> 3) * TILE + (l >> 4) + xy * X_DEV).astype(jnp.float32)
    y = ((t & 7) * TILE + (l & 15)).astype(jnp.float32)
    for v in range(VIEWS):
        at = subset * VIEWS + v
        u = coordinate(x, y, cosine[at : at + 1, 0:1], sine[at : at + 1, 0:1])
        u_ref[v] = u - own[at : at + 1, :]


def weights(u_ref, offsets, tile):
    c = iota((COLS_TILE, VOXELS), 0).astype(jnp.float32)
    pieces = []
    for v in range(VIEWS):
        u = u_ref[v, pl.ds(tile, 1), :] - offsets[v].astype(jnp.float32)
        pieces.append(jnp.maximum(0.0, 1.0 - jnp.abs(u - c)))
    pieces.insert(3, jnp.zeros((8, VOXELS), jnp.float32))
    return jnp.concatenate(pieces, axis=0).astype(jnp.bfloat16)


def forward(w_ref, slices, acc_refs, m_ref, table_ref, out_ref, subset, gz):
    for acc_ref in acc_refs:
        acc_ref[...] = jnp.zeros_like(acc_ref)
    for tile in range(TILES):
        offsets = tile_offsets(table_ref, subset, tile)
        part = lax.dot_general(
            w_ref[tile],
            jnp.concatenate([slices(tile)] * 3, axis=0),
            (((1,), (1,)), ((), ())),
            preferred_element_type=jnp.float32,
        )
        for v in range(VIEWS):
            acc_refs[v][pl.ds(offsets[v], COLS_TILE), :] += part[PLACE[v] : PLACE[v] + COLS_TILE]
    per = ROWS_PER[subset]
    half = per + 1
    size = GROUPS * 2 * half
    k = iota((size, 3 * Z_PAD), 0)
    lane = iota((size, 3 * Z_PAD), 1)
    i = lane & (Z_PAD - 1)
    group = (k * 43) >> 9 if half == 6 else (k * 205) >> 11
    slot = k - group * 2 * half
    is_low = slot < half
    slot = jnp.where(is_low, slot, slot - half)
    rows = slot_weights(group, slot, i, gz, subset)
    rows = jnp.where((slot == per) & (i == ONES), 1.0, rows)
    rounded = rows.astype(jnp.bfloat16).astype(jnp.float32)
    rows = jnp.where(lane < 2 * Z_PAD, rounded, rows - rounded).astype(jnp.bfloat16)
    left_over = (iota((WIN, 3 * Z_PAD), 1) & Z_PAD) != 0
    k = iota((size, 128), 0)
    group = (k * 43) >> 9 if half == 6 else (k * 205) >> 11
    is_low = k - group * 2 * half < half
    used = GROUPS * VIEWS * 2 * half
    out_ref[used:, :] = jnp.zeros((out_ref.shape[0] - used, 128), jnp.float32)
    for v in range(VIEWS):
        sums = acc_refs[v][...]
        rounded = sums.astype(jnp.bfloat16).astype(jnp.float32)
        sums = jnp.where(left_over, sums - rounded, rounded).astype(jnp.bfloat16)
        sums = lax.dot_general(
            rows, sums, (((1,), (1,)), ((), ())), preferred_element_type=jnp.float32
        )
        high = jnp.concatenate(
            (sums[:, 128:WIN], jnp.zeros((size, LANES - WIN), jnp.float32)), axis=1
        )
        part = jnp.where(is_low, sums[:, 0:128], high) + m_ref[v, 0:size, :]
        out_ref[v * size : (v + 1) * size, :] = part


def three_parts(x, third):
    first = x.astype(jnp.bfloat16).astype(jnp.float32)
    second = (x - first).astype(jnp.bfloat16).astype(jnp.float32)
    part = jnp.where(third == 0, first, jnp.where(third == 1, second, x - first - second))
    return part.astype(jnp.bfloat16)


def smear(recv_ref, sm_ref, gz):
    i = iota((3 * Z_PAD, 3 * GOT), 0)
    k = iota((3 * Z_PAD, 3 * GOT), 1)
    third = (k >= GOT).astype(jnp.int32) + (k >= 2 * GOT).astype(jnp.int32)
    k = k - GOT * third
    part = k & 7
    block = i >> 5
    slot = jnp.where(block == 0, part, 2 * (part - 5) + block - 1)
    rows = slot_weights(k >> 3, slot, i & (Z_PAD - 1), gz, 0)
    rows = three_parts(jnp.where((block == 0) == (part < 5), rows, 0.0), third)
    ones = iota((Z_PAD, LANES), 0) == ONES
    for v in range(VIEWS):
        got = recv_ref[v * GROUPS : (v + 1) * GROUPS].astype(jnp.float32)
        got = got.reshape(GOT, 128).astype(jnp.bfloat16)
        sums = jnp.dot(
            rows, jnp.concatenate((got, got, got), axis=0), preferred_element_type=jnp.float32
        )
        high = sums[Z_PAD : 2 * Z_PAD] + pltpu.roll(sums[2 * Z_PAD :], 128 - COLS_DEV, 1)
        smeared = jnp.concatenate((sums[0:Z_PAD], high), axis=1)
        sm_ref[v] = jnp.where(ones, 1.0, smeared).astype(jnp.bfloat16).astype(jnp.float32)


def smear_last(recv_ref, sm_ref, res_ref, gz):
    size = 2 * Z_PAD + 24
    i = iota((size, 3 * GOT), 0)
    k = iota((size, 3 * GOT), 1)
    third = (k >= GOT).astype(jnp.int32) + (k >= 2 * GOT).astype(jnp.int32)
    k = k - GOT * third
    part = k & 7
    rows = slot_weights(k >> 3, part & 3, i & (Z_PAD - 1), gz, 1)
    rows = three_parts(jnp.where((part >= 4) == (i >= Z_PAD), rows, 0.0), third)
    j = i - 2 * Z_PAD + ((gz + 1) >> 1)
    picked = jnp.where(k == ((j >> 2) << 3) + 4 + (j & 3), 1.0, 0.0).astype(jnp.bfloat16)
    rows = jnp.where(i >= 2 * Z_PAD, picked.astype(jnp.float32), rows.astype(jnp.float32))
    rows = rows.astype(jnp.bfloat16)
    ones = iota((Z_PAD, LANES), 0) == ONES
    part = iota((GOT, 128), 0) & 7
    exact = (part >= 4) & (iota((GOT, 128), 1) >= MEAS_AT - 128)
    for v in range(VIEWS):
        got = recv_ref[v * GOT : (v + 1) * GOT, :]
        first = got.astype(jnp.bfloat16).astype(jnp.float32)
        second = (got - first).astype(jnp.bfloat16).astype(jnp.float32)
        parts = (
            first,
            jnp.where(exact, second, first),
            jnp.where(exact, got - first - second, first),
        )
        sums = jnp.dot(
            rows,
            jnp.concatenate(parts, axis=0).astype(jnp.bfloat16),
            preferred_element_type=jnp.float32,
        )
        smeared = jnp.concatenate((sums[0:Z_PAD], sums[Z_PAD : 2 * Z_PAD]), axis=1)
        sm_ref[v] = jnp.where(ones, 1.0, smeared).astype(jnp.bfloat16).astype(jnp.float32)
        own = pltpu.roll(sums[2 * Z_PAD :], 256 - MEAS_AT, 1)
        res_ref[v] = own[0:ROWS_DEV, 0:COLS_DEV]


def windows(sm_ref, offsets):
    lane = iota((Z_PAD, 128), 1)
    placed = []
    for v in range(VIEWS):
        at = PLACE[v] & 127
        shift = (at - offsets[v]) & 127
        low = pltpu.roll(sm_ref[v, :, 0:128], shift, 1)
        high = pltpu.roll(sm_ref[v, :, 128:256], shift, 1)
        placed.append(jnp.where(lane < at + 128 - offsets[v], low, high))
    first = jnp.where(lane < 40, placed[0], jnp.where(lane < 80, placed[1], placed[2]))
    first = jnp.where(lane < 120, first, 0.0)
    second = jnp.where(lane < 40, placed[3], jnp.where(lane < 80, placed[4], 0.0))
    both = jnp.concatenate((first, second), axis=1)
    return both.astype(jnp.bfloat16)[:, 0:DEPTH]


def backward(w_ref, sm_ref, table_ref, old, store, subset, gz):
    zi = slice_of(iota((Z_PAD, LANES), 0), gz)
    inside = iota((Z_PAD, LANES), 0) < Z_ALL
    total = jnp.sum(jnp.where(inside, hat(iota((Z_PAD, LANES), 1), zi), 0.0), axis=1, keepdims=True)

    for tile in range(TILES):
        offsets = tile_offsets(table_ref, subset, tile)
        back = jnp.dot(
            windows(sm_ref, offsets), w_ref[tile], preferred_element_type=jnp.float32
        )
        norm = total * back[ONES : ONES + 1, :]
        store(tile, old(tile), back / jnp.maximum(norm, 1.0))


def swapped(rows, index, turn, axis):
    for d in (4, 2, 1):
        high = (index & d) != 0
        new = list(rows)
        for i in range(8):
            if i & d == 0:
                a, b = (rows[i], rows[i + d])
                new[i] = jnp.where(high, pltpu.roll(b, turn * d, axis), a)
                new[i + d] = jnp.where(high, b, pltpu.roll(a, turn * (8 - d), axis))
        rows = new
    return rows


def swap_blocks(rows):
    return swapped(rows, iota((8, 128), 1) >> 4, 16, 1)


def swap_sublanes(rows):
    return swapped(rows, iota((8, 128), 0), 1, 0)


def relay(read, out_ref, unrolled):
    def step(xb, nothing):
        for half in range(2):
            for b in range(2):
                x = xb * TILE + half * 8
                rows = swap_sublanes([read(b * 8 + z, x) for z in range(8)])
                for q, block in enumerate(swap_blocks(rows)):
                    out_ref[
                        xb * TILES_Y + q, b * 8 : b * 8 + 8, half * 128 : half * 128 + 128
                    ] = block
        return nothing

    if unrolled:
        for xb in range(X_DEV // TILE):
            step(xb, 0)
    else:
        lax.fori_loop(0, X_DEV // TILE, step, 0)


def pack_kernel(
    vol_hbm, meas_hbm, order_hbm, up_ref, down_ref, vol_ref, meas_ref, order_ref, row_ref, sems
):
    copies = [
        pltpu.make_async_copy(vol_hbm, vol_ref, sems.at[0]),
        pltpu.make_async_copy(meas_hbm, meas_ref, sems.at[1]),
        pltpu.make_async_copy(order_hbm, order_ref, sems.at[2]),
    ]
    for copy in copies:
        copy.start()
    row_ref[...] = jnp.zeros_like(row_ref)
    for copy in copies:
        copy.wait()
    for out_ref, z, r in (
        (up_ref, Z_DEV - Z_HALO, ROWS_DEV - M_HALO),
        (down_ref, 0, 0),
    ):
        slices = vol_ref[z * X_DEV : (z + Z_HALO) * X_DEV, :]
        out_ref[0:HALO_ROWS, :] = slices.astype(jnp.bfloat16)
        for v in range(VIEWS):
            at = (v * ROWS_DEV + r) * SUBSETS
            row_ref[:, 0:COLS_DEV] = meas_ref[at : at + SUBSETS * M_HALO, :]
            row = row_ref[...]
            rounded = row.astype(jnp.bfloat16).astype(jnp.float32)
            both = pltpu.roll(rounded, MEAS_AT - 128, 1)
            both = both + pltpu.roll(row - rounded, MEAS_AT - 128 - COLS_DEV, 1)
            at = EDGE_AT + v * SUBSETS * M_HALO
            out_ref[at : at + SUBSETS * M_HALO, :] = both.astype(jnp.bfloat16)


def prepare_kernel(
    order_ref, vol_ref, meas_ref,
    w0_ref, w1_ref, own_ref, mown_ref, table_ref, u_ref, flat_ref, sem,
):
    xy = lax.axis_index("xy")
    chosen = iota((TABLE[0], ANGLES), 0) == iota((TABLE[0], ANGLES), 1)
    chosen = jnp.where(chosen, order_ref[...].astype(jnp.float32), 0.0)
    chosen = jnp.broadcast_to(jnp.sum(chosen, axis=1, keepdims=True), TABLE)
    angles = 2.0 * math.pi * chosen / ANGLES
    cosine = jnp.cos(angles)
    sine = jnp.sin(angles)
    flat_ref[...], own = fill_table(cosine, sine, xy)
    copy = pltpu.make_async_copy(flat_ref, table_ref, sem)
    copy.start()
    relay(
        lambda z, x: vol_ref[pl.ds(pl.multiple_of(z * X_DEV + x, 8), 8), :], own_ref, False
    )
    mown_ref[...] = jnp.zeros_like(mown_ref)
    for s in range(SUBSETS):
        for v in range(VIEWS):
            for at, count in ((0, 8), (8, 8), (16, 4)):
                rows = meas_ref[pl.ds((v * ROWS_DEV + at) * 2 + s, count, stride=2), :]
                mown_ref[s, v, at : at + count, MEAS_AT - 128 : 128] = rows
    copy.wait()
    for subset, w_ref in ((0, w0_ref), (1, w1_ref)):
        positions(u_ref, cosine, sine, own, subset, xy)

        def step(tt, nothing):
            for t in range(8):
                tile = tt * 8 + t
                w_ref[tile] = weights(u_ref, tile_offsets(table_ref, subset, tile), tile)
            return nothing

        lax.fori_loop(0, TILES // 8, step, 0)


def first_kernel(
    table_ref, w_ref, own_ref, mown_ref, low_ref, high_ref,
    out_ref, side_ref, m1_ref, raw_ref, m0_ref, edge_ref, *acc_refs,
):
    gz = lax.axis_index("gz")
    for side, sent_ref in enumerate((low_ref, high_ref)):
        edge = sent_ref[EDGE_AT:SENT_ROWS, :].astype(jnp.float32)
        edge = edge + pltpu.roll(edge, COLS_DEV, 1)
        edge_ref[side] = jnp.where(iota(edge.shape, 1) >= MEAS_AT - 128, edge, 0.0)

    def read(z, x):
        if z >= 2 * Z_HALO:
            return jnp.full((8, NY), 1.0 if z == ONES - Z_DEV else 0.0, jnp.float32)
        sent_ref = low_ref if z < Z_HALO else high_ref
        at = z % Z_HALO * X_DEV + x
        return sent_ref[at : at + 8, :].astype(jnp.float32)

    relay(read, side_ref, True)
    for s, m_ref in ((0, m0_ref), (1, m1_ref)):
        per = ROWS_PER[s]
        m_ref[...] = jnp.zeros_like(m_ref)
        for v in range(VIEWS):
            edge = pl.ds(v * 2 * M_HALO + s, M_HALO, stride=2)
            high = edge_ref[1, edge, :]
            joined = jnp.concatenate(
                (
                    edge_ref[0, edge, :],
                    mown_ref[s, v, 0:16, :],
                    jnp.concatenate((mown_ref[s, v, 16:20, :], high[0:4]), axis=0),
                    jnp.concatenate((high[4:8], jnp.zeros((4, 128), jnp.float32)), axis=0),
                ),
                axis=0,
            )
            raw_ref[s, v] = pltpu.roll(
                joined, M_ROWS + ((gz + 1) >> 1) - (M_HALO - ROWS_BELOW[s]), 0
            )
            for group in range(GROUPS):
                at = group * 2 * (per + 1) + per + 1
                m_ref[v, at : at + per, :] = raw_ref[s, v, group * per : (group + 1) * per, :]

    def slices(tile):
        return jnp.concatenate((own_ref[tile], side_ref[tile]), axis=0).astype(jnp.bfloat16)

    forward(w_ref, slices, acc_refs, m0_ref, table_ref, out_ref, 0, gz)


def middle_kernel(
    table_ref, recv_ref, own_ref, side_ref, m_ref, w0_ref, w1_ref,
    out_ref, new_ref, sm_ref, vb_ref, *acc_refs,
):
    gz = lax.axis_index("gz")
    smear(recv_ref, sm_ref, gz)
    ones = iota((Z_PAD, VOXELS), 0) == ONES

    def old(tile):
        return jnp.concatenate((own_ref[tile], side_ref[tile]), axis=0)

    def store(tile, old, change):
        new = jnp.where(ones, 1.0, old + change)
        new_ref[tile] = new[0:Z_DEV]
        vb_ref[tile] = new.astype(jnp.bfloat16)

    backward(w0_ref, sm_ref, table_ref, old, store, 0, gz)
    forward(w1_ref, lambda tile: vb_ref[tile], acc_refs, m_ref, table_ref, out_ref, 1, gz)


def last_kernel(
    table_ref, recv_ref, old_ref, w_ref,
    out_ref, res_ref, sm_ref, new_ref, block_ref, own_ref, sems,
):
    gz = lax.axis_index("gz")
    smear_last(recv_ref, sm_ref, own_ref, gz)
    copies = [pltpu.make_async_copy(own_ref, res_ref, sems.at[X_DEV // TILE])]
    copies[0].start()

    def store(tile, old, change):
        new_ref[tile] = old + change[0:Z_DEV]
        xb = tile // TILES_Y
        if tile % TILES_Y < TILES_Y - 1:
            return
        for half in range(2):
            for b in range(Z_DEV // 8):
                blocks = [
                    new_ref[xb * TILES_Y + q, b * 8 : b * 8 + 8, half * 128 : half * 128 + 128]
                    for q in range(TILES_Y)
                ]
                x = xb * TILE + half * 8
                for z, row in enumerate(swap_sublanes(swap_blocks(blocks))):
                    block_ref[b * 8 + z, x : x + 8, :] = row
        columns = pl.ds(xb * TILE, TILE)
        copies.append(
            pltpu.make_async_copy(
                block_ref.at[:, columns, :], out_ref.at[:, columns, :], sems.at[xb]
            )
        )
        copies[-1].start()

    backward(w_ref, sm_ref, table_ref, lambda tile: old_ref[tile], store, 1, gz)
    for copy in copies:
        copy.wait()


def owner_kernel(table_ref, recv_ref, out_ref, acc_ref, mea_ref, *sum_refs, subset):
    gz = lax.axis_index("gz")
    xy = lax.axis_index("xy")
    view = jnp.minimum(xy // GROUPS, VIEWS - 1)
    group = xy % GROUPS
    at = subset * VIEWS + view
    per = ROWS_PER[subset]
    half = per + 1
    lane = iota((8, 128), 1)
    for sum_ref in sum_refs:
        sum_ref[...] = jnp.zeros_like(sum_ref)
    mea_ref[...] = jnp.zeros_like(mea_ref)
    end = N_XY * 2 * half - 8

    def upper(s):
        row = s * 2 * half + half
        last = recv_ref[min(row, end) : min(row, end) + 8, :]
        return pltpu.roll(last, 8 - (row - end), 0) if row > end else last

    for s in range(N_XY):
        column = s * COLS_DEV
        own = jnp.where(lane >= MEAS_AT - 128, upper(s), 0.0)
        own = pltpu.roll(own, (column + 256 - MEAS_AT) % 128, 1)
        block = column // 128 * 128
        offset = column - block
        mea_ref[:, block : block + 128] += jnp.where(lane >= offset, own, 0.0)
        if offset + COLS_DEV > 128:
            mea_ref[:, block + 128 : block + 256] += jnp.where(lane < offset, own, 0.0)
    for s in range(N_XY):
        base = pl.multiple_of(table_ref[at, s], 128)
        shift = table_ref[at, SHIFT_AT + s]
        row = s * 2 * half
        low = pltpu.roll(recv_ref[row : row + 8, :], shift, 1)
        high = pltpu.roll(jnp.where(lane < WIN - 128, upper(s), 0.0), shift, 1)
        wrapped = lane < shift
        part_ref = sum_refs[s % SUMS]
        part_ref[:, pl.ds(base, 128)] += jnp.where(wrapped, 0.0, low)
        part_ref[:, pl.ds(base + 128, 128)] += jnp.where(wrapped, low, high)
        part_ref[:, pl.ds(base + 256, 128)] += jnp.where(wrapped, high, 0.0)
    slot = iota((8, NZ), 0)
    row = first_row(gz, subset) + group * per + slot
    ray_rows = jnp.where(slot < per, hat(row, iota((8, NZ), 1)), 0.0)
    ray_rows = jnp.sum(ray_rows, axis=1, keepdims=True)
    sums = sum_refs[0][...]
    for part_ref in sum_refs[1:]:
        sums = sums + part_ref[...]
    totals = sums[per : per + 1, :]
    acc_ref[...] = mea_ref[...] - sums / jnp.maximum(ray_rows * totals, 1.0)
    for t in range(N_XY):
        base = pl.multiple_of(table_ref[at, t], 128)
        shift = table_ref[at, SHIFT_AT + t]
        back = (128 - shift) & 127
        a = pltpu.roll(acc_ref[:, pl.ds(base, 128)], back, 1)
        b = pltpu.roll(acc_ref[:, pl.ds(base + 128, 128)], back, 1)
        c = pltpu.roll(acc_ref[:, pl.ds(base + 256, 128)], back, 1)
        kept = lane < 128 - shift
        low = jnp.where(kept, a, b)
        high = jnp.where(kept, b, c)
        if subset == 0:
            other = pltpu.roll(high, COLS_DEV, 1)
            even = jnp.where(
                slot == 5,
                pltpu.roll(high, 5, 0),
                jnp.where(slot == 6, pltpu.roll(high, 4, 0), pltpu.roll(high, 3, 0)),
            )
            odd = jnp.where(slot == 5, pltpu.roll(other, 4, 0), pltpu.roll(other, 3, 0))
            rest = jnp.where(lane < COLS_DEV, even, odd)
            out_ref[t] = jnp.where(slot < 5, low, rest).astype(jnp.bfloat16)
            continue
        column = t * COLS_DEV
        block = column // 128 * 128
        offset = column - block
        turn = (MEAS_AT - 128 - offset) % 128
        own = pltpu.roll(acc_ref[:, block : block + 128], turn, 1)
        if offset + COLS_DEV > 128:
            more = pltpu.roll(acc_ref[:, block + 128 : block + 256], turn, 1)
            own = jnp.where(lane < MEAS_AT - offset, own, more)
        high = jnp.where(lane >= MEAS_AT - 128, own, high)
        out_ref[t * 8 : (t + 1) * 8, :] = jnp.where(slot < 4, low, pltpu.roll(high, 4, 0))


def call(kernel, inputs, outs, scratch, name):
    vmem = pl.BlockSpec(memory_space=pltpu.VMEM)
    smem = pl.BlockSpec(memory_space=pltpu.SMEM)
    anywhere = pl.BlockSpec(memory_space=pl.ANY)

    def spec(x):
        if x.dtype == jnp.int32:
            return smem
        return anywhere if isinstance(x, jax.ShapeDtypeStruct) else vmem

    inputs = [
        x if x.dtype == jnp.int32 else pltpu.with_memory_space_constraint(x, pltpu.VMEM)
        for x in inputs
    ]
    return pl.pallas_call(
        kernel,
        in_specs=[spec(x) for x in inputs],
        out_specs=[spec(x) for x in outs],
        out_shape=outs,
        scratch_shapes=scratch,
        compiler_params=pltpu.CompilerParams(vmem_limit_bytes=12 * 1024 * 1024),
        name=name,
    )(*inputs)


def exchanged(parts, shape):
    sent = lax.all_to_all(
        parts.reshape(shape), "xy", split_axis=0, concat_axis=0, tiled=True
    )
    return sent.reshape(parts.shape)


def local(volume, measured, view_order):
    f32 = jnp.float32
    bf16 = jnp.bfloat16
    vmem = pltpu.VMEM
    flat = volume.reshape(Z_DEV * X_DEV, NY)
    order = view_order.reshape(1, ANGLES)
    rows = measured.transpose(1, 2, 0, 3).reshape(VIEWS * ROWS_DEV * SUBSETS, COLS_DEV)
    made = vmem((TILES, DEPTH, VOXELS), bf16)
    slices = vmem((TILES, Z_DEV, VOXELS), f32)
    sm_scratch = vmem((VIEWS, Z_PAD, LANES), f32)
    acc_scratch = [vmem((WIN, 3 * Z_PAD), f32)] * VIEWS
    row_scratch = vmem((8, FULL), f32)
    owner_scratch = [row_scratch] * (2 + SUMS)

    sent = vmem((SENT_ROWS, 128), bf16)
    hbm = pl.BlockSpec(memory_space=pltpu.HBM)
    up, down, flat, rows, order = pl.pallas_call(
        pack_kernel,
        in_specs=[hbm] * 3,
        out_specs=[pl.BlockSpec(memory_space=vmem)] * 5,
        out_shape=[
            sent, sent, vmem(flat.shape, f32), vmem(rows.shape, f32), vmem((1, ANGLES), jnp.int32)
        ],
        scratch_shapes=[vmem((SUBSETS * M_HALO, 128), f32), pltpu.SemaphoreType.DMA((3,))],
        compiler_params=pltpu.CompilerParams(vmem_limit_bytes=12 * 1024 * 1024),
        name="pack",
    )(*(pltpu.with_memory_space_constraint(x, pltpu.HBM) for x in (flat, rows, order)))
    next_up = [(i, (i + 1) % N_GZ) for i in range(N_GZ)]
    low = lax.ppermute(up, "gz", next_up)
    high = lax.ppermute(down, "gz", [(j, i) for i, j in next_up])
    w0, w1, own, mown, table = pl.pallas_call(
        prepare_kernel,
        in_specs=[pl.BlockSpec(memory_space=vmem)] * 3,
        out_specs=[pl.BlockSpec(memory_space=m) for m in (vmem, vmem, vmem, vmem, pltpu.SMEM)],
        out_shape=[
            made, made, slices, vmem((SUBSETS, VIEWS, 24, 128), f32), pltpu.SMEM(TABLE, jnp.int32)
        ],
        scratch_shapes=[
            vmem((VIEWS, TILES, VOXELS), f32), vmem(TABLE, jnp.int32), pltpu.SemaphoreType.DMA
        ],
        compiler_params=pltpu.CompilerParams(vmem_limit_bytes=12 * 1024 * 1024),
        name="prepare",
    )(*(pltpu.with_memory_space_constraint(x, vmem) for x in (order, flat, rows)))
    partial, side, m1 = call(
        first_kernel,
        (table, w0, own, mown, low, high),
        [vmem((N_XY * 12, 128), f32), slices, vmem((VIEWS, 64, 128), f32)],
        [
            vmem((SUBSETS, VIEWS, M_ROWS, 128), f32),
            vmem((VIEWS, 72, 128), f32),
            vmem((2, EDGE_ROWS, 128), f32),
            *acc_scratch,
        ],
        "first",
    )
    (rounded,) = call(
        functools.partial(owner_kernel, subset=0),
        (table, exchanged(partial, (N_XY, 3, 4, 128))),
        [vmem((N_XY, 8, 128), bf16)],
        owner_scratch,
        "owner_a",
    )
    partial, new = call(
        middle_kernel,
        (table, exchanged(rounded, rounded.shape), own, side, m1, w0, w1),
        [vmem((N_XY * 10, 128), f32), slices],
        [sm_scratch, vmem((TILES, Z_PAD, VOXELS), bf16), *acc_scratch],
        "middle",
    )
    (final,) = call(
        functools.partial(owner_kernel, subset=1),
        (table, exchanged(partial, (N_XY, 5, 2, 128))),
        [vmem((N_XY * 8, 128), f32)],
        owner_scratch,
        "owner_b",
    )
    volume_out, residual = call(
        last_kernel,
        (table, exchanged(final, (N_XY, 8, 128)), new, w1),
        [
            jax.ShapeDtypeStruct(VOLUME, f32),
            jax.ShapeDtypeStruct((VIEWS, ROWS_DEV, COLS_DEV), f32),
        ],
        [
            sm_scratch,
            slices,
            vmem(VOLUME, f32),
            vmem((VIEWS, ROWS_DEV, COLS_DEV), f32),
            pltpu.SemaphoreType.DMA((X_DEV // TILE + 1,)),
        ],
        "last",
    )
    return volume_out, residual


def solution(mesh):
    in_specs = (P("gz", "xy", None), P(None, None, "gz", "xy"), P())
    out_specs = (P("gz", "xy", None), P(None, "gz", "xy"))
    return jax.shard_map(local, mesh=mesh, in_specs=in_specs, out_specs=out_specs, check_vma=False)
```

```python
import functools
import math

import jax
import jax.numpy as jnp
from jax import lax
from jax.experimental import pallas as pl
from jax.experimental.pallas import tpu as pltpu
from jax.sharding import PartitionSpec as P

Z_DEV = 16
X_DEV = 48
NY = 128
COLS_DEV = 48
ROWS_DEV = 20
VIEWS = 5
SUBSETS = 2
ANGLES = 48
N_XY = 32
N_GZ = 8
NX = X_DEV * N_XY
NZ = Z_DEV * N_GZ
DR = ROWS_DEV * N_GZ
DC = COLS_DEV * N_XY

WIN = 176
LANES = 256
MEAS_AT = LANES - COLS_DEV
Z_HALO = 6
Z_ALL = Z_DEV + 2 * Z_HALO
ONES = Z_ALL
Z_PAD = 32
GROUPS = 6
GOT = GROUPS * 8
ROWS_PER = (5, 4)
ROWS_BELOW = (3, 0)
M_HALO = 8
M_ROWS = 40
FULL = 15 * 128
SUMS = 4
TILE = 16
TILES_Y = NY // TILE
TILES = X_DEV // TILE * TILES_Y
VOXELS = TILE * TILE
COLS_TILE = 40
VOLUME = (Z_DEV, X_DEV, NY)
PLACE = (0, 40, 80, 128, 168)
DEPTH = 208
HALO_ROWS = Z_HALO * X_DEV
EDGE_AT = HALO_ROWS
EDGE_ROWS = SUBSETS * VIEWS * M_HALO
SENT_ROWS = EDGE_AT + EDGE_ROWS
TABLE = (16, 128)
SHIFT_AT = 32
TILE_AT = 64


def iota(shape, dim):
    return lax.broadcasted_iota(jnp.int32, shape, dim)


def slice_of(i, gz):
    low = Z_DEV * gz - Z_HALO + (i - Z_DEV)
    high = Z_DEV * gz + Z_DEV + (i - Z_DEV - Z_HALO)
    return jnp.where(i < Z_DEV, Z_DEV * gz + i, jnp.where(i < Z_DEV + Z_HALO, low, high))


def hat(row, z):
    position = (DR - 1) / 2.0 + 0.96 * (DR / NZ) * (z.astype(jnp.float32) - (NZ - 1) / 2.0)
    value = jnp.maximum(0.0, 1.0 - jnp.abs(position - row.astype(jnp.float32)) / 2.0)
    ok = (row >= 0) & (row < DR) & (z >= 0) & (z < NZ)
    return jnp.where(ok, value, 0.0)


def first_row(gz, subset):
    return ROWS_DEV * gz - ROWS_BELOW[subset] - ((gz + 1) >> 1)


def slot_weights(group, slot, i, gz, subset):
    per = ROWS_PER[subset]
    row = first_row(gz, subset) + group * per + slot
    return jnp.where((slot < per) & (i < Z_ALL), hat(row, slice_of(i, gz)), 0.0)


def tile_offsets(table_ref, subset, tile):
    return [
        pl.multiple_of(table_ref[subset * VIEWS + v, TILE_AT + tile], 8) for v in range(VIEWS)
    ]


def coordinate(x, y, cosine, sine):
    xc = x - (NX - 1) / 2.0
    yc = y - (NY - 1) / 2.0
    source = 2.0 * NX
    along = xc * cosine + yc * sine
    depth = yc * cosine - xc * sine
    return (DC - 1) / 2.0 + 0.9 * (DC / NX) * along * source / (source + depth)


def fill_table(cosine, sine, xy):
    lane = iota(TABLE, 1)
    tile = lane - TILE_AT
    is_tile = lane >= TILE_AT
    strip = lane & (N_XY - 1)
    x = jnp.where(is_tile, xy * X_DEV + (tile >> 3) * TILE, strip * X_DEV).astype(jnp.float32)
    y = jnp.where(is_tile, (tile & 7) * TILE, 0).astype(jnp.float32)
    dx = jnp.where(is_tile, TILE - 1.0, X_DEV - 1.0)
    dy = jnp.where(is_tile, TILE - 1.0, NY - 1.0)
    least = jnp.minimum(
        jnp.minimum(coordinate(x, y, cosine, sine), coordinate(x + dx, y, cosine, sine)),
        jnp.minimum(coordinate(x, y + dy, cosine, sine), coordinate(x + dx, y + dy, cosine, sine)),
    )
    least = jnp.floor(least).astype(jnp.int32)
    start = least - 2
    own = jnp.sum(jnp.where(lane == xy, start, 0).astype(jnp.float32), axis=1, keepdims=True)
    tiles = jnp.maximum(least - 1 - own.astype(jnp.int32), 0) & ~7
    table = jnp.where(lane < SHIFT_AT, start & ~127, start & 127)
    return jnp.where(is_tile, tiles, table), own


def positions(u_ref, cosine, sine, own, subset, xy):
    t = iota((TILES, VOXELS), 0)
    l = iota((TILES, VOXELS), 1)
    x = ((t >> 3) * TILE + (l >> 4) + xy * X_DEV).astype(jnp.float32)
    y = ((t & 7) * TILE + (l & 15)).astype(jnp.float32)
    for v in range(VIEWS):
        at = subset * VIEWS + v
        u = coordinate(x, y, cosine[at : at + 1, 0:1], sine[at : at + 1, 0:1])
        u_ref[v] = u - own[at : at + 1, :]


def weights(u_ref, offsets, tile):
    c = iota((COLS_TILE, VOXELS), 0).astype(jnp.float32)
    pieces = []
    for v in range(VIEWS):
        u = u_ref[v, pl.ds(tile, 1), :] - offsets[v].astype(jnp.float32)
        pieces.append(jnp.maximum(0.0, 1.0 - jnp.abs(u - c)))
    pieces.insert(3, jnp.zeros((8, VOXELS), jnp.float32))
    return jnp.concatenate(pieces, axis=0).astype(jnp.bfloat16)


def forward(w_ref, slices, acc_refs, m_ref, table_ref, out_ref, subset, gz):
    for acc_ref in acc_refs:
        acc_ref[...] = jnp.zeros_like(acc_ref)
    for tile in range(TILES):
        offsets = tile_offsets(table_ref, subset, tile)
        part = lax.dot_general(
            w_ref[tile],
            jnp.concatenate([slices(tile)] * 4, axis=0),
            (((1,), (1,)), ((), ())),
            preferred_element_type=jnp.float32,
        )
        for v in range(VIEWS):
            acc_refs[v][pl.ds(offsets[v], COLS_TILE), :] += part[PLACE[v] : PLACE[v] + COLS_TILE]
    per = ROWS_PER[subset]
    half = per + 1
    size = GROUPS * 2 * half
    k = iota((size, 128), 0)
    lane = iota((size, 128), 1)
    i = lane & (Z_PAD - 1)
    group = (k * 43) >> 9 if half == 6 else (k * 205) >> 11
    slot = k - group * 2 * half
    is_low = slot < half
    slot = jnp.where(is_low, slot, slot - half)
    rows = slot_weights(group, slot, i, gz, subset)
    rows = jnp.where((slot == per) & (i == ONES), 1.0, rows)
    rounded = rows.astype(jnp.bfloat16).astype(jnp.float32)
    rows = jnp.where(lane < 2 * Z_PAD, rounded, rows - rounded).astype(jnp.bfloat16)
    left_over = (iota((WIN, 128), 1) & Z_PAD) != 0
    used = GROUPS * VIEWS * 2 * half
    out_ref[used:, :] = jnp.zeros((out_ref.shape[0] - used, 128), jnp.float32)
    for v in range(VIEWS):
        sums = acc_refs[v][...]
        rounded = sums.astype(jnp.bfloat16).astype(jnp.float32)
        sums = jnp.where(left_over, sums - rounded, rounded).astype(jnp.bfloat16)
        sums = lax.dot_general(
            rows, sums, (((1,), (1,)), ((), ())), preferred_element_type=jnp.float32
        )
        high = jnp.concatenate(
            (sums[:, 128:WIN], jnp.zeros((size, LANES - WIN), jnp.float32)), axis=1
        )
        part = jnp.where(is_low, sums[:, 0:128], high) + m_ref[v, 0:size, :]
        out_ref[v * size : (v + 1) * size, :] = part


def three_parts(x, third):
    first = x.astype(jnp.bfloat16).astype(jnp.float32)
    second = (x - first).astype(jnp.bfloat16).astype(jnp.float32)
    part = jnp.where(third == 0, first, jnp.where(third == 1, second, x - first - second))
    return part.astype(jnp.bfloat16)


def smear(recv_ref, sm_ref, gz):
    i = iota((3 * Z_PAD, 3 * GOT), 0)
    k = iota((3 * Z_PAD, 3 * GOT), 1)
    third = (k >= GOT).astype(jnp.int32) + (k >= 2 * GOT).astype(jnp.int32)
    k = k - GOT * third
    part = k & 7
    block = i >> 5
    slot = jnp.where(block == 0, part, 2 * (part - 5) + block - 1)
    rows = slot_weights(k >> 3, slot, i & (Z_PAD - 1), gz, 0)
    rows = three_parts(jnp.where((block == 0) == (part < 5), rows, 0.0), third)
    ones = iota((Z_PAD, LANES), 0) == ONES
    for v in range(VIEWS):
        got = recv_ref[v * GROUPS : (v + 1) * GROUPS].astype(jnp.float32)
        got = got.reshape(GOT, 128).astype(jnp.bfloat16)
        sums = jnp.dot(
            rows, jnp.concatenate((got, got, got), axis=0), preferred_element_type=jnp.float32
        )
        high = sums[Z_PAD : 2 * Z_PAD] + pltpu.roll(sums[2 * Z_PAD :], 128 - COLS_DEV, 1)
        smeared = jnp.concatenate((sums[0:Z_PAD], high), axis=1)
        sm_ref[v] = jnp.where(ones, 1.0, smeared).astype(jnp.bfloat16).astype(jnp.float32)


def smear_last(recv_ref, sm_ref, res_ref, gz):
    size = 2 * Z_PAD + 24
    i = iota((size, 3 * GOT), 0)
    k = iota((size, 3 * GOT), 1)
    third = (k >= GOT).astype(jnp.int32) + (k >= 2 * GOT).astype(jnp.int32)
    k = k - GOT * third
    part = k & 7
    rows = slot_weights(k >> 3, part & 3, i & (Z_PAD - 1), gz, 1)
    rows = three_parts(jnp.where((part >= 4) == (i >= Z_PAD), rows, 0.0), third)
    j = i - 2 * Z_PAD + ((gz + 1) >> 1)
    picked = jnp.where(k == ((j >> 2) << 3) + 4 + (j & 3), 1.0, 0.0).astype(jnp.bfloat16)
    rows = jnp.where(i >= 2 * Z_PAD, picked.astype(jnp.float32), rows.astype(jnp.float32))
    rows = rows.astype(jnp.bfloat16)
    ones = iota((Z_PAD, LANES), 0) == Z_DEV
    part = iota((GOT, 128), 0) & 7
    exact = (part >= 4) & (iota((GOT, 128), 1) >= MEAS_AT - 128)
    for v in range(VIEWS):
        got = recv_ref[v * GOT : (v + 1) * GOT, :]
        first = got.astype(jnp.bfloat16).astype(jnp.float32)
        second = (got - first).astype(jnp.bfloat16).astype(jnp.float32)
        parts = (
            first,
            jnp.where(exact, second, first),
            jnp.where(exact, got - first - second, first),
        )
        sums = jnp.dot(
            rows,
            jnp.concatenate(parts, axis=0).astype(jnp.bfloat16),
            preferred_element_type=jnp.float32,
        )
        smeared = jnp.concatenate((sums[0:Z_PAD], sums[Z_PAD : 2 * Z_PAD]), axis=1)
        sm_ref[v] = jnp.where(ones, 1.0, smeared).astype(jnp.bfloat16).astype(jnp.float32)
        own = pltpu.roll(sums[2 * Z_PAD :], 256 - MEAS_AT, 1)
        res_ref[v] = own[0:ROWS_DEV, 0:COLS_DEV]


def windows(sm_ref, offsets, size):
    lane = iota((size, 128), 1)
    placed = []
    for v in range(VIEWS):
        at = PLACE[v] & 127
        shift = (at - offsets[v]) & 127
        low = pltpu.roll(sm_ref[v, 0:size, 0:128], shift, 1)
        high = pltpu.roll(sm_ref[v, 0:size, 128:256], shift, 1)
        placed.append(jnp.where(lane < at + 128 - offsets[v], low, high))
    first = jnp.where(lane < 40, placed[0], jnp.where(lane < 80, placed[1], placed[2]))
    first = jnp.where(lane < 120, first, 0.0)
    second = jnp.where(lane < 40, placed[3], jnp.where(lane < 80, placed[4], 0.0))
    both = jnp.concatenate((first, second), axis=1)
    return both.astype(jnp.bfloat16)[:, 0:DEPTH]


def backward(w_ref, sm_ref, table_ref, old, store, subset, gz, size, ones):
    zi = slice_of(iota((size, LANES), 0), gz)
    inside = iota((size, LANES), 0) < min(Z_ALL, ones)
    total = jnp.sum(jnp.where(inside, hat(iota((size, LANES), 1), zi), 0.0), axis=1, keepdims=True)

    for tile in range(TILES):
        offsets = tile_offsets(table_ref, subset, tile)
        back = jnp.dot(
            windows(sm_ref, offsets, size), w_ref[tile], preferred_element_type=jnp.float32
        )
        norm = total * back[ones : ones + 1, :]
        store(tile, old(tile), back / jnp.maximum(norm, 1.0))


def swapped(rows, index, turn, axis):
    for d in (4, 2, 1):
        high = (index & d) != 0
        new = list(rows)
        for i in range(8):
            if i & d == 0:
                a, b = (rows[i], rows[i + d])
                new[i] = jnp.where(high, pltpu.roll(b, turn * d, axis), a)
                new[i + d] = jnp.where(high, b, pltpu.roll(a, turn * (8 - d), axis))
        rows = new
    return rows


def swap_blocks(rows):
    return swapped(rows, iota((8, 128), 1) >> 4, 16, 1)


def swap_sublanes(rows):
    return swapped(rows, iota((8, 128), 0), 1, 0)


def relay(read, out_ref, unrolled):
    def step(xb, nothing):
        for half in range(2):
            for b in range(2):
                x = xb * TILE + half * 8
                rows = swap_sublanes([read(b * 8 + z, x) for z in range(8)])
                for q, block in enumerate(swap_blocks(rows)):
                    out_ref[
                        xb * TILES_Y + q, b * 8 : b * 8 + 8, half * 128 : half * 128 + 128
                    ] = block
        return nothing

    if unrolled:
        for xb in range(X_DEV // TILE):
            step(xb, 0)
    else:
        lax.fori_loop(0, X_DEV // TILE, step, 0)


def pack_kernel(
    vol_hbm, meas_hbm, order_hbm, up_ref, down_ref, vol_ref, meas_ref, order_ref, row_ref, sems
):
    copies = [
        pltpu.make_async_copy(vol_hbm, vol_ref, sems.at[0]),
        pltpu.make_async_copy(meas_hbm, meas_ref, sems.at[1]),
        pltpu.make_async_copy(order_hbm, order_ref, sems.at[2]),
    ]
    for copy in copies:
        copy.start()
    row_ref[...] = jnp.zeros_like(row_ref)
    for copy in copies:
        copy.wait()
    for out_ref, z, r in (
        (up_ref, Z_DEV - Z_HALO, ROWS_DEV - M_HALO),
        (down_ref, 0, 0),
    ):
        slices = vol_ref[z * X_DEV : (z + Z_HALO) * X_DEV, :]
        out_ref[0:HALO_ROWS, :] = slices.astype(jnp.bfloat16)
        for v in range(VIEWS):
            at = (v * ROWS_DEV + r) * SUBSETS
            row_ref[:, 0:COLS_DEV] = meas_ref[at : at + SUBSETS * M_HALO, :]
            row = row_ref[...]
            rounded = row.astype(jnp.bfloat16).astype(jnp.float32)
            both = pltpu.roll(rounded, MEAS_AT - 128, 1)
            both = both + pltpu.roll(row - rounded, MEAS_AT - 128 - COLS_DEV, 1)
            at = EDGE_AT + v * SUBSETS * M_HALO
            out_ref[at : at + SUBSETS * M_HALO, :] = both.astype(jnp.bfloat16)


def prepare_kernel(
    order_ref, vol_ref, meas_ref,
    w0_ref, w1_ref, own_ref, mown_ref, table_ref, u_ref, flat_ref, sem,
):
    xy = lax.axis_index("xy")
    chosen = iota((TABLE[0], ANGLES), 0) == iota((TABLE[0], ANGLES), 1)
    chosen = jnp.where(chosen, order_ref[...].astype(jnp.float32), 0.0)
    chosen = jnp.broadcast_to(jnp.sum(chosen, axis=1, keepdims=True), TABLE)
    angles = 2.0 * math.pi * chosen / ANGLES
    cosine = jnp.cos(angles)
    sine = jnp.sin(angles)
    flat_ref[...], own = fill_table(cosine, sine, xy)
    copy = pltpu.make_async_copy(flat_ref, table_ref, sem)
    copy.start()
    relay(
        lambda z, x: vol_ref[pl.ds(pl.multiple_of(z * X_DEV + x, 8), 8), :], own_ref, False
    )
    mown_ref[...] = jnp.zeros_like(mown_ref)
    for s in range(SUBSETS):
        for v in range(VIEWS):
            for at, count in ((0, 8), (8, 8), (16, 4)):
                rows = meas_ref[pl.ds((v * ROWS_DEV + at) * 2 + s, count, stride=2), :]
                mown_ref[s, v, at : at + count, MEAS_AT - 128 : 128] = rows
    copy.wait()
    for subset, w_ref in ((0, w0_ref), (1, w1_ref)):
        positions(u_ref, cosine, sine, own, subset, xy)

        def step(tt, nothing):
            for t in range(8):
                tile = tt * 8 + t
                w_ref[tile] = weights(u_ref, tile_offsets(table_ref, subset, tile), tile)
            return nothing

        lax.fori_loop(0, TILES // 8, step, 0)


def first_kernel(
    table_ref, w_ref, own_ref, mown_ref, low_ref, high_ref,
    out_ref, side_ref, m1_ref, raw_ref, m0_ref, edge_ref, *acc_refs,
):
    gz = lax.axis_index("gz")
    for side, sent_ref in enumerate((low_ref, high_ref)):
        edge = sent_ref[EDGE_AT:SENT_ROWS, :].astype(jnp.float32)
        edge = edge + pltpu.roll(edge, COLS_DEV, 1)
        edge_ref[side] = jnp.where(iota(edge.shape, 1) >= MEAS_AT - 128, edge, 0.0)

    def read(z, x):
        if z >= 2 * Z_HALO:
            return jnp.full((8, NY), 1.0 if z == ONES - Z_DEV else 0.0, jnp.float32)
        sent_ref = low_ref if z < Z_HALO else high_ref
        at = z % Z_HALO * X_DEV + x
        return sent_ref[at : at + 8, :].astype(jnp.float32)

    relay(read, side_ref, True)
    for s, m_ref in ((0, m0_ref), (1, m1_ref)):
        per = ROWS_PER[s]
        m_ref[...] = jnp.zeros_like(m_ref)
        for v in range(VIEWS):
            edge = pl.ds(v * 2 * M_HALO + s, M_HALO, stride=2)
            high = edge_ref[1, edge, :]
            joined = jnp.concatenate(
                (
                    edge_ref[0, edge, :],
                    mown_ref[s, v, 0:16, :],
                    jnp.concatenate((mown_ref[s, v, 16:20, :], high[0:4]), axis=0),
                    jnp.concatenate((high[4:8], jnp.zeros((4, 128), jnp.float32)), axis=0),
                ),
                axis=0,
            )
            raw_ref[s, v] = pltpu.roll(
                joined, M_ROWS + ((gz + 1) >> 1) - (M_HALO - ROWS_BELOW[s]), 0
            )
            for group in range(GROUPS):
                at = group * 2 * (per + 1) + per + 1
                m_ref[v, at : at + per, :] = raw_ref[s, v, group * per : (group + 1) * per, :]

    def slices(tile):
        return jnp.concatenate((own_ref[tile], side_ref[tile]), axis=0).astype(jnp.bfloat16)

    forward(w_ref, slices, acc_refs, m0_ref, table_ref, out_ref, 0, gz)


def middle_kernel(
    table_ref, recv_ref, own_ref, side_ref, m_ref, w0_ref, w1_ref,
    out_ref, new_ref, sm_ref, vb_ref, *acc_refs,
):
    gz = lax.axis_index("gz")
    smear(recv_ref, sm_ref, gz)
    ones = iota((Z_PAD, VOXELS), 0) == ONES

    def old(tile):
        return jnp.concatenate((own_ref[tile], side_ref[tile]), axis=0)

    def store(tile, old, change):
        new = jnp.where(ones, 1.0, old + change)
        new_ref[tile] = new[0:Z_DEV]
        vb_ref[tile] = new.astype(jnp.bfloat16)

    backward(w0_ref, sm_ref, table_ref, old, store, 0, gz, Z_PAD, ONES)
    forward(w1_ref, lambda tile: vb_ref[tile], acc_refs, m_ref, table_ref, out_ref, 1, gz)


def last_kernel(
    table_ref, recv_ref, old_ref, w_ref,
    out_ref, res_ref, sm_ref, new_ref, block_ref, own_ref, sems,
):
    gz = lax.axis_index("gz")
    smear_last(recv_ref, sm_ref, own_ref, gz)
    copies = [pltpu.make_async_copy(own_ref, res_ref, sems.at[X_DEV // TILE])]
    copies[0].start()

    def store(tile, old, change):
        new_ref[tile] = old + change[0:Z_DEV]
        xb = tile // TILES_Y
        if tile % TILES_Y < TILES_Y - 1:
            return
        for half in range(2):
            for b in range(Z_DEV // 8):
                blocks = [
                    new_ref[xb * TILES_Y + q, b * 8 : b * 8 + 8, half * 128 : half * 128 + 128]
                    for q in range(TILES_Y)
                ]
                x = xb * TILE + half * 8
                for z, row in enumerate(swap_sublanes(swap_blocks(blocks))):
                    block_ref[b * 8 + z, x : x + 8, :] = row
        columns = pl.ds(xb * TILE, TILE)
        copies.append(
            pltpu.make_async_copy(
                block_ref.at[:, columns, :], out_ref.at[:, columns, :], sems.at[xb]
            )
        )
        copies[-1].start()

    backward(w_ref, sm_ref, table_ref, lambda tile: old_ref[tile], store, 1, gz, 24, Z_DEV)
    for copy in copies:
        copy.wait()


def owner_kernel(table_ref, recv_ref, out_ref, acc_ref, mea_ref, *sum_refs, subset):
    gz = lax.axis_index("gz")
    xy = lax.axis_index("xy")
    view = jnp.minimum(xy // GROUPS, VIEWS - 1)
    group = xy % GROUPS
    at = subset * VIEWS + view
    per = ROWS_PER[subset]
    half = per + 1
    lane = iota((8, 128), 1)
    for sum_ref in sum_refs:
        sum_ref[...] = jnp.zeros_like(sum_ref)
    mea_ref[...] = jnp.zeros_like(mea_ref)
    end = N_XY * 2 * half - 8

    def upper(s):
        row = s * 2 * half + half
        last = recv_ref[min(row, end) : min(row, end) + 8, :]
        return pltpu.roll(last, 8 - (row - end), 0) if row > end else last

    for s in range(N_XY):
        column = s * COLS_DEV
        own = jnp.where(lane >= MEAS_AT - 128, upper(s), 0.0)
        own = pltpu.roll(own, (column + 256 - MEAS_AT) % 128, 1)
        block = column // 128 * 128
        offset = column - block
        mea_ref[:, block : block + 128] += jnp.where(lane >= offset, own, 0.0)
        if offset + COLS_DEV > 128:
            mea_ref[:, block + 128 : block + 256] += jnp.where(lane < offset, own, 0.0)
    for s in range(N_XY):
        base = pl.multiple_of(table_ref[at, s], 128)
        shift = table_ref[at, SHIFT_AT + s]
        row = s * 2 * half
        low = pltpu.roll(recv_ref[row : row + 8, :], shift, 1)
        high = pltpu.roll(jnp.where(lane < WIN - 128, upper(s), 0.0), shift, 1)
        wrapped = lane < shift
        part_ref = sum_refs[s % SUMS]
        part_ref[:, pl.ds(base, 128)] += jnp.where(wrapped, 0.0, low)
        part_ref[:, pl.ds(base + 128, 128)] += jnp.where(wrapped, low, high)
        part_ref[:, pl.ds(base + 256, 128)] += jnp.where(wrapped, high, 0.0)
    slot = iota((8, NZ), 0)
    row = first_row(gz, subset) + group * per + slot
    ray_rows = jnp.where(slot < per, hat(row, iota((8, NZ), 1)), 0.0)
    ray_rows = jnp.sum(ray_rows, axis=1, keepdims=True)
    sums = sum_refs[0][...]
    for part_ref in sum_refs[1:]:
        sums = sums + part_ref[...]
    totals = sums[per : per + 1, :]
    acc_ref[...] = mea_ref[...] - sums / jnp.maximum(ray_rows * totals, 1.0)
    for t in range(N_XY):
        base = pl.multiple_of(table_ref[at, t], 128)
        shift = table_ref[at, SHIFT_AT + t]
        back = (128 - shift) & 127
        a = pltpu.roll(acc_ref[:, pl.ds(base, 128)], back, 1)
        b = pltpu.roll(acc_ref[:, pl.ds(base + 128, 128)], back, 1)
        c = pltpu.roll(acc_ref[:, pl.ds(base + 256, 128)], back, 1)
        kept = lane < 128 - shift
        low = jnp.where(kept, a, b)
        high = jnp.where(kept, b, c)
        if subset == 0:
            other = pltpu.roll(high, COLS_DEV, 1)
            even = jnp.where(
                slot == 5,
                pltpu.roll(high, 5, 0),
                jnp.where(slot == 6, pltpu.roll(high, 4, 0), pltpu.roll(high, 3, 0)),
            )
            odd = jnp.where(slot == 5, pltpu.roll(other, 4, 0), pltpu.roll(other, 3, 0))
            rest = jnp.where(lane < COLS_DEV, even, odd)
            out_ref[t] = jnp.where(slot < 5, low, rest).astype(jnp.bfloat16)
            continue
        column = t * COLS_DEV
        block = column // 128 * 128
        offset = column - block
        turn = (MEAS_AT - 128 - offset) % 128
        own = pltpu.roll(acc_ref[:, block : block + 128], turn, 1)
        if offset + COLS_DEV > 128:
            more = pltpu.roll(acc_ref[:, block + 128 : block + 256], turn, 1)
            own = jnp.where(lane < MEAS_AT - offset, own, more)
        high = jnp.where(lane >= MEAS_AT - 128, own, high)
        out_ref[t * 8 : (t + 1) * 8, :] = jnp.where(slot < 4, low, pltpu.roll(high, 4, 0))


def call(kernel, inputs, outs, scratch, name):
    vmem = pl.BlockSpec(memory_space=pltpu.VMEM)
    smem = pl.BlockSpec(memory_space=pltpu.SMEM)
    anywhere = pl.BlockSpec(memory_space=pl.ANY)

    def spec(x):
        if x.dtype == jnp.int32:
            return smem
        return anywhere if isinstance(x, jax.ShapeDtypeStruct) else vmem

    inputs = [
        x if x.dtype == jnp.int32 else pltpu.with_memory_space_constraint(x, pltpu.VMEM)
        for x in inputs
    ]
    return pl.pallas_call(
        kernel,
        in_specs=[spec(x) for x in inputs],
        out_specs=[spec(x) for x in outs],
        out_shape=outs,
        scratch_shapes=scratch,
        compiler_params=pltpu.CompilerParams(vmem_limit_bytes=12 * 1024 * 1024),
        name=name,
    )(*inputs)


def exchanged(parts, shape):
    sent = lax.all_to_all(
        parts.reshape(shape), "xy", split_axis=0, concat_axis=0, tiled=True
    )
    return sent.reshape(parts.shape)


def local(volume, measured, view_order):
    f32 = jnp.float32
    bf16 = jnp.bfloat16
    vmem = pltpu.VMEM
    flat = volume.reshape(Z_DEV * X_DEV, NY)
    order = view_order.reshape(1, ANGLES)
    rows = measured.transpose(1, 2, 0, 3).reshape(VIEWS * ROWS_DEV * SUBSETS, COLS_DEV)
    made = vmem((TILES, DEPTH, VOXELS), bf16)
    slices = vmem((TILES, Z_DEV, VOXELS), f32)
    sm_scratch = vmem((VIEWS, Z_PAD, LANES), f32)
    acc_scratch = [vmem((WIN, 128), f32)] * VIEWS
    row_scratch = vmem((8, FULL), f32)
    owner_scratch = [row_scratch] * (2 + SUMS)

    sent = vmem((SENT_ROWS, 128), bf16)
    hbm = pl.BlockSpec(memory_space=pltpu.HBM)
    up, down, flat, rows, order = pl.pallas_call(
        pack_kernel,
        in_specs=[hbm] * 3,
        out_specs=[pl.BlockSpec(memory_space=vmem)] * 5,
        out_shape=[
            sent, sent, vmem(flat.shape, f32), vmem(rows.shape, f32), vmem((1, ANGLES), jnp.int32)
        ],
        scratch_shapes=[vmem((SUBSETS * M_HALO, 128), f32), pltpu.SemaphoreType.DMA((3,))],
        compiler_params=pltpu.CompilerParams(vmem_limit_bytes=12 * 1024 * 1024),
        name="pack",
    )(*(pltpu.with_memory_space_constraint(x, pltpu.HBM) for x in (flat, rows, order)))
    next_up = [(i, (i + 1) % N_GZ) for i in range(N_GZ)]
    low = lax.ppermute(up, "gz", next_up)
    high = lax.ppermute(down, "gz", [(j, i) for i, j in next_up])
    w0, w1, own, mown, table = pl.pallas_call(
        prepare_kernel,
        in_specs=[pl.BlockSpec(memory_space=vmem)] * 3,
        out_specs=[pl.BlockSpec(memory_space=m) for m in (vmem, vmem, vmem, vmem, pltpu.SMEM)],
        out_shape=[
            made, made, slices, vmem((SUBSETS, VIEWS, 24, 128), f32), pltpu.SMEM(TABLE, jnp.int32)
        ],
        scratch_shapes=[
            vmem((VIEWS, TILES, VOXELS), f32), vmem(TABLE, jnp.int32), pltpu.SemaphoreType.DMA
        ],
        compiler_params=pltpu.CompilerParams(vmem_limit_bytes=12 * 1024 * 1024),
        name="prepare",
    )(*(pltpu.with_memory_space_constraint(x, vmem) for x in (order, flat, rows)))
    partial, side, m1 = call(
        first_kernel,
        (table, w0, own, mown, low, high),
        [vmem((N_XY * 12, 128), f32), slices, vmem((VIEWS, 64, 128), f32)],
        [
            vmem((SUBSETS, VIEWS, M_ROWS, 128), f32),
            vmem((VIEWS, 72, 128), f32),
            vmem((2, EDGE_ROWS, 128), f32),
            *acc_scratch,
        ],
        "first",
    )
    (rounded,) = call(
        functools.partial(owner_kernel, subset=0),
        (table, exchanged(partial, (N_XY, 3, 4, 128))),
        [vmem((N_XY, 8, 128), bf16)],
        owner_scratch,
        "owner_a",
    )
    partial, new = call(
        middle_kernel,
        (table, exchanged(rounded, rounded.shape), own, side, m1, w0, w1),
        [vmem((N_XY * 10, 128), f32), slices],
        [sm_scratch, vmem((TILES, Z_PAD, VOXELS), bf16), *acc_scratch],
        "middle",
    )
    (final,) = call(
        functools.partial(owner_kernel, subset=1),
        (table, exchanged(partial, (N_XY, 5, 2, 128))),
        [vmem((N_XY * 8, 128), f32)],
        owner_scratch,
        "owner_b",
    )
    volume_out, residual = call(
        last_kernel,
        (table, exchanged(final, (N_XY, 8, 128)), new, w1),
        [
            jax.ShapeDtypeStruct(VOLUME, f32),
            jax.ShapeDtypeStruct((VIEWS, ROWS_DEV, COLS_DEV), f32),
        ],
        [
            sm_scratch,
            slices,
            vmem(VOLUME, f32),
            vmem((VIEWS, ROWS_DEV, COLS_DEV), f32),
            pltpu.SemaphoreType.DMA((X_DEV // TILE + 1,)),
        ],
        "last",
    )
    return volume_out, residual


def solution(mesh):
    in_specs = (P("gz", "xy", None), P(None, None, "gz", "xy"), P())
    out_specs = (P("gz", "xy", None), P(None, "gz", "xy"))
    return jax.shard_map(local, mesh=mesh, in_specs=in_specs, out_specs=out_specs, check_vma=False)
```
